32 devices in a mesh: group: 2 (over x), grid: 8 (over z, y), var: 2 (over core).
Axes of the slice: x: 2, y: 2, z: 4, core: 2. Of those that a mesh axis runs over, the one named last changes fastest.
Arguments:
- tokens: bfloat16 [96, 96, 3, 512], P('group', 'grid'), parts along dimension 0, may hold values from -6 to 6
- key_mask: int32 [96, 96], P('group', 'grid'), parts along dimension 0, may hold values 0 or 1
- w_qkv: bfloat16 [3, 512, 512], P(None, None, 'var'), may hold values from -16 to 16
- w_proj: bfloat16 [512, 512], P('var'), may hold values from -0.25 to 0.25
- w_up: bfloat16 [512, 2048], P(None, 'var'), may hold values from -0.25 to 0.25
- w_down: bfloat16 [2048, 512], P('var'), may hold values from -0.125 to 0.125
- level_query: bfloat16 [13, 512], replicated, may hold values from -1200 to 1200
- w_dec_q: bfloat16 [512, 512], P(None, 'var'), may hold values from -0.25 to 0.25
- w_dec_kv: bfloat16 [2, 512, 512], P(None, None, 'var'), may hold values from -0.25 to 0.25
- w_dec_o: bfloat16 [512, 512], P('var'), may hold values from -0.25 to 0.25
- decode_matrix: float32 [512, 64], replicated, may hold values from -0.25 to 0.25
Outputs:
- estimated_maps: float32 [4, 26, 192, 384], P('var', 'group', 'grid'), parts along dimension 1
The draws below stay inside these ranges and needn't reach their ends.
There are 2 independent parts, one for each index of `group`. The reference program is written for one: setup_inputs(seed, part) draws one part's arguments, and reference() takes and returns one part's arrays. A program takes and returns all parts, laid end to end along the dimension named above; an argument that names none is the same for every part. Nothing has to cross between parts.
All inputs are finite; a program needn't handle non-finite values. No bound on the sum of `key_mask` on one device may be relied on, other than what follows from the above.
Results may differ from the reference program's by a relative error of at most 0.025.
Values may be sent and summed in bfloat16 or wider, within the bound.
A program may use at most 128 MiB of HBM per device.

```python
import jax
import jax.numpy as jnp
from jax import lax

EMBED_WIDTH = 512
HD = 64
FF = 2048
TARGET_QUANTITY = 4
ISOBAR_NUMBER = 13
LEV = 3
SQUARE_SPAN = 4
WIN_LAT = 6
WINDOW_EASTWARD = 12
LAT = 48
LON = 96


def draw_w_qkv(key, part):
    key = jax.random.fold_in(key, 11)
    base_key = jax.random.fold_in(key, 0)
    result = jnp.clip(jax.random.normal(base_key, (3, EMBED_WIDTH, EMBED_WIDTH), jnp.float32), -6.0, 6.0) * EMBED_WIDTH ** (-0.5)
    return result.astype(jnp.bfloat16)


def draw_level_query(key, part):
    key = jax.random.fold_in(key, 23)
    base_key = jax.random.fold_in(key, 0)
    result = jnp.clip(jax.random.normal(base_key, (ISOBAR_NUMBER, EMBED_WIDTH), jnp.float32), -6.0, 6.0)
    return result.astype(jnp.bfloat16)


def touch_ends(array, rng, smallest, top_value):
    shape = array.shape
    spot = [jax.random.randint(jax.random.fold_in(rng, axis), (), 0, shape[axis]) for axis in range(len(shape))]
    array = array.at[tuple(spot)].set(smallest)
    longest = shape.index(max(shape))
    spot[longest] = (spot[longest] + 1) % shape[longest]
    return array.at[tuple(spot)].set(top_value)


def shard_levels(key, shape, pieces, low, high):
    level, own = 1.0, jax.random.fold_in(key, 6)
    for dim, blocks in pieces:
        heights = jnp.exp(jax.random.uniform(jax.random.fold_in(own, dim), (blocks,), jnp.float32, low / len(pieces), high / len(pieces)))
        level = level * jnp.repeat(heights, shape[dim] // blocks).reshape([-1 if axis == dim else 1 for axis in range(len(shape))])
    return level


def normal_values(key, dims, scale, bound, cuts=(), dtype=jnp.bfloat16):
    level = shard_levels(key, dims, cuts, -0.22, 0.18) if cuts else 1.0
    entries = jax.random.normal(key, dims, jnp.float32) * scale * level
    return jnp.minimum(jnp.maximum(entries, -bound), bound).astype(dtype)


def setup_inputs(seed: int = 0, part: int = 0) -> dict:
    streams_of = jax.random.split(jax.random.key(seed), 12)
    part_splits = jax.random.split(jax.random.fold_in(streams_of[11], part), 12)
    return {
        "tokens": normal_values(part_splits[0], (LAT, LON, LEV, EMBED_WIDTH), 1.0, 6.0, ((1, 8),)),
        "key_mask": touch_ends((jax.random.randint(part_splits[1], (LAT, LON), 0, 4) < 3).astype(jnp.int32), jax.random.fold_in(part_splits[1], 1), 0, 1),
        "w_qkv": draw_w_qkv(jax.random.fold_in(streams_of[11], 71), part),
        "w_proj": normal_values(streams_of[3], (EMBED_WIDTH, EMBED_WIDTH), EMBED_WIDTH ** -0.5, 0.25, ((0, 2),)),
        "w_up": normal_values(streams_of[4], (EMBED_WIDTH, FF), EMBED_WIDTH ** -0.5, 0.25, ((1, 2),)),
        "w_down": normal_values(streams_of[5], (FF, EMBED_WIDTH), FF ** -0.5, 0.125, ((0, 2),)),
        "level_query": draw_level_query(jax.random.fold_in(streams_of[11], 71), part),
        "w_dec_q": normal_values(streams_of[7], (EMBED_WIDTH, EMBED_WIDTH), EMBED_WIDTH ** -0.5, 0.25, ((1, 2),)),
        "w_dec_kv": normal_values(streams_of[8], (2, EMBED_WIDTH, EMBED_WIDTH), EMBED_WIDTH ** -0.5, 0.25, ((2, 2),)),
        "w_dec_o": normal_values(streams_of[9], (EMBED_WIDTH, EMBED_WIDTH), EMBED_WIDTH ** -0.5, 0.25, ((0, 2),)),
        "decode_matrix": normal_values(streams_of[10], (EMBED_WIDTH, TARGET_QUANTITY * SQUARE_SPAN * SQUARE_SPAN), EMBED_WIDTH ** -0.5, 0.25, (), jnp.float32),
    }


EPSILON = 1e-05

def layer_norm(values):
    center = values - lax.optimization_barrier(jnp.mean(values, axis=-1, keepdims=True))
    spread = lax.optimization_barrier(jnp.mean(center * center, axis=-1, keepdims=True))
    return center * lax.rsqrt(spread + EPSILON)

def window_attention(tile_tokens, key_marks, row_start, total_rows, w_qkv, w_proj):
    north_south_circles, columns, levels, features = tile_tokens.shape
    local_width = w_qkv.shape[2]
    head_count = local_width // HD
    normed = layer_norm(tile_tokens.astype(jnp.float32)).astype(jnp.bfloat16).reshape(-1, features)
    win_count = north_south_circles // WIN_LAT
    tok_count = WIN_LAT * columns * levels

    def project(which):
        result = jnp.dot(normed, w_qkv[which], preferred_element_type=jnp.float32)
        return result.astype(jnp.bfloat16).reshape(win_count, tok_count, head_count, HD)
    queries = project(0)
    key_heads = project(1)
    value_heads = project(2)
    scores = jnp.einsum('wqhd,wkhd->whqk', queries.astype(jnp.float32), key_heads.astype(jnp.float32)) * HD ** (-0.5)
    row_index = lax.broadcasted_iota(jnp.int32, (north_south_circles, columns, levels), 0).reshape(win_count, tok_count)
    region = row_index + row_start >= total_rows - WIN_LAT // 2
    open_key = jnp.broadcast_to(key_marks[:, :, None], (north_south_circles, columns, levels)).reshape(win_count, tok_count) > 0
    diagonal = lax.broadcasted_iota(jnp.int32, (tok_count, tok_count), 0) == lax.broadcasted_iota(jnp.int32, (tok_count, tok_count), 1)
    allowed = (region[:, :, None] == region[:, None, :]) & (open_key[:, None, :] | diagonal[None])
    scores = jnp.where(allowed[:, None], scores, jnp.float32(-1e+30))
    peak_score = lax.optimization_barrier(jnp.max(scores, axis=-1, keepdims=True))
    exp_scores = jnp.exp(scores - peak_score)
    weights = (exp_scores / lax.optimization_barrier(jnp.sum(exp_scores, axis=-1, keepdims=True))).astype(jnp.bfloat16)
    context = jnp.einsum('whqk,wkhd->wqhd', weights.astype(jnp.float32), value_heads.astype(jnp.float32))
    context = context.astype(jnp.bfloat16).reshape(-1, local_width)
    return jnp.dot(context, w_proj, preferred_element_type=jnp.float32).reshape(north_south_circles, columns, levels, features)

def level_decoder(latent, level_query, w_dec_q, w_dec_kv, w_dec_o):
    north_south_circles, columns, levels, features = latent.shape
    local_width = w_dec_kv.shape[2]
    head_count = local_width // HD
    patches = north_south_circles * columns
    normed = layer_norm(latent.astype(jnp.float32)).astype(jnp.bfloat16).reshape(-1, features)
    dkeys = jnp.dot(normed, w_dec_kv[0], preferred_element_type=jnp.float32).astype(jnp.bfloat16)
    dvals = jnp.dot(normed, w_dec_kv[1], preferred_element_type=jnp.float32).astype(jnp.bfloat16)
    dkeys = dkeys.reshape(patches, levels, head_count, HD)
    dvals = dvals.reshape(patches, levels, head_count, HD)
    dquery = jnp.dot(level_query, w_dec_q, preferred_element_type=jnp.float32).reshape(-1, head_count, HD)
    scores = jnp.einsum('lhd,pjhd->plhj', dquery, dkeys.astype(jnp.float32)) * HD ** (-0.5)
    peak_score = lax.optimization_barrier(jnp.max(scores, axis=-1, keepdims=True))
    exp_scores = jnp.exp(scores - peak_score)
    dweights = (exp_scores / lax.optimization_barrier(jnp.sum(exp_scores, axis=-1, keepdims=True))).astype(jnp.bfloat16)
    dcontext = jnp.einsum('plhj,pjhd->plhd', dweights.astype(jnp.float32), dvals.astype(jnp.float32))
    dcontext = dcontext.astype(jnp.bfloat16).reshape(-1, local_width)
    return jnp.dot(dcontext, w_dec_o, preferred_element_type=jnp.float32)

def reference(tokens, key_mask, w_qkv, w_proj, w_up, w_down, level_query, w_dec_q, w_dec_kv, w_dec_o, decode_matrix):
    north_south_circles, east_west_bands_set, levels, features = tokens.shape
    half_lat = WIN_LAT // 2
    half_lon = WINDOW_EASTWARD // 2
    block_count = east_west_bands_set // WINDOW_EASTWARD
    rolled = jnp.roll(tokens, (-half_lat, -half_lon), (0, 1))
    rolled_mask = jnp.roll(key_mask, (-half_lat, -half_lon), (0, 1))
    rolled = jnp.moveaxis(rolled.reshape(north_south_circles, block_count, WINDOW_EASTWARD, levels, features), 1, 0)
    rolled_mask = jnp.moveaxis(rolled_mask.reshape(north_south_circles, block_count, WINDOW_EASTWARD), 1, 0)

    def attend(block_pair):
        return window_attention(block_pair[0], block_pair[1], 0, north_south_circles, w_qkv, w_proj)
    attended = lax.map(attend, (rolled, rolled_mask))
    attended = jnp.moveaxis(attended, 0, 1).reshape(north_south_circles, east_west_bands_set, levels, features)
    attended = jnp.roll(attended, (half_lat, half_lon), (0, 1))
    x_one = tokens.astype(jnp.float32) + attended
    x_blocks = jnp.moveaxis(x_one.reshape(north_south_circles, block_count, WINDOW_EASTWARD, levels, features), 1, 0)

    def finish(x_block):
        normed = layer_norm(x_block).astype(jnp.bfloat16)
        hidden = jax.nn.gelu(jnp.dot(normed, w_up, preferred_element_type=jnp.float32), approximate=False).astype(jnp.bfloat16)
        latent = (x_block + jnp.dot(hidden, w_down, preferred_element_type=jnp.float32)).astype(jnp.bfloat16)
        dec_hidden = level_decoder(latent, level_query, w_dec_q, w_dec_kv, w_dec_o)
        cell_measures = jnp.dot(dec_hidden, decode_matrix, precision=lax.Precision.HIGHEST, preferred_element_type=jnp.float32)
        return cell_measures.reshape(north_south_circles, WINDOW_EASTWARD, ISOBAR_NUMBER, TARGET_QUANTITY, SQUARE_SPAN, SQUARE_SPAN)
    cell_measures = lax.map(finish, x_blocks)
    estimated_maps = jnp.transpose(cell_measures, (4, 3, 1, 5, 0, 2, 6))
    return estimated_maps.reshape(TARGET_QUANTITY, ISOBAR_NUMBER, north_south_circles * SQUARE_SPAN, east_west_bands_set * SQUARE_SPAN)
```

```python
import functools

import jax
import jax.numpy as jnp
import numpy as np
from jax import lax
from jax.experimental import pallas as pl
from jax.experimental.pallas import tpu as pltpu
from jax.sharding import PartitionSpec as P

HD = 64
TARGET_QUANTITY = 4
SQUARE_SPAN = 4
WIN_LAT = 6
EPSILON = 1e-05
BLOCK = 128
KEYS = 256
CHUNK = 256
LEVEL_SLOTS = 16
MESH = pl.DeviceIdType.MESH
NT = (((1,), (1,)), ((), ()))
F32 = jnp.float32
BF16 = jnp.bfloat16


def layer_norm(values):
    center = values - jnp.mean(values, axis=-1, keepdims=True)
    spread = jnp.mean(center * center, axis=-1, keepdims=True)
    return center * lax.rsqrt(spread + EPSILON)


class Geometry:
    def __init__(self, tokens, w_proj, level_query, decode_matrix, cores, bands):
        self.rows, self.cols, self.levels, self.features = tokens.shape
        self.cores, self.bands = cores, bands
        self.half_cols = self.cols // 2
        self.row_count = self.rows // cores
        self.windows = self.row_count // WIN_LAT
        self.taken = 8 * (-(-(self.row_count + WIN_LAT // 2) // 8))
        self.half_patches = WIN_LAT * self.half_cols
        self.half = 16 * (-(-(self.levels * self.half_patches) // 16))
        self.tokens = 2 * self.half
        self.patches = 2 * self.half_patches
        self.width = w_proj.shape[0]
        self.heads = self.width // HD
        self.isobars = level_query.shape[0]
        self.slots = self.isobars + self.isobars % 2
        self.pixels = decode_matrix.shape[1]
        self.scatter = bands * WIN_LAT == self.rows and (bands * self.cols * SQUARE_SPAN) % BLOCK == 0

    def place(self, half, level, r, c):
        return half * self.half + level * self.half_patches + r * self.half_cols + c

    def each(self):
        for half in range(2):
            for level in range(self.levels):
                for r in range(WIN_LAT):
                    for c in range(self.half_cols):
                        yield half, level, r, c

    def gather_table(self):
        table = np.zeros((self.windows, self.half, self.half_cols * self.levels * self.taken), np.float32)
        for w in range(self.windows):
            for half, level, r, c in self.each():
                if half == 0:
                    source = (c * self.levels + level) * self.taken + WIN_LAT * w + WIN_LAT // 2 + r
                    table[w, self.place(0, level, r, c), source] = 1.0
        return table.reshape(self.windows * self.half, -1)

    def order_table(self):
        table = np.zeros((KEYS, self.tokens), np.float32)
        for half, level, r, c in self.each():
            patch = r * self.cols + half * self.half_cols + c
            table[level * self.patches + patch, self.place(half, level, r, c)] = 1.0
        return table

    def position_table(self):
        table = np.full((8, KEYS), -1, np.int32)
        table[0] = 0
        for half, level, r, c in self.each():
            at = self.place(half, level, r, c)
            table[0, at] = r
            table[1 + half, at] = c + (self.half_cols if half == 0 else 0)
        return table

    def pixel_table(self):
        table = np.zeros((self.pixels, self.pixels), np.float32)
        own = TARGET_QUANTITY // self.cores
        for v in range(TARGET_QUANTITY):
            for a in range(SQUARE_SPAN):
                for b in range(SQUARE_SPAN):
                    target = ((v // own * SQUARE_SPAN + b) * own + v % own) * SQUARE_SPAN + a
                    table[target, (v * SQUARE_SPAN + a) * SQUARE_SPAN + b] = 1.0
        return table

    def pick_table(self):
        half_lat = WIN_LAT // 2
        run = self.cols * SQUARE_SPAN
        picks = np.zeros((SQUARE_SPAN, BLOCK, 3 * BLOCK), np.float32)
        for ih in range(2):
            for q in range(half_lat * run):
                r, rest = divmod(q, run)
                column, b = divmod(rest, SQUARE_SPAN)
                source = (half_lat * ih + r) * self.cols + column
                target = ih * BLOCK + q if q < BLOCK else 2 * BLOCK + ih * (BLOCK // 2) + q - BLOCK
                picks[b, source, target] = 1.0
        return picks


def fold_decoder(lq, wq, wkv_ref, wo, dm, perm, out_ref):
    width = wq.shape[1]
    heads = width // HD
    dquery = jnp.dot(lq, wq, preferred_element_type=F32) * HD ** (-0.5)
    d_hi = dquery.astype(BF16)
    d_lo = (dquery - d_hi.astype(F32)).astype(BF16)
    count = LEVEL_SLOTS * heads
    row = lax.broadcasted_iota(jnp.int32, (count, dquery.shape[0]), 0)
    slot = lax.broadcasted_iota(jnp.int32, (count, dquery.shape[0]), 1)
    spread = (row // heads == slot).astype(F32).astype(BF16)
    row = lax.broadcasted_iota(jnp.int32, (count, width), 0)
    mine = row % heads == lax.broadcasted_iota(jnp.int32, (count, width), 1) // HD
    q_hi = jnp.dot(spread, d_hi, preferred_element_type=F32)
    q_hi = jnp.where(mine, q_hi, 0.0).astype(BF16)
    q_lo = jnp.dot(spread, d_lo, preferred_element_type=F32)
    q_lo = jnp.where(mine, q_lo, 0.0).astype(BF16)
    wk = wkv_ref[0]
    g = lax.dot_general(q_hi, wk, NT, preferred_element_type=F32)
    g = g + lax.dot_general(q_lo, wk, NT, preferred_element_type=F32)
    g_hi = g.astype(BF16)
    out_ref[0, 0:count, :] = g_hi
    out_ref[0, count : 2 * count, :] = (g - g_hi.astype(F32)).astype(BF16)
    dm_hi = dm.astype(BF16)
    dm_lo = (dm - dm_hi.astype(F32)).astype(BF16)
    dm_hi = jnp.dot(perm, dm_hi, preferred_element_type=F32).astype(BF16)
    dm_lo = jnp.dot(perm, dm_lo, preferred_element_type=F32).astype(BF16)
    m_t = lax.dot_general(dm_hi, wo, NT, preferred_element_type=F32)
    m_t = m_t + lax.dot_general(dm_lo, wo, NT, preferred_element_type=F32)
    pixels = m_t.shape[0]
    stacked = jnp.concatenate([m_t] * heads, axis=0)
    row_head = lax.broadcasted_iota(jnp.int32, stacked.shape, 0) // pixels
    lane_head = lax.broadcasted_iota(jnp.int32, stacked.shape, 1) // HD
    stacked = jnp.where(row_head == lane_head, stacked, 0.0)
    s_hi = stacked.astype(BF16)
    s_lo = (stacked - s_hi.astype(F32)).astype(BF16)
    wv = wkv_ref[1]
    n_t = lax.dot_general(s_hi, wv, NT, preferred_element_type=F32)
    n_t = n_t + lax.dot_general(s_lo, wv, NT, preferred_element_type=F32)
    out_ref[0, 2 * count :, :] = n_t.astype(BF16)


def main_kernel(
    geo,
    tok_ref,
    mask_ref,
    wqkv_ref,
    wproj_ref,
    wup_ref,
    wdown_ref,
    lq_ref,
    wq_ref,
    wkv_ref,
    wo_ref,
    dm_ref,
    gather_ref,
    order_ref,
    position_ref,
    perm_ref,
    pick_ref,
    out_ref,
    raw,
    marks,
    qkv,
    proj,
    up,
    down,
    lq,
    wq,
    wkv,
    wo,
    dm,
    gather,
    order,
    position,
    perm,
    pick,
    fold,
    first,
    own,
    halo,
    differs,
    hid,
    dw,
    du,
    base_pix,
    pix,
    pieces,
    checked,
    load_sem,
    weight_send,
    weight_recv,
    halo_send,
    halo_recv,
    piece_send,
    piece_recv,
):
    group, grid, var = (lax.axis_index(name) for name in ("group", "grid", "var"))
    bands, cores, windows, half = geo.bands, geo.cores, geo.windows, geo.half
    features, levels, width, heads = geo.features, geo.levels, geo.width, geo.heads
    sibling = (group, grid, lax.rem(var + 1, cores))
    west = (group, lax.rem(grid + bands - 1, bands), var)
    east = (group, lax.rem(grid + 1, bands), var)
    barrier = pltpu.get_barrier_semaphore()
    if geo.scatter:
        peers = bands * cores
        me = grid * cores + var

        @pl.loop(1, peers)
        def _(step):
            peer = lax.rem(me + step, peers)
            pl.semaphore_signal(
                barrier, inc=1, device_id=(group, peer // cores, lax.rem(peer, cores)), device_id_type=MESH
            )

        greeted = peers - 1
    else:
        for peer in (sibling, west, east):
            pl.semaphore_signal(barrier, inc=1, device_id=peer, device_id_type=MESH)
        greeted = 3

    loads = []

    def load(source, target):
        copy = pltpu.make_async_copy(source, target, load_sem.at[len(loads)])
        copy.start()
        loads.append(copy)
        return copy

    tiles = geo.rows // 8
    first_tile = var * (geo.row_count // 8)
    slabs = []
    for s in range(geo.taken // 8):
        tile = lax.rem(first_tile + s, tiles)
        slabs.append(
            load(tok_ref.at[:, :, pl.ds(pl.multiple_of(tile * 8, 8), 8), :], raw.at[:, :, 8 * s : 8 * s + 8, :])
        )
    gather_load = load(gather_ref, gather)
    fold_loads = [
        load(a, b)
        for a, b in ((lq_ref, lq), (wq_ref, wq), (wkv_ref, wkv), (wo_ref, wo), (dm_ref, dm), (perm_ref, perm))
    ]
    late_loads = [
        load(a, b)
        for a, b in (
            (mask_ref, marks.at[0]),
            (wqkv_ref, qkv.at[0]),
            (wproj_ref, proj.at[0]),
            (wup_ref, up.at[0]),
            (wdown_ref, down.at[0]),
            (position_ref, position),
            (order_ref, order),
            (pick_ref, pick),
        )
    ]

    for copy in slabs:
        copy.wait()
    gather_load.wait()
    depth = geo.half_cols * levels * geo.taken
    for h, target in ((0, first), (1, own)):
        slab = raw[h * geo.half_cols : (h + 1) * geo.half_cols].reshape(depth, features)
        for c in range(0, features, CHUNK):
            rows = jnp.dot(gather[...], slab[:, c : c + CHUNK], preferred_element_type=F32).astype(BF16)
            target[:, :, c : c + CHUNK] = rows.reshape(windows, half, CHUNK)

    pl.semaphore_wait(barrier, greeted)

    def remote(source, target, send, recv, peer):
        copy = pltpu.make_async_remote_copy(
            src_ref=source, dst_ref=target, send_sem=send, recv_sem=recv, device_id=peer, device_id_type=MESH
        )
        copy.start()
        return copy

    copies = [remote(mask_ref, marks.at[1], weight_send.at[0], weight_recv.at[0], west)]
    halos = []
    for w in range(windows):
        halos.append(remote(first.at[w], halo.at[w], halo_send.at[w], halo_recv.at[w], west))
    for n, (source, target) in enumerate(((wqkv_ref, qkv), (wproj_ref, proj), (wup_ref, up), (wdown_ref, down))):
        copies.append(remote(source, target.at[1], weight_send.at[n + 1], weight_recv.at[n + 1], sibling))

    for copy in fold_loads:
        copy.wait()
    fold_decoder(lq[...], wq[...], wkv, wo[...], dm[...], perm[...], fold)

    tokens = geo.tokens
    q_pos = lax.broadcasted_iota(jnp.int32, (tokens, KEYS), 0)
    k_pos = lax.broadcasted_iota(jnp.int32, (tokens, KEYS), 1)
    diagonal = q_pos == k_pos

    def region_of(pos):
        pos = jnp.where(pos >= half, pos - half, pos)
        for level in range(levels - 1, 0, -1):
            start = geo.half_patches * level
            pos = jnp.where(pos >= start, pos - geo.half_patches, pos) if level == 1 else jnp.where(
                pos >= start, pos - start, pos
            )
        return pos >= geo.half_patches // 2

    differs[...] = jnp.where(region_of(q_pos) != region_of(k_pos), -1e30, 0.0)
    lane_head = lax.broadcasted_iota(jnp.int32, (tokens, width), 1) // HD
    lane_head_keys = lax.broadcasted_iota(jnp.int32, (KEYS, width), 1) // HD

    for copy in late_loads:
        copy.wait()
    copies.append(remote(fold.at[0], fold.at[1], weight_send.at[5], weight_recv.at[5], sibling))
    for copy in copies:
        copy.wait()

    count = heads * LEVEL_SLOTS
    pixels = geo.pixels
    patches = geo.patches
    row_size = pixels // cores // SQUARE_SPAN
    rows = geo.slots * row_size
    half_lat = WIN_LAT // 2
    extra = half_lat * geo.cols * SQUARE_SPAN - BLOCK
    pair = 8 // heads

    def piece_copy(w, ih, core, action):
        band = lax.rem(var * windows + w + ih, bands)
        here = jnp.logical_and(band == grid, core == var)
        source, target = pieces.at[w, ih, core], out_ref.at[grid, ih]

        @pl.when(here)
        def _():
            if action == "start":
                pltpu.make_async_copy(source, target, piece_recv.at[grid, ih]).start()

        @pl.when(jnp.logical_not(here))
        def _():
            if action == "start":
                pltpu.make_async_remote_copy(
                    src_ref=source,
                    dst_ref=target,
                    send_sem=piece_send.at[w, ih, core],
                    recv_sem=piece_recv.at[grid, ih],
                    device_id=(group, band, core),
                    device_id_type=MESH,
                ).start()
            else:
                pltpu.make_async_copy(source, source, piece_send.at[w, ih, core]).wait()

    @pl.loop(0, windows)
    def _(w):
        pltpu.make_async_copy(halo.at[w], halo.at[w], halo_recv.at[w]).wait()
        x = jnp.concatenate([own[w], halo[w]], axis=0).astype(F32)
        n1 = layer_norm(x).astype(BF16)
        target = position[0:1, :] + (var * geo.row_count + WIN_LAT * w + half_lat)
        target = jnp.where(target >= geo.rows, target - geo.rows, target)
        there = lax.broadcasted_iota(jnp.int32, (geo.rows, KEYS), 0) == target
        there = there.astype(F32).astype(BF16)
        opened = jnp.zeros((1, KEYS), F32)
        column = lax.broadcasted_iota(jnp.int32, (geo.cols, KEYS), 0)
        for h in range(2):
            seen = (marks[h] > 0).astype(F32).astype(BF16)
            seen = jnp.dot(seen, there, preferred_element_type=F32)
            seen = jnp.where(column == position[1 + h : 2 + h, :], seen, 0.0)
            opened = opened + jnp.sum(seen, axis=0, keepdims=True)
        allowed = jnp.logical_or(jnp.broadcast_to(opened, diagonal.shape) > 0.5, diagonal)
        cut = jnp.logical_and(var == cores - 1, w == windows - 1)
        bias = jnp.where(allowed, 0.0, -1e30) + differs[...] * jnp.where(cut, 1.0, 0.0)
        attended = jnp.zeros((tokens, features), F32)
        for s in range(cores):
            q = jnp.dot(n1, qkv[s, 0], preferred_element_type=F32).astype(BF16)
            q = q * jnp.asarray(HD ** (-0.5), BF16)
            k = jnp.dot(n1, qkv[s, 1], preferred_element_type=F32).astype(BF16)
            v = jnp.dot(n1, qkv[s, 2], preferred_element_type=F32).astype(BF16)
            tail = jnp.zeros((KEYS - tokens, width), BF16)
            k = jnp.concatenate([k, tail], axis=0)
            v = jnp.concatenate([v, tail], axis=0)
            q_all = jnp.concatenate(
                [jnp.where(lane_head == h, q, jnp.zeros_like(q)) for h in range(heads)], axis=0
            )
            scores = lax.dot_general(q_all, k, NT, preferred_element_type=F32)
            weights = []
            for h in range(heads):
                one = scores[h * tokens : (h + 1) * tokens] + bias
                peak = jnp.max(one, axis=-1, keepdims=True)
                e = jnp.exp(one - peak)
                total = jnp.sum(e, axis=-1, keepdims=True)
                weights.append((e * (1.0 / total)).astype(BF16))
            weights = jnp.concatenate(weights, axis=1)
            v_all = jnp.concatenate(
                [jnp.where(lane_head_keys == h, v, jnp.zeros_like(v)) for h in range(heads)], axis=0
            )
            context = jnp.dot(weights, v_all, preferred_element_type=F32).astype(BF16)
            attended = attended + jnp.dot(context, proj[s], preferred_element_type=F32)
        x_one = x + attended
        n2 = layer_norm(x_one).astype(BF16)
        units = up.shape[2]
        for s in range(cores):
            for c in range(0, units, CHUNK):
                one = jnp.dot(n2, up[s, :, c : c + CHUNK], preferred_element_type=F32)
                one = 0.5 * one * (1.0 + lax.erf(one * 2.0 ** (-0.5)))
                hid[:, s * units + c : s * units + c + CHUNK] = one.astype(BF16)
        latent = x_one + jnp.dot(
            hid[...], down[...].reshape(cores * units, features), preferred_element_type=F32
        )
        n3 = layer_norm(latent.astype(BF16).astype(F32)).astype(BF16)
        n3 = jnp.dot(order[...], n3, preferred_element_type=F32).astype(BF16)

        lane = lax.broadcasted_iota(jnp.int32, (1, BLOCK), 1)

        def by_level(value):
            low, high = value[:, :BLOCK], value[:, BLOCK:]
            found = []
            for level in range(levels):
                start = level * patches
                if start < BLOCK:
                    part = low if start == 0 else pltpu.roll(low, BLOCK - start, 1)
                    if start + patches > BLOCK:
                        part = jnp.where(lane < BLOCK - start, part, pltpu.roll(high, BLOCK - start, 1))
                else:
                    part = pltpu.roll(high, 2 * BLOCK - start, 1) if start > BLOCK else high
                found.append(part)
            return found

        base = jnp.zeros((pixels, BLOCK), F32)
        for s in range(cores):
            g = lax.dot_general(fold[s, 0 : 2 * count, :], n3, NT, preferred_element_type=F32)
            scores = by_level(g[:count] + g[count:])
            peak = functools.reduce(jnp.maximum, scores)
            e = [jnp.exp(one - peak) for one in scores]
            inverse = 1.0 / sum(e)
            for j in range(1, levels):
                dw[j - 1, s * count : (s + 1) * count, :] = e[j] * inverse
            u = by_level(
                lax.dot_general(fold[s, 2 * count :, :], n3, NT, preferred_element_type=F32)
            )
            for h in range(heads):
                base = base + u[0][h * pixels : (h + 1) * pixels]
            for j in range(1, levels):
                du[j - 1, s * heads * pixels : (s + 1) * heads * pixels, :] = u[j] - u[0]
        base_pix[...] = base

        @pl.loop(0, geo.slots // pair)
        def _(at):
            totals = [base_pix[...] for _ in range(pair)]
            for s in range(cores):
                for j in range(levels - 1):
                    start = pl.multiple_of(s * count + at * 8, 8)
                    some = dw[j, pl.ds(start, 8), :]
                    for h in range(heads):
                        top = (s * heads + h) * pixels
                        value = du[j, top : top + pixels, :]
                        for n in range(pair):
                            totals[n] = totals[n] + some[n * heads + h : n * heads + h + 1] * value
            for n in range(pair):
                pix[at * pair + n] = totals[n]

        lane = lax.broadcasted_iota(jnp.int32, (2 * row_size, BLOCK), 1)
        for core in range(cores):
            total = jnp.zeros((rows, 3 * BLOCK), F32)
            for b in range(SQUARE_SPAN):
                top = (core * SQUARE_SPAN + b) * row_size
                part = pix[:, top : top + row_size, :].reshape(rows, BLOCK)
                total = total + jnp.dot(part.astype(BF16), pick[b], preferred_element_type=F32)
            for ih in range(2):
                left = jnp.zeros((2 * row_size, BLOCK), F32)
                for k in range(geo.slots // 2):
                    at = slice(2 * row_size * k, 2 * row_size * (k + 1))
                    moved = pltpu.roll(
                        total[at, 2 * BLOCK :], (extra * k - (BLOCK // 2) * ih) % BLOCK, 1
                    )
                    inside = jnp.logical_and(lane >= extra * k, lane < extra * (k + 1))
                    left = jnp.where(inside, moved, left)
                main = total[:, ih * BLOCK : (ih + 1) * BLOCK]
                pieces[w, ih, core] = jnp.concatenate([main, left], axis=0).astype(BF16)
        if geo.scatter:
            checked[...] = pieces[w].astype(F32).max(axis=(0, 1))
            for ih in range(2):
                for core in range(cores):
                    piece_copy(w, ih, core, "start")

    for copy in halos:
        copy.wait_send()
    if geo.scatter:

        @pl.loop(0, bands)
        def _(s):
            for ih in range(2):
                target = out_ref.at[s, ih]
                pltpu.make_async_copy(target, target, piece_recv.at[s, ih]).wait()

        @pl.loop(0, windows)
        def _(w):
            for ih in range(2):
                for core in range(cores):
                    piece_copy(w, ih, core, "finish")

    else:
        copy = pltpu.make_async_copy(pieces, out_ref, load_sem.at[0])
        copy.start()
        copy.wait()


def forecast(geo, *args):
    tables = (
        jnp.asarray(geo.gather_table(), BF16),
        jnp.asarray(geo.order_table(), BF16),
        jnp.asarray(geo.position_table(), jnp.int32),
        jnp.asarray(geo.pixel_table(), BF16),
        jnp.asarray(geo.pick_table(), BF16),
    )
    features, width, cores, windows = geo.features, geo.width, geo.cores, geo.windows
    units = args[4].shape[1]
    fold_rows = geo.heads * (2 * LEVEL_SLOTS + geo.pixels)
    vmem = pltpu.VMEM
    dma = pltpu.SemaphoreType.DMA
    if geo.scatter:
        out_shape = (geo.bands, 2, BLOCK, BLOCK)
    else:
        out_shape = (windows, 2, cores, BLOCK, BLOCK)
    return pl.pallas_call(
        functools.partial(main_kernel, geo),
        out_shape=jax.ShapeDtypeStruct(out_shape, BF16),
        in_specs=[pl.BlockSpec(memory_space=pltpu.HBM)] * (len(args) + len(tables)),
        out_specs=pl.BlockSpec(memory_space=vmem if geo.scatter else pltpu.HBM),
        scratch_shapes=[
            vmem((geo.cols, geo.levels, geo.taken, features), BF16),
            vmem((2, geo.cols, geo.rows), jnp.int32),
            vmem((cores, 3, features, width), BF16),
            vmem((cores, width, features), BF16),
            vmem((cores, features, units), BF16),
            vmem((cores, units, features), BF16),
            *[vmem(one.shape, one.dtype) for one in args[6:]],
            *[vmem(one.shape, one.dtype) for one in tables],
            vmem((cores, fold_rows, features), BF16),
            vmem((windows, geo.half, features), BF16),
            vmem((windows, geo.half, features), BF16),
            vmem((windows, geo.half, features), BF16),
            vmem((geo.tokens, KEYS), F32),
            vmem((geo.tokens, cores * units), BF16),
            vmem((geo.levels - 1, cores * geo.heads * LEVEL_SLOTS, BLOCK), F32),
            vmem((geo.levels - 1, cores * geo.heads * geo.pixels, BLOCK), F32),
            vmem((geo.pixels, BLOCK), F32),
            vmem((geo.slots, geo.pixels, BLOCK), F32),
            vmem((windows, 2, cores, BLOCK, BLOCK), BF16),
            vmem((BLOCK, BLOCK), F32),
            dma((geo.taken // 8 + 15,)),
            dma((6,)),
            dma((6,)),
            dma((windows,)),
            dma((windows,)),
            dma((windows, 2, cores)),
            dma((geo.bands, 2)),
        ],
        compiler_params=pltpu.CompilerParams(
            collective_id=0, has_side_effects=True, vmem_limit_bytes=60 * 2**20
        ),
    )(*args, *tables)


def assemble_kernel(isobars, run, got_ref, out_ref):
    bands = got_ref.shape[0]
    half_lat = WIN_LAT // 2
    groups = (isobars + 1) // 2
    rows = groups * 16
    whole_run = out_ref.shape[-1]
    tiles = whole_run // BLOCK
    extra = half_lat * run - BLOCK
    lane = lax.broadcasted_iota(jnp.int32, (rows, BLOCK), 1)

    @pl.loop(0, 2)
    def _(ih):
        for r in range(half_lat):
            out = [jnp.zeros((rows, BLOCK), F32) for _ in range(tiles)]
            for s in range(bands):
                base = s * run + run // 2
                piece = got_ref[s, ih].astype(F32)
                whole = min(run, BLOCK - r * run)
                parts = [(pltpu.roll(piece[:rows], (base - r * run) % BLOCK, 1), base, base + whole)]
                if whole < run:
                    rest = piece[rows:]
                    moved = [
                        pltpu.roll(rest, (base + whole - extra * k) % BLOCK, 1) for k in range(groups)
                    ]
                    parts.append((jnp.concatenate(moved, axis=0), base + whole, base + run))
                for value, low, high in parts:
                    spans = [(low, min(high, whole_run)), (max(low, whole_run) - whole_run, high - whole_run)]
                    for low, high in spans:
                        if high <= low:
                            continue
                        for t in range(low // BLOCK, (high - 1) // BLOCK + 1):
                            at = lane + t * BLOCK
                            out[t] = jnp.where(jnp.logical_and(at >= low, at < high), value, out[t])
            for t in range(tiles):
                value = out[t].reshape(2 * groups, 8, BLOCK)[:isobars]
                for flag in range(2):
                    top = ((half_lat if flag == 0 else 0) + r) * SQUARE_SPAN

                    @pl.when(ih == flag)
                    def _():
                        for v in range(2):
                            out_ref[v, :, top : top + SQUARE_SPAN, t * BLOCK : (t + 1) * BLOCK] = value[
                                :, v * SQUARE_SPAN : (v + 1) * SQUARE_SPAN
                            ]


def assemble(got, columns, isobars):
    bands = got.shape[0]
    run = columns * SQUARE_SPAN
    shape = (TARGET_QUANTITY // 2, isobars, WIN_LAT * SQUARE_SPAN, bands * run)
    return pl.pallas_call(
        functools.partial(assemble_kernel, isobars, run),
        out_shape=jax.ShapeDtypeStruct(shape, F32),
        compiler_params=pltpu.CompilerParams(vmem_limit_bytes=40 * 2**20),
    )(got)


def exchange(pieces, geo):
    half_lat = WIN_LAT // 2
    run = geo.cols * SQUARE_SPAN
    quantities = TARGET_QUANTITY // geo.cores
    rows = geo.slots * quantities * SQUARE_SPAN
    extra = half_lat * run - BLOCK
    lead = pieces.shape[:3]
    main = pieces[:, :, :, :rows].reshape(*lead, geo.slots, quantities, SQUARE_SPAN, BLOCK)
    rest = pieces[:, :, :, rows:, : extra * (geo.slots // 2)]
    rest = rest.reshape(*lead, 2, quantities, SQUARE_SPAN, geo.slots // 2, extra)
    rest = jnp.moveaxis(rest, 6, 3).reshape(*lead, geo.slots, quantities, SQUARE_SPAN, extra)
    maps = jnp.concatenate([main, rest], axis=-1)[:, :, :, : geo.isobars]
    maps = maps.reshape(*lead, geo.isobars, quantities, SQUARE_SPAN, half_lat, run)
    maps = jnp.transpose(maps, (2, 4, 3, 0, 1, 6, 5, 7))
    maps = maps.reshape(TARGET_QUANTITY, geo.isobars, geo.row_count * SQUARE_SPAN, run)
    maps = lax.all_to_all(maps, "var", split_axis=0, concat_axis=2, tiled=True)
    maps = jnp.roll(maps, half_lat * SQUARE_SPAN, 2)
    maps = lax.all_to_all(maps, "grid", split_axis=2, concat_axis=3, tiled=True)
    return jnp.roll(maps, run // 2, 3).astype(F32)


def local(
    tokens,
    key_mask,
    w_qkv,
    w_proj,
    w_up,
    w_down,
    level_query,
    w_dec_q,
    w_dec_kv,
    w_dec_o,
    decode_matrix,
):
    geo = Geometry(
        tokens, w_proj, level_query, decode_matrix, lax.axis_size("var"), lax.axis_size("grid")
    )
    pieces = forecast(
        geo,
        jnp.transpose(tokens, (1, 2, 0, 3)),
        key_mask.T,
        w_qkv,
        w_proj,
        w_up,
        w_down,
        level_query,
        w_dec_q,
        w_dec_kv,
        w_dec_o,
        decode_matrix.T,
    )
    if geo.scatter:
        return assemble(pieces, geo.cols, geo.isobars)
    return exchange(pieces, geo)


def solution(mesh):
    placed = (
        P("group", "grid", None, None),
        P("group", "grid"),
        P(None, None, "var"),
        P("var", None),
        P(None, "var"),
        P("var", None),
        P(),
        P(None, "var"),
        P(None, None, "var"),
        P("var", None),
        P(),
    )
    return jax.shard_map(
        local,
        mesh=mesh,
        in_specs=placed,
        out_specs=P("var", "group", "grid", None),
        check_vma=False,
    )
```

```python
import functools

import jax
import jax.numpy as jnp
import numpy as np
from jax import lax
from jax.experimental import pallas as pl
from jax.experimental.pallas import tpu as pltpu
from jax.sharding import PartitionSpec as P

HD = 64
TARGET_QUANTITY = 4
SQUARE_SPAN = 4
WIN_LAT = 6
EPSILON = 1e-05
BLOCK = 128
KEYS = 256
CHUNK = 256
LEVEL_SLOTS = 16
MESH = pl.DeviceIdType.MESH
NT = (((1,), (1,)), ((), ()))
F32 = jnp.float32
BF16 = jnp.bfloat16


def layer_norm(values):
    center = values - jnp.mean(values, axis=-1, keepdims=True)
    spread = jnp.mean(center * center, axis=-1, keepdims=True)
    return center * lax.rsqrt(spread + EPSILON)


class Geometry:
    def __init__(self, tokens, w_proj, level_query, decode_matrix, cores, bands):
        self.rows, self.cols, self.levels, self.features = tokens.shape
        self.cores, self.bands = cores, bands
        self.half_cols = self.cols // 2
        self.row_count = self.rows // cores
        self.windows = self.row_count // WIN_LAT
        self.taken = 8 * (-(-(self.row_count + WIN_LAT // 2) // 8))
        self.half_patches = WIN_LAT * self.half_cols
        self.half = 16 * (-(-(self.levels * self.half_patches) // 16))
        self.tokens = 2 * self.half
        self.patches = 2 * self.half_patches
        self.width = w_proj.shape[0]
        self.heads = self.width // HD
        self.isobars = level_query.shape[0]
        self.slots = self.isobars + self.isobars % 2
        self.pixels = decode_matrix.shape[1]
        self.scatter = bands * WIN_LAT == self.rows and (bands * self.cols * SQUARE_SPAN) % BLOCK == 0

    def place(self, half, level, r, c):
        return half * self.half + level * self.half_patches + r * self.half_cols + c

    def each(self):
        for half in range(2):
            for level in range(self.levels):
                for r in range(WIN_LAT):
                    for c in range(self.half_cols):
                        yield half, level, r, c

    def gather_table(self):
        table = np.zeros((self.windows, self.half, self.half_cols * self.levels * self.taken), np.float32)
        for w in range(self.windows):
            for half, level, r, c in self.each():
                if half == 0:
                    source = (c * self.levels + level) * self.taken + WIN_LAT * w + WIN_LAT // 2 + r
                    table[w, self.place(0, level, r, c), source] = 1.0
        return table.reshape(self.windows * self.half, -1)

    def order_table(self):
        table = np.zeros((self.levels * BLOCK, self.tokens), np.float32)
        for half, level, r, c in self.each():
            patch = r * self.cols + half * self.half_cols + c
            table[level * BLOCK + patch, self.place(half, level, r, c)] = 1.0
            if level > 0:
                table[level * BLOCK + patch, self.place(half, 0, r, c)] = -1.0
        return table

    def position_table(self):
        table = np.full((8, KEYS), -1, np.int32)
        table[0] = 0
        for half, level, r, c in self.each():
            at = self.place(half, level, r, c)
            table[0, at] = r
            table[1 + half, at] = c + (self.half_cols if half == 0 else 0)
        return table

    def pixel_table(self):
        table = np.zeros((self.pixels, self.pixels), np.float32)
        own = TARGET_QUANTITY // self.cores
        for v in range(TARGET_QUANTITY):
            for a in range(SQUARE_SPAN):
                for b in range(SQUARE_SPAN):
                    target = ((v // own * SQUARE_SPAN + b) * own + v % own) * SQUARE_SPAN + a
                    table[target, (v * SQUARE_SPAN + a) * SQUARE_SPAN + b] = 1.0
        return table

    def pick_table(self):
        half_lat = WIN_LAT // 2
        run = self.cols * SQUARE_SPAN
        extra = half_lat * run - BLOCK
        picks = np.zeros((SQUARE_SPAN, BLOCK, 4 * BLOCK), np.float32)
        for ih in range(2):
            for q in range(half_lat * run):
                r, rest = divmod(q, run)
                column, b = divmod(rest, SQUARE_SPAN)
                source = (half_lat * ih + r) * self.cols + column
                if q < BLOCK:
                    picks[b, source, ih * BLOCK + q] = 1.0
                else:
                    for k in range(self.slots // 2):
                        picks[b, source, (2 + ih) * BLOCK + extra * k + q - BLOCK] = 1.0
        return picks


def fold_decoder(lq, wq, wkv_ref, wo, dm, perm, out_ref):
    width = wq.shape[1]
    heads = width // HD
    dquery = jnp.dot(lq, wq, preferred_element_type=F32) * HD ** (-0.5)
    d_hi = dquery.astype(BF16)
    d_lo = (dquery - d_hi.astype(F32)).astype(BF16)
    count = LEVEL_SLOTS * heads
    row = lax.broadcasted_iota(jnp.int32, (count, dquery.shape[0]), 0)
    slot = lax.broadcasted_iota(jnp.int32, (count, dquery.shape[0]), 1)
    spread = (row // heads == slot).astype(F32).astype(BF16)
    row = lax.broadcasted_iota(jnp.int32, (count, width), 0)
    mine = row % heads == lax.broadcasted_iota(jnp.int32, (count, width), 1) // HD
    q_hi = jnp.dot(spread, d_hi, preferred_element_type=F32)
    q_hi = jnp.where(mine, q_hi, 0.0).astype(BF16)
    q_lo = jnp.dot(spread, d_lo, preferred_element_type=F32)
    q_lo = jnp.where(mine, q_lo, 0.0).astype(BF16)
    wk = wkv_ref[0]
    g = lax.dot_general(q_hi, wk, NT, preferred_element_type=F32)
    g = g + lax.dot_general(q_lo, wk, NT, preferred_element_type=F32)
    g_hi = g.astype(BF16)
    out_ref[0, 0:count, :] = g_hi
    out_ref[0, count : 2 * count, :] = (g - g_hi.astype(F32)).astype(BF16)
    dm_hi = dm.astype(BF16)
    dm_lo = (dm - dm_hi.astype(F32)).astype(BF16)
    dm_hi = jnp.dot(perm, dm_hi, preferred_element_type=F32).astype(BF16)
    dm_lo = jnp.dot(perm, dm_lo, preferred_element_type=F32).astype(BF16)
    m_t = lax.dot_general(dm_hi, wo, NT, preferred_element_type=F32)
    m_t = m_t + lax.dot_general(dm_lo, wo, NT, preferred_element_type=F32)
    pixels = m_t.shape[0]
    stacked = jnp.concatenate([m_t] * heads, axis=0)
    row_head = lax.broadcasted_iota(jnp.int32, stacked.shape, 0) // pixels
    lane_head = lax.broadcasted_iota(jnp.int32, stacked.shape, 1) // HD
    stacked = jnp.where(row_head == lane_head, stacked, 0.0)
    s_hi = stacked.astype(BF16)
    s_lo = (stacked - s_hi.astype(F32)).astype(BF16)
    wv = wkv_ref[1]
    n_t = lax.dot_general(s_hi, wv, NT, preferred_element_type=F32)
    n_t = n_t + lax.dot_general(s_lo, wv, NT, preferred_element_type=F32)
    out_ref[0, 2 * count :, :] = n_t.astype(BF16)


def main_kernel(
    geo,
    tok_ref,
    mask_ref,
    wqkv_ref,
    wproj_ref,
    wup_ref,
    wdown_ref,
    lq_ref,
    wq_ref,
    wkv_ref,
    wo_ref,
    dm_ref,
    gather_ref,
    order_ref,
    position_ref,
    perm_ref,
    pick_ref,
    out_ref,
    raw,
    marks,
    qkv,
    proj,
    up,
    down,
    lq,
    wq,
    wkv,
    wo,
    dm,
    gather,
    order,
    position,
    perm,
    pick,
    fold,
    first,
    own,
    halo,
    differs,
    hid,
    dw,
    du,
    fold_base,
    x_one,
    pix,
    pieces,
    checked,
    load_sem,
    weight_send,
    weight_recv,
    halo_send,
    halo_recv,
    piece_send,
    piece_recv,
):
    group, grid, var = (lax.axis_index(name) for name in ("group", "grid", "var"))
    bands, cores, windows, half = geo.bands, geo.cores, geo.windows, geo.half
    features, levels, width, heads = geo.features, geo.levels, geo.width, geo.heads
    sibling = (group, grid, lax.rem(var + 1, cores))
    west = (group, lax.rem(grid + bands - 1, bands), var)
    east = (group, lax.rem(grid + 1, bands), var)
    barrier = pltpu.get_barrier_semaphore()
    if geo.scatter:
        peers = bands * cores
        me = grid * cores + var

        @pl.loop(1, peers)
        def _(step):
            peer = lax.rem(me + step, peers)
            pl.semaphore_signal(
                barrier, inc=1, device_id=(group, peer // cores, lax.rem(peer, cores)), device_id_type=MESH
            )

        greeted = peers - 1
    else:
        for peer in (sibling, west, east):
            pl.semaphore_signal(barrier, inc=1, device_id=peer, device_id_type=MESH)
        greeted = 3

    loads = []

    def load(source, target):
        copy = pltpu.make_async_copy(source, target, load_sem.at[len(loads)])
        copy.start()
        loads.append(copy)
        return copy

    tiles = geo.rows // 8
    first_tile = var * (geo.row_count // 8)
    slabs = []
    for s in range(geo.taken // 8):
        tile = lax.rem(first_tile + s, tiles)
        slabs.append(
            load(tok_ref.at[:, :, pl.ds(pl.multiple_of(tile * 8, 8), 8), :], raw.at[:, :, 8 * s : 8 * s + 8, :])
        )
    gather_load = load(gather_ref, gather)
    fold_loads = [
        load(a, b)
        for a, b in ((lq_ref, lq), (wq_ref, wq), (wkv_ref, wkv), (wo_ref, wo), (dm_ref, dm), (perm_ref, perm))
    ]
    late_loads = [
        load(a, b)
        for a, b in (
            (mask_ref, marks.at[0]),
            (wqkv_ref, qkv.at[0]),
            (wproj_ref, proj.at[0]),
            (wup_ref, up.at[0]),
            (wdown_ref, down.at[0]),
            (position_ref, position),
            (order_ref, order),
            (pick_ref, pick),
        )
    ]

    for copy in slabs:
        copy.wait()
    gather_load.wait()
    depth = geo.half_cols * levels * geo.taken
    for h, target in ((0, first), (1, own)):
        slab = raw[h * geo.half_cols : (h + 1) * geo.half_cols].reshape(depth, features)
        for c in range(0, features, CHUNK):
            rows = jnp.dot(gather[...], slab[:, c : c + CHUNK], preferred_element_type=F32).astype(BF16)
            target[:, :, c : c + CHUNK] = rows.reshape(windows, half, CHUNK)

    pl.semaphore_wait(barrier, greeted)

    def remote(source, target, send, recv, peer):
        copy = pltpu.make_async_remote_copy(
            src_ref=source, dst_ref=target, send_sem=send, recv_sem=recv, device_id=peer, device_id_type=MESH
        )
        copy.start()
        return copy

    copies = [remote(mask_ref, marks.at[1], weight_send.at[0], weight_recv.at[0], west)]
    halos = []
    for w in range(windows):
        halos.append(remote(first.at[w], halo.at[w], halo_send.at[w], halo_recv.at[w], west))
    for n, (source, target) in enumerate(((wqkv_ref, qkv), (wproj_ref, proj), (wup_ref, up), (wdown_ref, down))):
        copies.append(remote(source, target.at[1], weight_send.at[n + 1], weight_recv.at[n + 1], sibling))

    for copy in fold_loads:
        copy.wait()
    fold_decoder(lq[...], wq[...], wkv, wo[...], dm[...], perm[...], fold)

    tokens = geo.tokens
    q_pos = lax.broadcasted_iota(jnp.int32, (tokens, KEYS), 0)
    k_pos = lax.broadcasted_iota(jnp.int32, (tokens, KEYS), 1)
    diagonal = q_pos == k_pos

    def region_of(pos):
        pos = jnp.where(pos >= half, pos - half, pos)
        for level in range(levels - 1, 0, -1):
            start = geo.half_patches * level
            pos = jnp.where(pos >= start, pos - start, pos)
        return pos >= geo.half_patches // 2

    differs[...] = jnp.where(region_of(q_pos) != region_of(k_pos), -1e30, 0.0)
    lane_head = lax.broadcasted_iota(jnp.int32, (tokens, width), 1) // HD
    lane_head_keys = lax.broadcasted_iota(jnp.int32, (KEYS, width), 1) // HD

    for copy in late_loads:
        copy.wait()
    copies.append(remote(fold.at[0], fold.at[1], weight_send.at[5], weight_recv.at[5], sibling))

    count = heads * LEVEL_SLOTS
    pixels = geo.pixels
    row_size = pixels // cores // SQUARE_SPAN
    rows = geo.slots * row_size
    half_lat = WIN_LAT // 2
    extra = half_lat * geo.cols * SQUARE_SPAN - BLOCK
    pair = 8 // heads
    units = up.shape[2]

    def piece_copy(w, ih, core, action):
        band = lax.rem(var * windows + w + ih, bands)
        here = jnp.logical_and(band == grid, core == var)
        source, target = pieces.at[w, ih, core], out_ref.at[grid, ih]

        @pl.when(here)
        def _():
            if action == "start":
                pltpu.make_async_copy(source, target, piece_recv.at[grid, ih]).start()

        @pl.when(jnp.logical_not(here))
        def _():
            if action == "start":
                pltpu.make_async_remote_copy(
                    src_ref=source,
                    dst_ref=target,
                    send_sem=piece_send.at[w, ih, core],
                    recv_sem=piece_recv.at[grid, ih],
                    device_id=(group, band, core),
                    device_id_type=MESH,
                ).start()
            else:
                pltpu.make_async_copy(source, source, piece_send.at[w, ih, core]).wait()

    def arrive(w):
        pltpu.make_async_copy(halo.at[w], halo.at[w], halo_recv.at[w]).wait()

    def send(w):
        if geo.scatter:
            for ih in range(2):
                for core in range(cores):
                    piece_copy(w, ih, core, "start")

    def attend(w):
        x = jnp.concatenate([own[w], halo[w]], axis=0).astype(F32)
        n1 = layer_norm(x).astype(BF16)
        target = position[0:1, :] + (var * geo.row_count + WIN_LAT * w + half_lat)
        target = jnp.where(target >= geo.rows, target - geo.rows, target)
        there = lax.broadcasted_iota(jnp.int32, (geo.rows, KEYS), 0) == target
        there = there.astype(F32).astype(BF16)
        opened = jnp.zeros((1, KEYS), F32)
        column = lax.broadcasted_iota(jnp.int32, (geo.cols, KEYS), 0)
        for h in range(2):
            seen = (marks[h] > 0).astype(F32).astype(BF16)
            seen = jnp.dot(seen, there, preferred_element_type=F32)
            seen = jnp.where(column == position[1 + h : 2 + h, :], seen, 0.0)
            opened = opened + jnp.sum(seen, axis=0, keepdims=True)
        allowed = jnp.logical_or(jnp.broadcast_to(opened, diagonal.shape) > 0.5, diagonal)
        cut = jnp.logical_and(var == cores - 1, w == windows - 1)
        bias = jnp.where(allowed, 0.0, -1e30) + differs[...] * jnp.where(cut, 1.0, 0.0)
        attended = x
        for s in range(cores):
            q = jnp.dot(n1, qkv[s, 0], preferred_element_type=F32).astype(BF16)
            q = q * jnp.asarray(HD ** (-0.5), BF16)
            k = jnp.dot(n1, qkv[s, 1], preferred_element_type=F32).astype(BF16)
            v = jnp.dot(n1, qkv[s, 2], preferred_element_type=F32).astype(BF16)
            tail = jnp.zeros((KEYS - tokens, width), BF16)
            k = jnp.concatenate([k, tail], axis=0)
            v = jnp.concatenate([v, tail], axis=0)
            q_all = jnp.concatenate(
                [jnp.where(lane_head == h, q, jnp.zeros_like(q)) for h in range(heads)], axis=0
            )
            scores = lax.dot_general(q_all, k, NT, preferred_element_type=F32)
            weights = []
            for h in range(heads):
                one = scores[h * tokens : (h + 1) * tokens] + bias
                peak = jnp.max(one, axis=-1, keepdims=True)
                e = jnp.exp(one - peak)
                total = jnp.sum(e, axis=-1, keepdims=True)
                weights.append((e * (1.0 / total)).astype(BF16))
            weights = jnp.concatenate(weights, axis=1)
            v_all = jnp.concatenate(
                [jnp.where(lane_head_keys == h, v, jnp.zeros_like(v)) for h in range(heads)], axis=0
            )
            context = jnp.dot(weights, v_all, preferred_element_type=F32).astype(BF16)
            attended = attended + jnp.dot(context, proj[s], preferred_element_type=F32)
        x_one[w] = attended

    def finish(w):
        n2 = layer_norm(x_one[w]).astype(BF16)
        for s in range(cores):
            for c in range(0, units, CHUNK):
                one = jnp.dot(n2, up[s, :, c : c + CHUNK], preferred_element_type=F32)
                one = 0.5 * one * (1.0 + lax.erf(one * 2.0 ** (-0.5)))
                hid[:, s * units + c : s * units + c + CHUNK] = one.astype(BF16)
        latent = x_one[w] + jnp.dot(
            hid[...], down[...].reshape(cores * units, features), preferred_element_type=F32
        )
        n3 = layer_norm(latent.astype(BF16).astype(F32)).astype(BF16)
        n3 = jnp.dot(order[...], n3, preferred_element_type=F32).astype(BF16)
        n3, others = n3[:BLOCK], n3[BLOCK:]
        base = lax.dot_general(fold_base[...], n3, NT, preferred_element_type=F32)
        base = base[:pixels] + base[pixels:]
        for s in range(cores):
            g = lax.dot_general(fold[s, 0 : 2 * count, :], others, NT, preferred_element_type=F32)
            g = g[:count] + g[count:]
            scores = [jnp.zeros((count, BLOCK), F32)]
            scores += [g[:, j * BLOCK : (j + 1) * BLOCK] for j in range(levels - 1)]
            peak = functools.reduce(jnp.maximum, scores)
            e = [jnp.exp(one - peak) for one in scores]
            inverse = 1.0 / sum(e)
            u = lax.dot_general(fold[s, 2 * count :, :], others, NT, preferred_element_type=F32)
            for j in range(levels - 1):
                dw[j, s * count : (s + 1) * count, :] = e[j + 1] * inverse
                du[j, s * heads * pixels : (s + 1) * heads * pixels, :] = u[:, j * BLOCK : (j + 1) * BLOCK]
        for at in range(geo.slots // pair):
            totals = [base for _ in range(pair)]
            for s in range(cores):
                for j in range(levels - 1):
                    some = dw[j, s * count + at * 8 : s * count + at * 8 + 8, :]
                    for h in range(heads):
                        top = (s * heads + h) * pixels
                        value = du[j, top : top + pixels, :]
                        for n in range(pair):
                            totals[n] = totals[n] + some[n * heads + h : n * heads + h + 1] * value
            for n in range(pair):
                pix[at * pair + n] = totals[n]
        lane = lax.broadcasted_iota(jnp.int32, (2 * row_size, BLOCK), 1)
        for core in range(cores):
            total = jnp.zeros((rows, 4 * BLOCK), F32)
            for b in range(SQUARE_SPAN):
                top = (core * SQUARE_SPAN + b) * row_size
                part = pix[:, top : top + row_size, :].reshape(rows, BLOCK)
                total = total + jnp.dot(part.astype(BF16), pick[b], preferred_element_type=F32)
            for ih in range(2):
                left = jnp.zeros((2 * row_size, BLOCK), F32)
                for k in range(geo.slots // 2):
                    at = slice(2 * row_size * k, 2 * row_size * (k + 1))
                    inside = jnp.logical_and(lane >= extra * k, lane < extra * (k + 1))
                    left = jnp.where(inside, total[at, (2 + ih) * BLOCK : (3 + ih) * BLOCK], left)
                main = total[:, ih * BLOCK : (ih + 1) * BLOCK]
                pieces[w, ih, core] = jnp.concatenate([main, left], axis=0).astype(BF16)
        checked[...] = pieces[w].astype(F32).max(axis=(0, 1))

    mask_copy, qkv_copy, proj_copy, up_copy, down_copy, fold_copy = copies
    for copy in (mask_copy, qkv_copy, proj_copy):
        copy.wait()
    arrive(0)
    attend(0)
    for copy in (up_copy, down_copy, fold_copy):
        copy.wait()
    whole = jnp.zeros((pixels, features), F32)
    for s in range(cores):
        for h in range(heads):
            top = 2 * count + h * pixels
            whole = whole + fold[s, top : top + pixels, :].astype(F32)
    whole_hi = whole.astype(BF16)
    fold_base[0:pixels, :] = whole_hi
    fold_base[pixels:, :] = (whole - whole_hi.astype(F32)).astype(BF16)

    @pl.loop(0, windows - 1)
    def _(w):
        arrive(w + 1)
        finish(w)
        attend(w + 1)
        send(w)

    finish(windows - 1)
    send(windows - 1)

    for copy in halos:
        copy.wait_send()
    if geo.scatter:

        @pl.loop(0, bands)
        def _(s):
            for ih in range(2):
                target = out_ref.at[s, ih]
                pltpu.make_async_copy(target, target, piece_recv.at[s, ih]).wait()

        @pl.loop(0, windows)
        def _(w):
            for ih in range(2):
                for core in range(cores):
                    piece_copy(w, ih, core, "finish")

    else:
        copy = pltpu.make_async_copy(pieces, out_ref, load_sem.at[0])
        copy.start()
        copy.wait()


def forecast(geo, *args):
    tables = (
        jnp.asarray(geo.gather_table(), BF16),
        jnp.asarray(geo.order_table(), BF16),
        jnp.asarray(geo.position_table(), jnp.int32),
        jnp.asarray(geo.pixel_table(), BF16),
        jnp.asarray(geo.pick_table(), BF16),
    )
    features, width, cores, windows = geo.features, geo.width, geo.cores, geo.windows
    units = args[4].shape[1]
    fold_rows = geo.heads * (2 * LEVEL_SLOTS + geo.pixels)
    vmem = pltpu.VMEM
    dma = pltpu.SemaphoreType.DMA
    if geo.scatter:
        out_shape = (geo.bands, 2, BLOCK, BLOCK)
    else:
        out_shape = (windows, 2, cores, BLOCK, BLOCK)
    return pl.pallas_call(
        functools.partial(main_kernel, geo),
        out_shape=jax.ShapeDtypeStruct(out_shape, BF16),
        in_specs=[pl.BlockSpec(memory_space=pltpu.HBM)] * (len(args) + len(tables)),
        out_specs=pl.BlockSpec(memory_space=vmem if geo.scatter else pltpu.HBM),
        scratch_shapes=[
            vmem((geo.cols, geo.levels, geo.taken, features), BF16),
            vmem((2, geo.cols, geo.rows), jnp.int32),
            vmem((cores, 3, features, width), BF16),
            vmem((cores, width, features), BF16),
            vmem((cores, features, units), BF16),
            vmem((cores, units, features), BF16),
            *[vmem(one.shape, one.dtype) for one in args[6:]],
            *[vmem(one.shape, one.dtype) for one in tables],
            vmem((cores, fold_rows, features), BF16),
            vmem((windows, geo.half, features), BF16),
            vmem((windows, geo.half, features), BF16),
            vmem((windows, geo.half, features), BF16),
            vmem((geo.tokens, KEYS), F32),
            vmem((geo.tokens, cores * units), BF16),
            vmem((geo.levels - 1, cores * geo.heads * LEVEL_SLOTS, BLOCK), F32),
            vmem((geo.levels - 1, cores * geo.heads * geo.pixels, BLOCK), F32),
            vmem((2 * geo.pixels, features), BF16),
            vmem((windows, geo.tokens, features), F32),
            vmem((geo.slots, geo.pixels, BLOCK), F32),
            vmem((windows, 2, cores, BLOCK, BLOCK), BF16),
            vmem((BLOCK, BLOCK), F32),
            dma((geo.taken // 8 + 15,)),
            dma((6,)),
            dma((6,)),
            dma((windows,)),
            dma((windows,)),
            dma((windows, 2, cores)),
            dma((geo.bands, 2)),
        ],
        compiler_params=pltpu.CompilerParams(
            collective_id=0, has_side_effects=True, vmem_limit_bytes=60 * 2**20
        ),
    )(*args, *tables)


def assemble_kernel(isobars, run, got_ref, out_ref):
    bands = got_ref.shape[0]
    half_lat = WIN_LAT // 2
    groups = (isobars + 1) // 2
    rows = groups * 16
    whole_run = out_ref.shape[-1]
    tiles = whole_run // BLOCK
    extra = half_lat * run - BLOCK
    lane = lax.broadcasted_iota(jnp.int32, (rows, BLOCK), 1)

    @pl.loop(0, 2)
    def _(ih):
        for r in range(half_lat):
            out = [jnp.zeros((rows, BLOCK), F32) for _ in range(tiles)]
            for s in range(bands):
                base = s * run + run // 2
                piece = got_ref[s, ih].astype(F32)
                whole = min(run, BLOCK - r * run)
                parts = [(pltpu.roll(piece[:rows], (base - r * run) % BLOCK, 1), base, base + whole)]
                if whole < run:
                    rest = piece[rows:]
                    moved = [
                        pltpu.roll(rest, (base + whole - extra * k) % BLOCK, 1) for k in range(groups)
                    ]
                    parts.append((jnp.concatenate(moved, axis=0), base + whole, base + run))
                for value, low, high in parts:
                    spans = [(low, min(high, whole_run)), (max(low, whole_run) - whole_run, high - whole_run)]
                    for low, high in spans:
                        if high <= low:
                            continue
                        for t in range(low // BLOCK, (high - 1) // BLOCK + 1):
                            at = lane + t * BLOCK
                            out[t] = jnp.where(jnp.logical_and(at >= low, at < high), value, out[t])
            for t in range(tiles):
                value = out[t].reshape(2 * groups, 8, BLOCK)[:isobars]
                for flag in range(2):
                    top = ((half_lat if flag == 0 else 0) + r) * SQUARE_SPAN

                    @pl.when(ih == flag)
                    def _():
                        for v in range(2):
                            out_ref[v, :, top : top + SQUARE_SPAN, t * BLOCK : (t + 1) * BLOCK] = value[
                                :, v * SQUARE_SPAN : (v + 1) * SQUARE_SPAN
                            ]


def assemble(got, columns, isobars):
    bands = got.shape[0]
    run = columns * SQUARE_SPAN
    shape = (TARGET_QUANTITY // 2, isobars, WIN_LAT * SQUARE_SPAN, bands * run)
    return pl.pallas_call(
        functools.partial(assemble_kernel, isobars, run),
        out_shape=jax.ShapeDtypeStruct(shape, F32),
        compiler_params=pltpu.CompilerParams(vmem_limit_bytes=40 * 2**20),
    )(got)


def exchange(pieces, geo):
    half_lat = WIN_LAT // 2
    run = geo.cols * SQUARE_SPAN
    quantities = TARGET_QUANTITY // geo.cores
    rows = geo.slots * quantities * SQUARE_SPAN
    extra = half_lat * run - BLOCK
    lead = pieces.shape[:3]
    main = pieces[:, :, :, :rows].reshape(*lead, geo.slots, quantities, SQUARE_SPAN, BLOCK)
    rest = pieces[:, :, :, rows:, : extra * (geo.slots // 2)]
    rest = rest.reshape(*lead, 2, quantities, SQUARE_SPAN, geo.slots // 2, extra)
    rest = jnp.moveaxis(rest, 6, 3).reshape(*lead, geo.slots, quantities, SQUARE_SPAN, extra)
    maps = jnp.concatenate([main, rest], axis=-1)[:, :, :, : geo.isobars]
    maps = maps.reshape(*lead, geo.isobars, quantities, SQUARE_SPAN, half_lat, run)
    maps = jnp.transpose(maps, (2, 4, 3, 0, 1, 6, 5, 7))
    maps = maps.reshape(TARGET_QUANTITY, geo.isobars, geo.row_count * SQUARE_SPAN, run)
    maps = lax.all_to_all(maps, "var", split_axis=0, concat_axis=2, tiled=True)
    maps = jnp.roll(maps, half_lat * SQUARE_SPAN, 2)
    maps = lax.all_to_all(maps, "grid", split_axis=2, concat_axis=3, tiled=True)
    return jnp.roll(maps, run // 2, 3).astype(F32)


def local(
    tokens,
    key_mask,
    w_qkv,
    w_proj,
    w_up,
    w_down,
    level_query,
    w_dec_q,
    w_dec_kv,
    w_dec_o,
    decode_matrix,
):
    geo = Geometry(
        tokens, w_proj, level_query, decode_matrix, lax.axis_size("var"), lax.axis_size("grid")
    )
    pieces = forecast(
        geo,
        jnp.transpose(tokens, (1, 2, 0, 3)),
        key_mask.T,
        w_qkv,
        w_proj,
        w_up,
        w_down,
        level_query,
        w_dec_q,
        w_dec_kv,
        w_dec_o,
        decode_matrix.T,
    )
    if geo.scatter:
        return assemble(pieces, geo.cols, geo.isobars)
    return exchange(pieces, geo)


def solution(mesh):
    placed = (
        P("group", "grid", None, None),
        P("group", "grid"),
        P(None, None, "var"),
        P("var", None),
        P(None, "var"),
        P("var", None),
        P(),
        P(None, "var"),
        P(None, None, "var"),
        P("var", None),
        P(),
    )
    return jax.shard_map(
        local,
        mesh=mesh,
        in_specs=placed,
        out_specs=P("var", "group", "grid", None),
        check_vma=False,
    )
```

```python
import functools

import jax
import jax.numpy as jnp
import numpy as np
from jax import lax
from jax.experimental import pallas as pl
from jax.experimental.pallas import tpu as pltpu
from jax.sharding import PartitionSpec as P

HD = 64
TARGET_QUANTITY = 4
SQUARE_SPAN = 4
WIN_LAT = 6
EPSILON = 1e-05
BLOCK = 128
KEYS = 256
CHUNK = 256
LEVEL_SLOTS = 16
ORDER = "abaabbbbaaabbbbabaabbbb"
MESH = pl.DeviceIdType.MESH
NT = (((1,), (1,)), ((), ()))
F32 = jnp.float32
BF16 = jnp.bfloat16


def layer_norm(values):
    center = values - jnp.mean(values, axis=-1, keepdims=True)
    spread = jnp.mean(center * center, axis=-1, keepdims=True)
    return center * lax.rsqrt(spread + EPSILON)


class Geometry:
    def __init__(self, tokens, w_proj, level_query, decode_matrix, cores, bands):
        self.rows, self.cols, self.levels, self.features = tokens.shape
        self.cores, self.bands = cores, bands
        self.half_cols = self.cols // 2
        self.row_count = self.rows // cores
        self.windows = self.row_count // WIN_LAT
        self.taken = 8 * (-(-(self.row_count + WIN_LAT // 2) // 8))
        self.half_patches = WIN_LAT * self.half_cols
        self.half = 16 * (-(-(self.levels * self.half_patches) // 16))
        self.tokens = 2 * self.half
        self.patches = 2 * self.half_patches
        self.width = w_proj.shape[0]
        self.heads = self.width // HD
        self.isobars = level_query.shape[0]
        self.slots = self.isobars + self.isobars % 2
        self.pixels = decode_matrix.shape[1]
        self.scatter = bands * WIN_LAT == self.rows and (bands * self.cols * SQUARE_SPAN) % BLOCK == 0

    def place(self, half, level, r, c):
        return half * self.half + level * self.half_patches + r * self.half_cols + c

    def each(self):
        for half in range(2):
            for level in range(self.levels):
                for r in range(WIN_LAT):
                    for c in range(self.half_cols):
                        yield half, level, r, c

    def gather_table(self):
        table = np.zeros((self.windows, self.half, self.half_cols * self.levels * self.taken), np.float32)
        for w in range(self.windows):
            for half, level, r, c in self.each():
                if half == 0:
                    source = (c * self.levels + level) * self.taken + WIN_LAT * w + WIN_LAT // 2 + r
                    table[w, self.place(0, level, r, c), source] = 1.0
        return table.reshape(self.windows * self.half, -1)

    def order_table(self):
        table = np.zeros((self.levels * BLOCK, self.tokens), np.float32)
        for half, level, r, c in self.each():
            patch = r * self.cols + (1 - half) * self.half_cols + c
            table[level * BLOCK + patch, self.place(half, level, r, c)] = 1.0
            if level > 0:
                table[level * BLOCK + patch, self.place(half, 0, r, c)] = -1.0
        return table

    def position_table(self):
        table = np.full((8, KEYS), -1, np.int32)
        table[0] = 0
        for half, level, r, c in self.each():
            at = self.place(half, level, r, c)
            table[0, at] = r
            table[1 + half, at] = c + half * self.half_cols
        return table

    def pixel_table(self):
        table = np.zeros((self.pixels, self.pixels), np.float32)
        own = TARGET_QUANTITY // self.cores
        for v in range(TARGET_QUANTITY):
            for a in range(SQUARE_SPAN):
                for b in range(SQUARE_SPAN):
                    target = ((v // own * SQUARE_SPAN + b) * own + v % own) * SQUARE_SPAN + a
                    table[target, (v * SQUARE_SPAN + a) * SQUARE_SPAN + b] = 1.0
        return table

    def pick_table(self):
        half_lat = WIN_LAT // 2
        run = self.cols * SQUARE_SPAN
        extra = half_lat * run - BLOCK
        picks = np.zeros((SQUARE_SPAN, BLOCK, 4 * BLOCK), np.float32)
        for ih in range(2):
            for q in range(half_lat * run):
                r, rest = divmod(q, run)
                column, b = divmod(rest, SQUARE_SPAN)
                source = (half_lat * ih + r) * self.cols + column
                if q < BLOCK:
                    picks[b, source, ih * BLOCK + q] = 1.0
                else:
                    for k in range(self.slots // 2):
                        picks[b, source, (2 + ih) * BLOCK + extra * k + q - BLOCK] = 1.0
        return picks


def fold_decoder(lq, wq, wkv_ref, wo, dm, perm, out_ref):
    width = wq.shape[1]
    heads = width // HD
    dquery = jnp.dot(lq, wq, preferred_element_type=F32) * HD ** (-0.5)
    d_hi = dquery.astype(BF16)
    d_lo = (dquery - d_hi.astype(F32)).astype(BF16)
    count = LEVEL_SLOTS * heads
    row = lax.broadcasted_iota(jnp.int32, (count, dquery.shape[0]), 0)
    slot = lax.broadcasted_iota(jnp.int32, (count, dquery.shape[0]), 1)
    spread = (row // heads == slot).astype(F32).astype(BF16)
    row = lax.broadcasted_iota(jnp.int32, (count, width), 0)
    mine = row % heads == lax.broadcasted_iota(jnp.int32, (count, width), 1) // HD
    q_hi = jnp.dot(spread, d_hi, preferred_element_type=F32)
    q_hi = jnp.where(mine, q_hi, 0.0).astype(BF16)
    q_lo = jnp.dot(spread, d_lo, preferred_element_type=F32)
    q_lo = jnp.where(mine, q_lo, 0.0).astype(BF16)
    wk = wkv_ref[0]
    g = lax.dot_general(q_hi, wk, NT, preferred_element_type=F32)
    g = g + lax.dot_general(q_lo, wk, NT, preferred_element_type=F32)
    g_hi = g.astype(BF16)
    out_ref[0, 0:count, :] = g_hi
    out_ref[0, count : 2 * count, :] = (g - g_hi.astype(F32)).astype(BF16)
    dm_hi = dm.astype(BF16)
    dm_lo = (dm - dm_hi.astype(F32)).astype(BF16)
    dm_hi = jnp.dot(perm, dm_hi, preferred_element_type=F32).astype(BF16)
    dm_lo = jnp.dot(perm, dm_lo, preferred_element_type=F32).astype(BF16)
    m_t = lax.dot_general(dm_hi, wo, NT, preferred_element_type=F32)
    m_t = m_t + lax.dot_general(dm_lo, wo, NT, preferred_element_type=F32)
    pixels = m_t.shape[0]
    stacked = jnp.concatenate([m_t] * heads, axis=0)
    row_head = lax.broadcasted_iota(jnp.int32, stacked.shape, 0) // pixels
    lane_head = lax.broadcasted_iota(jnp.int32, stacked.shape, 1) // HD
    stacked = jnp.where(row_head == lane_head, stacked, 0.0)
    s_hi = stacked.astype(BF16)
    s_lo = (stacked - s_hi.astype(F32)).astype(BF16)
    wv = wkv_ref[1]
    n_t = lax.dot_general(s_hi, wv, NT, preferred_element_type=F32)
    n_t = n_t + lax.dot_general(s_lo, wv, NT, preferred_element_type=F32)
    out_ref[0, 2 * count :, :] = n_t.astype(BF16)


def main_kernel(
    geo,
    tok_ref,
    mask_ref,
    wqkv_ref,
    wproj_ref,
    wup_ref,
    wdown_ref,
    lq_ref,
    wq_ref,
    wkv_ref,
    wo_ref,
    dm_ref,
    gather_ref,
    order_ref,
    position_ref,
    perm_ref,
    pick_ref,
    out_ref,
    raw,
    marks,
    qkv,
    proj,
    up,
    down,
    lq,
    wq,
    wkv,
    wo,
    dm,
    gather,
    order,
    position,
    perm,
    pick,
    fold,
    first,
    own,
    halo,
    differs,
    hid,
    dw,
    du,
    fold_base,
    x_one,
    base_pix,
    pix,
    pieces,
    checked,
    load_sem,
    weight_send,
    weight_recv,
    halo_send,
    halo_recv,
    piece_send,
    piece_recv,
):
    group, grid, var = (lax.axis_index(name) for name in ("group", "grid", "var"))
    bands, cores, windows, half = geo.bands, geo.cores, geo.windows, geo.half
    features, levels, width, heads = geo.features, geo.levels, geo.width, geo.heads
    sibling = (group, grid, lax.rem(var + 1, cores))

    def turn(step, column=grid):
        return lax.rem(column + step + 1, windows)

    east_grid = lax.rem(grid + 1, bands)
    west = (group, lax.rem(grid + bands - 1, bands), var)
    east = (group, east_grid, var)
    barrier = pltpu.get_barrier_semaphore()
    if geo.scatter:
        peers = bands * cores
        me = grid * cores + var

        @pl.loop(1, peers)
        def _(step):
            peer = lax.rem(me + step, peers)
            pl.semaphore_signal(
                barrier, inc=1, device_id=(group, peer // cores, lax.rem(peer, cores)), device_id_type=MESH
            )

        greeted = peers - 1
    else:
        for peer in (sibling, west, east):
            pl.semaphore_signal(barrier, inc=1, device_id=peer, device_id_type=MESH)
        greeted = 3

    loads = []

    def load(source, target):
        copy = pltpu.make_async_copy(source, target, load_sem.at[len(loads)])
        copy.start()
        loads.append(copy)
        return copy

    gather_load = load(gather_ref, gather)
    tiles = geo.rows // 8
    first_tile = var * (geo.row_count // 8)
    slabs = []
    for s in range(geo.taken // 8):
        tile = lax.rem(first_tile + s, tiles)
        for h in (0, 1):
            some = slice(h * geo.half_cols, (h + 1) * geo.half_cols)
            slabs.append(
                load(
                    tok_ref.at[some, :, pl.ds(pl.multiple_of(tile * 8, 8), 8), :],
                    raw.at[some, :, 8 * s : 8 * s + 8, :],
                )
            )
    fold_loads = [
        load(a, b)
        for a, b in ((lq_ref, lq), (wq_ref, wq), (wkv_ref, wkv), (wo_ref, wo), (dm_ref, dm), (perm_ref, perm))
    ]
    late_loads = [
        load(a, b)
        for a, b in (
            (mask_ref, marks.at[0]),
            (wqkv_ref, qkv.at[0]),
            (wproj_ref, proj.at[0]),
            (wup_ref, up.at[0]),
            (wdown_ref, down.at[0]),
            (position_ref, position),
            (order_ref, order),
            (pick_ref, pick),
        )
    ]

    depth = geo.half_cols * levels * geo.taken

    def collect(h, w, target):
        slab = raw[h * geo.half_cols : (h + 1) * geo.half_cols].reshape(depth, features)
        picked = gather[pl.ds(pl.multiple_of(w * half, 16), half), :]
        target[w] = jnp.dot(picked, slab, preferred_element_type=F32).astype(BF16)

    gather_load.wait()
    for copy in slabs[1::2]:
        copy.wait()
    collect(1, turn(0, east_grid), first)
    pl.semaphore_wait(barrier, greeted)

    def remote(source, target, send, recv, peer):
        copy = pltpu.make_async_remote_copy(
            src_ref=source, dst_ref=target, send_sem=send, recv_sem=recv, device_id=peer, device_id_type=MESH
        )
        copy.start()
        return copy

    copies = [remote(mask_ref, marks.at[1], weight_send.at[0], weight_recv.at[0], east)]
    halos = []

    def pass_on(step):
        w = turn(step, east_grid)
        halos.append(remote(first.at[w], halo.at[w], halo_send.at[w], halo_recv.at[w], east))

    pass_on(0)
    for n, (source, target) in enumerate(((wqkv_ref, qkv), (wproj_ref, proj), (wup_ref, up), (wdown_ref, down))):
        copies.append(remote(source, target.at[1], weight_send.at[n + 1], weight_recv.at[n + 1], sibling))

    for step in range(1, windows):
        collect(1, turn(step, east_grid), first)
    for copy in slabs[0::2]:
        copy.wait()
    for step in range(windows):
        collect(0, turn(step), own)
    for step in range(1, windows):
        pass_on(step)
    for copy in fold_loads:
        copy.wait()
    fold_decoder(lq[...], wq[...], wkv, wo[...], dm[...], perm[...], fold)

    tokens = geo.tokens
    q_pos = lax.broadcasted_iota(jnp.int32, (tokens, KEYS), 0)
    k_pos = lax.broadcasted_iota(jnp.int32, (tokens, KEYS), 1)
    diagonal = q_pos == k_pos

    def region_of(pos):
        pos = jnp.where(pos >= half, pos - half, pos)
        for level in range(levels - 1, 0, -1):
            start = geo.half_patches * level
            pos = jnp.where(pos >= start, pos - start, pos)
        return pos >= geo.half_patches // 2

    differs[...] = jnp.where(region_of(q_pos) != region_of(k_pos), -1e30, 0.0)
    lane_head = lax.broadcasted_iota(jnp.int32, (tokens, width), 1) // HD
    lane_head_keys = lax.broadcasted_iota(jnp.int32, (KEYS, width), 1) // HD

    for copy in late_loads:
        copy.wait()
    copies.append(remote(fold.at[0], fold.at[1], weight_send.at[5], weight_recv.at[5], sibling))

    count = heads * LEVEL_SLOTS
    pixels = geo.pixels
    row_size = pixels // cores // SQUARE_SPAN
    rows = geo.slots * row_size
    half_lat = WIN_LAT // 2
    extra = half_lat * geo.cols * SQUARE_SPAN - BLOCK
    pix[geo.isobars :] = jnp.zeros((geo.slots - geo.isobars, pixels, BLOCK), F32)
    units = up.shape[2]

    def piece_copy(w, ih, core, action):
        band = lax.rem(var * windows + w + ih, bands)
        here = jnp.logical_and(band == grid, core == var)
        source, target = pieces.at[w, ih, core], out_ref.at[grid, ih]

        @pl.when(here)
        def _():
            if action == "start":
                pltpu.make_async_copy(source, target, piece_recv.at[grid, ih]).start()

        @pl.when(jnp.logical_not(here))
        def _():
            if action == "start":
                pltpu.make_async_remote_copy(
                    src_ref=source,
                    dst_ref=target,
                    send_sem=piece_send.at[w, ih, core],
                    recv_sem=piece_recv.at[grid, ih],
                    device_id=(group, band, core),
                    device_id_type=MESH,
                ).start()
            else:
                pltpu.make_async_copy(source, source, piece_send.at[w, ih, core]).wait()

    def arrive(w):
        pltpu.make_async_copy(halo.at[w], halo.at[w], halo_recv.at[w]).wait()

    def send(w, some=range(cores)):
        for core in some:
            checked[...] = pieces[w, :, core].astype(F32).max(axis=0)
        if geo.scatter:
            for core in some:
                for ih in range(2):
                    piece_copy(w, ih, core, "start")

    def attend(w):
        x = jnp.concatenate([own[w], halo[w]], axis=0).astype(F32)
        n1 = layer_norm(x).astype(BF16)
        target = position[0:1, :] + (var * geo.row_count + WIN_LAT * w + half_lat)
        target = jnp.where(target >= geo.rows, target - geo.rows, target)
        there = lax.broadcasted_iota(jnp.int32, (geo.rows, KEYS), 0) == target
        there = there.astype(F32).astype(BF16)
        opened = jnp.zeros((1, KEYS), F32)
        column = lax.broadcasted_iota(jnp.int32, (geo.cols, KEYS), 0)
        for h in range(2):
            seen = (marks[h] > 0).astype(F32).astype(BF16)
            seen = jnp.dot(seen, there, preferred_element_type=F32)
            seen = jnp.where(column == position[1 + h : 2 + h, :], seen, 0.0)
            opened = opened + jnp.sum(seen, axis=0, keepdims=True)
        allowed = jnp.logical_or(jnp.broadcast_to(opened, diagonal.shape) > 0.5, diagonal)
        cut = jnp.logical_and(var == cores - 1, w == windows - 1)
        bias = jnp.where(allowed, 0.0, -1e30) + differs[...] * jnp.where(cut, 1.0, 0.0)
        yield
        scores, values = [], []
        for s in range(cores):
            q = jnp.dot(n1, qkv[s, 0], preferred_element_type=F32).astype(BF16)
            q = q * jnp.asarray(HD ** (-0.5), BF16)
            k = jnp.dot(n1, qkv[s, 1], preferred_element_type=F32).astype(BF16)
            v = jnp.dot(n1, qkv[s, 2], preferred_element_type=F32).astype(BF16)
            tail = jnp.zeros((KEYS - tokens, width), BF16)
            k = jnp.concatenate([k, tail], axis=0)
            values.append(jnp.concatenate([v, tail], axis=0))
            q_all = jnp.concatenate(
                [jnp.where(lane_head == h, q, jnp.zeros_like(q)) for h in range(heads)], axis=0
            )
            yield
            scores.append(lax.dot_general(q_all, k, NT, preferred_element_type=F32))
            yield
        attended = x
        for s in range(cores):
            weights = []
            for h in range(heads):
                one = scores[s][h * tokens : (h + 1) * tokens] + bias
                peak = jnp.max(one, axis=-1, keepdims=True)
                e = jnp.exp(one - peak)
                total = jnp.sum(e, axis=-1, keepdims=True)
                weights.append((e * (1.0 / total)).astype(BF16))
            weights = jnp.concatenate(weights, axis=1)
            v = values[s]
            v_all = jnp.concatenate(
                [jnp.where(lane_head_keys == h, v, jnp.zeros_like(v)) for h in range(heads)], axis=0
            )
            context = jnp.dot(weights, v_all, preferred_element_type=F32).astype(BF16)
            yield
            attended = attended + jnp.dot(context, proj[s], preferred_element_type=F32)
            if s == cores - 1:
                x_one[w] = attended
            yield

    def finish(w):
        n2 = layer_norm(x_one[w]).astype(BF16)
        yield
        for s in range(cores):
            for c in range(0, units, CHUNK):
                one = jnp.dot(n2, up[s, :, c : c + CHUNK], preferred_element_type=F32)
                one = 0.5 * one * (1.0 + lax.erf(one * 2.0 ** (-0.5)))
                hid[:, s * units + c : s * units + c + CHUNK] = one.astype(BF16)
                yield
        latent = x_one[w] + jnp.dot(
            hid[...], down[...].reshape(cores * units, features), preferred_element_type=F32
        )
        yield
        n3 = layer_norm(latent.astype(BF16).astype(F32)).astype(BF16)
        n3 = jnp.dot(order[...], n3, preferred_element_type=F32).astype(BF16)
        n3, others = n3[:BLOCK], n3[BLOCK:]
        yield
        base = lax.dot_general(fold_base[...], n3, NT, preferred_element_type=F32)
        base_pix[...] = base[:pixels] + base[pixels:]
        for s in range(cores):
            g = lax.dot_general(fold[s, 0 : 2 * count, :], others, NT, preferred_element_type=F32)
            g = g[:count] + g[count:]
            scores = [jnp.zeros((count, BLOCK), F32)]
            scores += [g[:, j * BLOCK : (j + 1) * BLOCK] for j in range(levels - 1)]
            peak = functools.reduce(jnp.maximum, scores)
            e = [jnp.exp(one - peak) for one in scores]
            inverse = 1.0 / sum(e)
            u = lax.dot_general(fold[s, 2 * count :, :], others, NT, preferred_element_type=F32)
            for j in range(levels - 1):
                dw[j, s * count : (s + 1) * count, :] = e[j + 1] * inverse
                du[j, s * heads * pixels : (s + 1) * heads * pixels, :] = u[:, j * BLOCK : (j + 1) * BLOCK]
        yield

    def paint(w):
        low = pixels // cores
        lane = lax.broadcasted_iota(jnp.int32, (2 * row_size, BLOCK), 1)
        for core in range(cores):
            top = core * low
            for first_level in range(0, geo.isobars, 5):
                some = range(first_level, min(first_level + 5, geo.isobars))
                totals = [base_pix[top : top + low, :] for _ in some]
                for s in range(cores):
                    for h in range(heads):
                        for j in range(levels - 1):
                            at = (s * heads + h) * pixels + top
                            value = du[j, at : at + low, :]
                            for n, level in enumerate(some):
                                row = s * count + level * heads + h
                                totals[n] = totals[n] + dw[j, row : row + 1, :] * value
                for n, level in enumerate(some):
                    pix[level, top : top + low, :] = totals[n]
            total = jnp.zeros((rows, 4 * BLOCK), F32)
            for b in range(SQUARE_SPAN):
                at = top + b * row_size
                part = pix[:, at : at + row_size, :].reshape(rows, BLOCK)
                total = total + jnp.dot(part.astype(BF16), pick[b], preferred_element_type=F32)
            for ih in range(2):
                left = jnp.zeros((2 * row_size, BLOCK), F32)
                for k in range(geo.slots // 2):
                    at = slice(2 * row_size * k, 2 * row_size * (k + 1))
                    inside = jnp.logical_and(lane >= extra * k, lane < extra * (k + 1))
                    left = jnp.where(inside, total[at, (2 + ih) * BLOCK : (3 + ih) * BLOCK], left)
                main = total[:, ih * BLOCK : (ih + 1) * BLOCK]
                pieces[w, ih, core] = jnp.concatenate([main, left], axis=0).astype(BF16)
            yield

    def run(order="", **steps):
        for name in order:
            next(steps[name])

    mask_copy, qkv_copy, proj_copy, up_copy, down_copy, fold_copy = copies
    for copy in (mask_copy, qkv_copy, proj_copy):
        copy.wait()
    arrive(turn(0))
    run("a" * ORDER.count("a"), a=attend(turn(0)))
    for copy in (up_copy, down_copy, fold_copy):
        copy.wait()
    whole = jnp.zeros((pixels, features), F32)
    for s in range(cores):
        for h in range(heads):
            top = 2 * count + h * pixels
            whole = whole + fold[s, top : top + pixels, :].astype(F32)
    whole_hi = whole.astype(BF16)
    fold_base[0:pixels, :] = whole_hi
    fold_base[pixels:, :] = (whole - whole_hi.astype(F32)).astype(BF16)

    last = windows - 1

    def complete(w):
        yield from finish(w)
        yield from paint(w)

    @pl.loop(0, last)
    def _(step):
        arrive(turn(step + 1))
        run(ORDER, a=attend(turn(step + 1)), b=complete(turn(step)))
        send(turn(step))

    finishing = complete(turn(last))
    run("b" * (ORDER.count("b") - cores), b=finishing)
    for core in range(cores):
        next(finishing)
        send(turn(last), (core,))

    for copy in halos:
        copy.wait_send()
    if geo.scatter:

        @pl.loop(0, bands)
        def _(s):
            for ih in range(2):
                target = out_ref.at[s, ih]
                pltpu.make_async_copy(target, target, piece_recv.at[s, ih]).wait()

        @pl.loop(0, windows)
        def _(w):
            for ih in range(2):
                for core in range(cores):
                    piece_copy(w, ih, core, "finish")

    else:
        copy = pltpu.make_async_copy(pieces, out_ref, load_sem.at[0])
        copy.start()
        copy.wait()


def forecast(geo, *args):
    tables = (
        jnp.asarray(geo.gather_table(), BF16),
        jnp.asarray(geo.order_table(), BF16),
        jnp.asarray(geo.position_table(), jnp.int32),
        jnp.asarray(geo.pixel_table(), BF16),
        jnp.asarray(geo.pick_table(), BF16),
    )
    features, width, cores, windows = geo.features, geo.width, geo.cores, geo.windows
    units = args[4].shape[1]
    fold_rows = geo.heads * (2 * LEVEL_SLOTS + geo.pixels)
    vmem = pltpu.VMEM
    dma = pltpu.SemaphoreType.DMA
    if geo.scatter:
        out_shape = (geo.bands, 2, BLOCK, BLOCK)
    else:
        out_shape = (windows, 2, cores, BLOCK, BLOCK)
    return pl.pallas_call(
        functools.partial(main_kernel, geo),
        out_shape=jax.ShapeDtypeStruct(out_shape, BF16),
        in_specs=[pl.BlockSpec(memory_space=pltpu.HBM)] * (len(args) + len(tables)),
        out_specs=pl.BlockSpec(memory_space=vmem if geo.scatter else pltpu.HBM),
        scratch_shapes=[
            vmem((geo.cols, geo.levels, geo.taken, features), BF16),
            vmem((2, geo.cols, geo.rows), jnp.int32),
            vmem((cores, 3, features, width), BF16),
            vmem((cores, width, features), BF16),
            vmem((cores, features, units), BF16),
            vmem((cores, units, features), BF16),
            *[vmem(one.shape, one.dtype) for one in args[6:]],
            *[vmem(one.shape, one.dtype) for one in tables],
            vmem((cores, fold_rows, features), BF16),
            vmem((windows, geo.half, features), BF16),
            vmem((windows, geo.half, features), BF16),
            vmem((windows, geo.half, features), BF16),
            vmem((geo.tokens, KEYS), F32),
            vmem((geo.tokens, cores * units), BF16),
            vmem((geo.levels - 1, cores * geo.heads * LEVEL_SLOTS, BLOCK), F32),
            vmem((geo.levels - 1, cores * geo.heads * geo.pixels, BLOCK), F32),
            vmem((2 * geo.pixels, features), BF16),
            vmem((windows, geo.tokens, features), F32),
            vmem((geo.pixels, BLOCK), F32),
            vmem((geo.slots, geo.pixels, BLOCK), F32),
            vmem((windows, 2, cores, BLOCK, BLOCK), BF16),
            vmem((BLOCK, BLOCK), F32),
            dma((geo.taken // 4 + 15,)),
            dma((6,)),
            dma((6,)),
            dma((windows,)),
            dma((windows,)),
            dma((windows, 2, cores)),
            dma((geo.bands, 2)),
        ],
        compiler_params=pltpu.CompilerParams(
            collective_id=0, has_side_effects=True, vmem_limit_bytes=60 * 2**20
        ),
    )(*args, *tables)


def assemble_kernel(isobars, run, got_ref, out_ref):
    bands = got_ref.shape[0]
    half_lat = WIN_LAT // 2
    groups = (isobars + 1) // 2
    rows = groups * 16
    whole_run = out_ref.shape[-1]
    tiles = whole_run // BLOCK
    extra = half_lat * run - BLOCK
    lane = lax.broadcasted_iota(jnp.int32, (rows, BLOCK), 1)

    @pl.loop(0, 2)
    def _(ih):
        for r in range(half_lat):
            out = [jnp.zeros((rows, BLOCK), F32) for _ in range(tiles)]
            for s in range(bands):
                base = (s * run + whole_run - run // 2) % whole_run
                piece = got_ref[s, ih].astype(F32)
                whole = min(run, BLOCK - r * run)
                parts = [(pltpu.roll(piece[:rows], (base - r * run) % BLOCK, 1), base, base + whole)]
                if whole < run:
                    rest = piece[rows:]
                    moved = [
                        pltpu.roll(rest, (base + whole - extra * k) % BLOCK, 1) for k in range(groups)
                    ]
                    parts.append((jnp.concatenate(moved, axis=0), base + whole, base + run))
                for value, low, high in parts:
                    spans = [(low, min(high, whole_run)), (max(low, whole_run) - whole_run, high - whole_run)]
                    for low, high in spans:
                        if high <= low:
                            continue
                        for t in range(low // BLOCK, (high - 1) // BLOCK + 1):
                            at = lane + t * BLOCK
                            out[t] = jnp.where(jnp.logical_and(at >= low, at < high), value, out[t])
            for t in range(tiles):
                value = out[t].reshape(2 * groups, 8, BLOCK)[:isobars]
                for flag in range(2):
                    top = ((half_lat if flag == 0 else 0) + r) * SQUARE_SPAN

                    @pl.when(ih == flag)
                    def _():
                        for v in range(2):
                            out_ref[v, :, top : top + SQUARE_SPAN, t * BLOCK : (t + 1) * BLOCK] = value[
                                :, v * SQUARE_SPAN : (v + 1) * SQUARE_SPAN
                            ]


def assemble(got, columns, isobars):
    bands = got.shape[0]
    run = columns * SQUARE_SPAN
    shape = (TARGET_QUANTITY // 2, isobars, WIN_LAT * SQUARE_SPAN, bands * run)
    return pl.pallas_call(
        functools.partial(assemble_kernel, isobars, run),
        out_shape=jax.ShapeDtypeStruct(shape, F32),
        compiler_params=pltpu.CompilerParams(vmem_limit_bytes=40 * 2**20),
    )(got)


def exchange(pieces, geo):
    half_lat = WIN_LAT // 2
    run = geo.cols * SQUARE_SPAN
    quantities = TARGET_QUANTITY // geo.cores
    rows = geo.slots * quantities * SQUARE_SPAN
    extra = half_lat * run - BLOCK
    lead = pieces.shape[:3]
    main = pieces[:, :, :, :rows].reshape(*lead, geo.slots, quantities, SQUARE_SPAN, BLOCK)
    rest = pieces[:, :, :, rows:, : extra * (geo.slots // 2)]
    rest = rest.reshape(*lead, 2, quantities, SQUARE_SPAN, geo.slots // 2, extra)
    rest = jnp.moveaxis(rest, 6, 3).reshape(*lead, geo.slots, quantities, SQUARE_SPAN, extra)
    maps = jnp.concatenate([main, rest], axis=-1)[:, :, :, : geo.isobars]
    maps = maps.reshape(*lead, geo.isobars, quantities, SQUARE_SPAN, half_lat, run)
    maps = jnp.transpose(maps, (2, 4, 3, 0, 1, 6, 5, 7))
    maps = maps.reshape(TARGET_QUANTITY, geo.isobars, geo.row_count * SQUARE_SPAN, run)
    maps = lax.all_to_all(maps, "var", split_axis=0, concat_axis=2, tiled=True)
    maps = jnp.roll(maps, half_lat * SQUARE_SPAN, 2)
    maps = lax.all_to_all(maps, "grid", split_axis=2, concat_axis=3, tiled=True)
    return jnp.roll(maps, -(run // 2), 3).astype(F32)


def local(
    tokens,
    key_mask,
    w_qkv,
    w_proj,
    w_up,
    w_down,
    level_query,
    w_dec_q,
    w_dec_kv,
    w_dec_o,
    decode_matrix,
):
    geo = Geometry(
        tokens, w_proj, level_query, decode_matrix, lax.axis_size("var"), lax.axis_size("grid")
    )
    pieces = forecast(
        geo,
        jnp.transpose(tokens, (1, 2, 0, 3)),
        key_mask.T,
        w_qkv,
        w_proj,
        w_up,
        w_down,
        level_query,
        w_dec_q,
        w_dec_kv,
        w_dec_o,
        decode_matrix.T,
    )
    if geo.scatter:
        return assemble(pieces, geo.cols, geo.isobars)
    return exchange(pieces, geo)


def solution(mesh):
    placed = (
        P("group", "grid", None, None),
        P("group", "grid"),
        P(None, None, "var"),
        P("var", None),
        P(None, "var"),
        P("var", None),
        P(),
        P(None, "var"),
        P(None, None, "var"),
        P("var", None),
        P(),
    )
    return jax.shard_map(
        local,
        mesh=mesh,
        in_specs=placed,
        out_specs=P("var", "group", "grid", None),
        check_vma=False,
    )
```

```python
import functools

import jax
import jax.numpy as jnp
import numpy as np
from jax import lax
from jax.experimental import pallas as pl
from jax.experimental.pallas import tpu as pltpu
from jax.sharding import PartitionSpec as P

HD = 64
TARGET_QUANTITY = 4
SQUARE_SPAN = 4
WIN_LAT = 6
EPSILON = 1e-05
BLOCK = 128
KEYS = 256
CHUNK = 256
LEVEL_SLOTS = 16
ORDER = "abaabbbbaaabbbbabaabbbb"
MESH = pl.DeviceIdType.MESH
NT = (((1,), (1,)), ((), ()))
F32 = jnp.float32
BF16 = jnp.bfloat16


def layer_norm(values):
    center = values - jnp.mean(values, axis=-1, keepdims=True)
    spread = jnp.mean(center * center, axis=-1, keepdims=True)
    return center * lax.rsqrt(spread + EPSILON)


class Geometry:
    def __init__(self, tokens, w_proj, level_query, decode_matrix, cores, bands):
        self.rows, self.cols, self.levels, self.features = tokens.shape
        self.cores, self.bands = cores, bands
        self.half_cols = self.cols // 2
        self.row_count = self.rows // cores
        self.windows = self.row_count // WIN_LAT
        self.taken = 8 * (-(-(self.row_count + WIN_LAT // 2) // 8))
        self.half_patches = WIN_LAT * self.half_cols
        self.half = 16 * (-(-(self.levels * self.half_patches) // 16))
        self.tokens = 2 * self.half
        self.patches = 2 * self.half_patches
        self.width = w_proj.shape[0]
        self.heads = self.width // HD
        self.isobars = level_query.shape[0]
        self.slots = self.isobars + self.isobars % 2
        self.pixels = decode_matrix.shape[1]
        self.scatter = bands * WIN_LAT == self.rows and (bands * self.cols * SQUARE_SPAN) % BLOCK == 0

    def place(self, half, level, r, c):
        return half * self.half + level * self.half_patches + r * self.half_cols + c

    def each(self):
        for half in range(2):
            for level in range(self.levels):
                for r in range(WIN_LAT):
                    for c in range(self.half_cols):
                        yield half, level, r, c

    def gather_table(self):
        table = np.zeros((self.windows, self.half, self.half_cols * self.levels * self.taken), np.float32)
        for w in range(self.windows):
            for half, level, r, c in self.each():
                if half == 0:
                    source = (c * self.levels + level) * self.taken + WIN_LAT * w + WIN_LAT // 2 + r
                    table[w, self.place(0, level, r, c), source] = 1.0
        return table.reshape(self.windows * self.half, -1)

    def order_table(self):
        table = np.zeros((self.levels * BLOCK, self.tokens), np.float32)
        for half, level, r, c in self.each():
            patch = r * self.cols + (1 - half) * self.half_cols + c
            table[level * BLOCK + patch, self.place(half, level, r, c)] = 1.0
            if level > 0:
                table[level * BLOCK + patch, self.place(half, 0, r, c)] = -1.0
        return table

    def position_table(self):
        table = np.full((8, KEYS), -1, np.int32)
        table[0] = 0
        for half, level, r, c in self.each():
            at = self.place(half, level, r, c)
            table[0, at] = r
            table[1 + half, at] = c + half * self.half_cols
        return table

    def pixel_table(self):
        table = np.zeros((self.pixels, self.pixels), np.float32)
        own = TARGET_QUANTITY // self.cores
        for v in range(TARGET_QUANTITY):
            for a in range(SQUARE_SPAN):
                for b in range(SQUARE_SPAN):
                    target = ((v // own * SQUARE_SPAN + b) * own + v % own) * SQUARE_SPAN + a
                    table[target, (v * SQUARE_SPAN + a) * SQUARE_SPAN + b] = 1.0
        return table

    def pick_table(self):
        half_lat = WIN_LAT // 2
        run = self.cols * SQUARE_SPAN
        extra = half_lat * run - BLOCK
        picks = np.zeros((SQUARE_SPAN, BLOCK, 4 * BLOCK), np.float32)
        for ih in range(2):
            for q in range(half_lat * run):
                r, rest = divmod(q, run)
                column, b = divmod(rest, SQUARE_SPAN)
                source = (half_lat * ih + r) * self.cols + column
                if q < BLOCK:
                    picks[b, source, ih * BLOCK + q] = 1.0
                else:
                    for k in range(self.slots // 2):
                        picks[b, source, (2 + ih) * BLOCK + extra * k + q - BLOCK] = 1.0
        return picks


def fold_decoder(lq, wq, wkv_ref, wo, dm, perm, out_ref):
    width = wq.shape[1]
    heads = width // HD
    dquery = jnp.dot(lq, wq, preferred_element_type=F32) * HD ** (-0.5)
    d_hi = dquery.astype(BF16)
    d_lo = (dquery - d_hi.astype(F32)).astype(BF16)
    count = LEVEL_SLOTS * heads
    row = lax.broadcasted_iota(jnp.int32, (count, dquery.shape[0]), 0)
    slot = lax.broadcasted_iota(jnp.int32, (count, dquery.shape[0]), 1)
    spread = (row // heads == slot).astype(F32).astype(BF16)
    row = lax.broadcasted_iota(jnp.int32, (count, width), 0)
    mine = row % heads == lax.broadcasted_iota(jnp.int32, (count, width), 1) // HD
    q_hi = jnp.dot(spread, d_hi, preferred_element_type=F32)
    q_hi = jnp.where(mine, q_hi, 0.0).astype(BF16)
    q_lo = jnp.dot(spread, d_lo, preferred_element_type=F32)
    q_lo = jnp.where(mine, q_lo, 0.0).astype(BF16)
    wk = wkv_ref[0]
    g = lax.dot_general(q_hi, wk, NT, preferred_element_type=F32)
    g = g + lax.dot_general(q_lo, wk, NT, preferred_element_type=F32)
    g_hi = g.astype(BF16)
    out_ref[0, 0:count, :] = g_hi
    out_ref[0, count : 2 * count, :] = (g - g_hi.astype(F32)).astype(BF16)
    dm_hi = dm.astype(BF16)
    dm_lo = (dm - dm_hi.astype(F32)).astype(BF16)
    dm_hi = jnp.dot(perm, dm_hi, preferred_element_type=F32).astype(BF16)
    dm_lo = jnp.dot(perm, dm_lo, preferred_element_type=F32).astype(BF16)
    m_t = lax.dot_general(dm_hi, wo, NT, preferred_element_type=F32)
    m_t = m_t + lax.dot_general(dm_lo, wo, NT, preferred_element_type=F32)
    pixels = m_t.shape[0]
    stacked = jnp.concatenate([m_t] * heads, axis=0)
    row_head = lax.broadcasted_iota(jnp.int32, stacked.shape, 0) // pixels
    lane_head = lax.broadcasted_iota(jnp.int32, stacked.shape, 1) // HD
    stacked = jnp.where(row_head == lane_head, stacked, 0.0)
    s_hi = stacked.astype(BF16)
    s_lo = (stacked - s_hi.astype(F32)).astype(BF16)
    wv = wkv_ref[1]
    n_t = lax.dot_general(s_hi, wv, NT, preferred_element_type=F32)
    n_t = n_t + lax.dot_general(s_lo, wv, NT, preferred_element_type=F32)
    out_ref[0, 2 * count :, :] = n_t.astype(BF16)


def main_kernel(
    geo,
    tok_ref,
    mask_ref,
    wqkv_ref,
    wproj_ref,
    wup_ref,
    wdown_ref,
    lq_ref,
    wq_ref,
    wkv_ref,
    wo_ref,
    dm_ref,
    gather_ref,
    order_ref,
    position_ref,
    perm_ref,
    pick_ref,
    out_ref,
    raw,
    marks,
    qkv,
    proj,
    up,
    down,
    lq,
    wq,
    wkv,
    wo,
    dm,
    gather,
    order,
    position,
    perm,
    pick,
    fold,
    first,
    own,
    halo,
    differs,
    hid,
    dw,
    du,
    ready,
    fold_base,
    x_one,
    base_pix,
    pix,
    pieces,
    checked,
    load_sem,
    weight_send,
    weight_recv,
    halo_send,
    halo_recv,
    piece_send,
    piece_recv,
):
    group, grid, var = (lax.axis_index(name) for name in ("group", "grid", "var"))
    bands, cores, windows, half = geo.bands, geo.cores, geo.windows, geo.half
    features, levels, width, heads = geo.features, geo.levels, geo.width, geo.heads
    sibling = (group, grid, lax.rem(var + 1, cores))

    def turn(step, column=grid):
        near = column * cores // bands == var
        rest = lax.rem(step + column + windows - 2, windows - 1)
        return jnp.where(near, jnp.where(step == 0, windows - 1, rest), step)

    east_grid = lax.rem(grid + 1, bands)
    west = (group, lax.rem(grid + bands - 1, bands), var)
    east = (group, east_grid, var)
    barrier = pltpu.get_barrier_semaphore()
    if geo.scatter:
        peers = bands * cores
        me = grid * cores + var

        @pl.loop(1, peers)
        def _(step):
            peer = lax.rem(me + step, peers)
            pl.semaphore_signal(
                barrier, inc=1, device_id=(group, peer // cores, lax.rem(peer, cores)), device_id_type=MESH
            )

        greeted = peers - 1
    else:
        for peer in (sibling, west, east):
            pl.semaphore_signal(barrier, inc=1, device_id=peer, device_id_type=MESH)
        greeted = 3

    loads = []

    def load(source, target):
        copy = pltpu.make_async_copy(source, target, load_sem.at[len(loads)])
        copy.start()
        loads.append(copy)
        return copy

    gather_load = load(gather_ref, gather)
    tiles = geo.rows // 8
    first_tile = var * (geo.row_count // 8)
    slabs = []
    for s in range(geo.taken // 8):
        tile = lax.rem(first_tile + s, tiles)
        for h in (0, 1):
            some = slice(h * geo.half_cols, (h + 1) * geo.half_cols)
            slabs.append(
                load(
                    tok_ref.at[some, :, pl.ds(pl.multiple_of(tile * 8, 8), 8), :],
                    raw.at[some, :, 8 * s : 8 * s + 8, :],
                )
            )
    fold_loads = [
        load(a, b)
        for a, b in ((lq_ref, lq), (wq_ref, wq), (wkv_ref, wkv), (wo_ref, wo), (dm_ref, dm), (perm_ref, perm))
    ]
    late_loads = [
        load(a, b)
        for a, b in (
            (mask_ref, marks.at[0]),
            (wqkv_ref, qkv.at[0]),
            (wproj_ref, proj.at[0]),
            (wup_ref, up.at[0]),
            (wdown_ref, down.at[0]),
            (position_ref, position),
            (order_ref, order),
            (pick_ref, pick),
        )
    ]

    depth = geo.half_cols * levels * geo.taken

    def collect(h, w, target):
        slab = raw[h * geo.half_cols : (h + 1) * geo.half_cols].reshape(depth, features)
        picked = gather[pl.ds(pl.multiple_of(w * half, 16), half), :]
        target[w] = jnp.dot(picked, slab, preferred_element_type=F32).astype(BF16)

    gather_load.wait()
    for copy in slabs[1::2]:
        copy.wait()
    collect(1, turn(0, east_grid), first)
    pl.semaphore_wait(barrier, greeted)

    def remote(source, target, send, recv, peer):
        copy = pltpu.make_async_remote_copy(
            src_ref=source, dst_ref=target, send_sem=send, recv_sem=recv, device_id=peer, device_id_type=MESH
        )
        copy.start()
        return copy

    copies = [remote(mask_ref, marks.at[1], weight_send.at[0], weight_recv.at[0], east)]
    halos = []

    def pass_on(step):
        w = turn(step, east_grid)
        halos.append(remote(first.at[w], halo.at[w], halo_send.at[w], halo_recv.at[w], east))

    pass_on(0)
    for n, (source, target) in enumerate(((wqkv_ref, qkv), (wproj_ref, proj), (wup_ref, up), (wdown_ref, down))):
        copies.append(remote(source, target.at[1], weight_send.at[n + 1], weight_recv.at[n + 1], sibling))

    for step in range(1, windows):
        collect(1, turn(step, east_grid), first)
    for copy in slabs[0::2]:
        copy.wait()
    for step in range(windows):
        collect(0, turn(step), own)
    for step in range(1, windows):
        pass_on(step)
    for copy in fold_loads:
        copy.wait()
    fold_decoder(lq[...], wq[...], wkv, wo[...], dm[...], perm[...], fold)

    tokens = geo.tokens
    q_pos = lax.broadcasted_iota(jnp.int32, (tokens, KEYS), 0)
    k_pos = lax.broadcasted_iota(jnp.int32, (tokens, KEYS), 1)
    diagonal = q_pos == k_pos

    def region_of(pos):
        pos = jnp.where(pos >= half, pos - half, pos)
        for level in range(levels - 1, 0, -1):
            start = geo.half_patches * level
            pos = jnp.where(pos >= start, pos - start, pos)
        return pos >= geo.half_patches // 2

    differs[...] = jnp.where(region_of(q_pos) != region_of(k_pos), -1e30, 0.0)
    lane_head = lax.broadcasted_iota(jnp.int32, (tokens, width), 1) // HD
    lane_head_keys = lax.broadcasted_iota(jnp.int32, (KEYS, width), 1) // HD

    for copy in late_loads:
        copy.wait()
    copies.append(remote(fold.at[0], fold.at[1], weight_send.at[5], weight_recv.at[5], sibling))

    count = heads * LEVEL_SLOTS
    pixels = geo.pixels
    row_size = pixels // cores // SQUARE_SPAN
    rows = geo.slots * row_size
    half_lat = WIN_LAT // 2
    extra = half_lat * geo.cols * SQUARE_SPAN - BLOCK
    pix[geo.isobars :] = jnp.zeros((geo.slots - geo.isobars, pixels, BLOCK), F32)
    units = up.shape[2]

    def piece_copy(w, ih, core, action):
        band = lax.rem(var * windows + w + ih, bands)
        here = jnp.logical_and(band == grid, core == var)
        source, target = pieces.at[w, ih, core], out_ref.at[grid, ih]

        @pl.when(here)
        def _():
            if action == "start":
                pltpu.make_async_copy(source, target, piece_recv.at[grid, ih]).start()

        @pl.when(jnp.logical_not(here))
        def _():
            if action == "start":
                pltpu.make_async_remote_copy(
                    src_ref=source,
                    dst_ref=target,
                    send_sem=piece_send.at[w, ih, core],
                    recv_sem=piece_recv.at[grid, ih],
                    device_id=(group, band, core),
                    device_id_type=MESH,
                ).start()
            else:
                pltpu.make_async_copy(source, source, piece_send.at[w, ih, core]).wait()

    def arrive(w):
        pltpu.make_async_copy(halo.at[w], halo.at[w], halo_recv.at[w]).wait()

    def send(w, some=range(cores)):
        for core in some:
            checked[...] = pieces[w, :, core].astype(F32).max(axis=0)
        if geo.scatter:
            for core in some:
                for ih in range(2):
                    piece_copy(w, ih, core, "start")

    def attend(w):
        x = jnp.concatenate([own[w], halo[w]], axis=0).astype(F32)
        n1 = layer_norm(x[half:]).astype(BF16)
        target = position[0:1, :] + (var * geo.row_count + WIN_LAT * w + half_lat)
        target = jnp.where(target >= geo.rows, target - geo.rows, target)
        there = lax.broadcasted_iota(jnp.int32, (geo.rows, KEYS), 0) == target
        there = there.astype(F32).astype(BF16)
        opened = jnp.zeros((1, KEYS), F32)
        column = lax.broadcasted_iota(jnp.int32, (geo.cols, KEYS), 0)
        for h in range(2):
            seen = (marks[h] > 0).astype(F32).astype(BF16)
            seen = jnp.dot(seen, there, preferred_element_type=F32)
            seen = jnp.where(column == position[1 + h : 2 + h, :], seen, 0.0)
            opened = opened + jnp.sum(seen, axis=0, keepdims=True)
        allowed = jnp.logical_or(jnp.broadcast_to(opened, diagonal.shape) > 0.5, diagonal)
        cut = jnp.logical_and(var == cores - 1, w == windows - 1)
        bias = jnp.where(allowed, 0.0, -1e30) + differs[...] * jnp.where(cut, 1.0, 0.0)
        yield
        scores, values = [], []
        for s in range(cores):
            q, k, v = (
                jnp.concatenate(
                    [ready[s, i, w], jnp.dot(n1, qkv[s, i], preferred_element_type=F32).astype(BF16)], axis=0
                )
                for i in range(3)
            )
            q = q * jnp.asarray(HD ** (-0.5), BF16)
            tail = jnp.zeros((KEYS - tokens, width), BF16)
            k = jnp.concatenate([k, tail], axis=0)
            values.append(jnp.concatenate([v, tail], axis=0))
            q_all = jnp.concatenate(
                [jnp.where(lane_head == h, q, jnp.zeros_like(q)) for h in range(heads)], axis=0
            )
            yield
            scores.append(lax.dot_general(q_all, k, NT, preferred_element_type=F32))
            yield
        attended = x
        for s in range(cores):
            weights = []
            for h in range(heads):
                one = scores[s][h * tokens : (h + 1) * tokens] + bias
                peak = jnp.max(one, axis=-1, keepdims=True)
                e = jnp.exp(one - peak)
                total = jnp.sum(e, axis=-1, keepdims=True)
                weights.append((e * (1.0 / total)).astype(BF16))
            weights = jnp.concatenate(weights, axis=1)
            v = values[s]
            v_all = jnp.concatenate(
                [jnp.where(lane_head_keys == h, v, jnp.zeros_like(v)) for h in range(heads)], axis=0
            )
            context = jnp.dot(weights, v_all, preferred_element_type=F32).astype(BF16)
            yield
            attended = attended + jnp.dot(context, proj[s], preferred_element_type=F32)
            if s == cores - 1:
                x_one[w] = attended
            yield

    def finish(w):
        n2 = layer_norm(x_one[w]).astype(BF16)
        yield
        for s in range(cores):
            for c in range(0, units, CHUNK):
                one = jnp.dot(n2, up[s, :, c : c + CHUNK], preferred_element_type=F32)
                one = 0.5 * one * (1.0 + lax.erf(one * 2.0 ** (-0.5)))
                hid[:, s * units + c : s * units + c + CHUNK] = one.astype(BF16)
                yield
        latent = x_one[w] + jnp.dot(
            hid[...], down[...].reshape(cores * units, features), preferred_element_type=F32
        )
        yield
        n3 = layer_norm(latent.astype(BF16).astype(F32)).astype(BF16)
        n3 = jnp.dot(order[...], n3, preferred_element_type=F32).astype(BF16)
        n3, others = n3[:BLOCK], n3[BLOCK:]
        yield
        base = lax.dot_general(fold_base[...], n3, NT, preferred_element_type=F32)
        base_pix[...] = base[:pixels] + base[pixels:]
        for s in range(cores):
            g = lax.dot_general(fold[s, 0 : 2 * count, :], others, NT, preferred_element_type=F32)
            g = g[:count] + g[count:]
            scores = [jnp.zeros((count, BLOCK), F32)]
            scores += [g[:, j * BLOCK : (j + 1) * BLOCK] for j in range(levels - 1)]
            peak = functools.reduce(jnp.maximum, scores)
            e = [jnp.exp(one - peak) for one in scores]
            inverse = 1.0 / sum(e)
            u = lax.dot_general(fold[s, 2 * count :, :], others, NT, preferred_element_type=F32)
            for j in range(levels - 1):
                dw[j, s * count : (s + 1) * count, :] = e[j + 1] * inverse
                du[j, s * heads * pixels : (s + 1) * heads * pixels, :] = u[:, j * BLOCK : (j + 1) * BLOCK]
        yield

    def paint(w):
        low = pixels // cores
        lane = lax.broadcasted_iota(jnp.int32, (2 * row_size, BLOCK), 1)
        for core in range(cores):
            top = core * low
            for first_level in range(0, geo.isobars, 5):
                some = range(first_level, min(first_level + 5, geo.isobars))
                totals = [base_pix[top : top + low, :] for _ in some]
                for s in range(cores):
                    for h in range(heads):
                        for j in range(levels - 1):
                            at = (s * heads + h) * pixels + top
                            value = du[j, at : at + low, :]
                            for n, level in enumerate(some):
                                row = s * count + level * heads + h
                                totals[n] = totals[n] + dw[j, row : row + 1, :] * value
                for n, level in enumerate(some):
                    pix[level, top : top + low, :] = totals[n]
            total = jnp.zeros((rows, 4 * BLOCK), F32)
            for b in range(SQUARE_SPAN):
                at = top + b * row_size
                part = pix[:, at : at + row_size, :].reshape(rows, BLOCK)
                total = total + jnp.dot(part.astype(BF16), pick[b], preferred_element_type=F32)
            for ih in range(2):
                left = jnp.zeros((2 * row_size, BLOCK), F32)
                for k in range(geo.slots // 2):
                    at = slice(2 * row_size * k, 2 * row_size * (k + 1))
                    inside = jnp.logical_and(lane >= extra * k, lane < extra * (k + 1))
                    left = jnp.where(inside, total[at, (2 + ih) * BLOCK : (3 + ih) * BLOCK], left)
                main = total[:, ih * BLOCK : (ih + 1) * BLOCK]
                pieces[w, ih, core] = jnp.concatenate([main, left], axis=0).astype(BF16)
            yield

    def run(order="", **steps):
        for name in order:
            next(steps[name])

    mask_copy, qkv_copy, proj_copy, up_copy, down_copy, fold_copy = copies
    for copy in (mask_copy, qkv_copy, proj_copy):
        copy.wait()
    n_own = layer_norm(own[...].reshape(windows * half, features).astype(F32)).astype(BF16)
    for s in range(cores):
        for i in range(3):
            one = jnp.dot(n_own, qkv[s, i], preferred_element_type=F32).astype(BF16)
            ready[s, i] = one.reshape(windows, half, width)
    arrive(turn(0))
    run("a" * ORDER.count("a"), a=attend(turn(0)))
    for copy in (up_copy, down_copy, fold_copy):
        copy.wait()
    whole = jnp.zeros((pixels, features), F32)
    for s in range(cores):
        for h in range(heads):
            top = 2 * count + h * pixels
            whole = whole + fold[s, top : top + pixels, :].astype(F32)
    whole_hi = whole.astype(BF16)
    fold_base[0:pixels, :] = whole_hi
    fold_base[pixels:, :] = (whole - whole_hi.astype(F32)).astype(BF16)

    last = windows - 1

    def complete(w):
        yield from finish(w)
        yield from paint(w)

    @pl.loop(0, last)
    def _(step):
        arrive(turn(step + 1))
        run(ORDER, a=attend(turn(step + 1)), b=complete(turn(step)))
        send(turn(step))

    finishing = complete(turn(last))
    run("b" * (ORDER.count("b") - cores), b=finishing)
    for core in range(cores):
        next(finishing)
        send(turn(last), (core,))

    for copy in halos:
        copy.wait_send()
    if geo.scatter:

        @pl.loop(0, bands)
        def _(s):
            for ih in range(2):
                target = out_ref.at[s, ih]
                pltpu.make_async_copy(target, target, piece_recv.at[s, ih]).wait()

        @pl.loop(0, windows)
        def _(w):
            for ih in range(2):
                for core in range(cores):
                    piece_copy(w, ih, core, "finish")

    else:
        copy = pltpu.make_async_copy(pieces, out_ref, load_sem.at[0])
        copy.start()
        copy.wait()


def forecast(geo, *args):
    tables = (
        jnp.asarray(geo.gather_table(), BF16),
        jnp.asarray(geo.order_table(), BF16),
        jnp.asarray(geo.position_table(), jnp.int32),
        jnp.asarray(geo.pixel_table(), BF16),
        jnp.asarray(geo.pick_table(), BF16),
    )
    features, width, cores, windows = geo.features, geo.width, geo.cores, geo.windows
    units = args[4].shape[1]
    fold_rows = geo.heads * (2 * LEVEL_SLOTS + geo.pixels)
    vmem = pltpu.VMEM
    dma = pltpu.SemaphoreType.DMA
    if geo.scatter:
        out_shape = (geo.bands, 2, BLOCK, BLOCK)
    else:
        out_shape = (windows, 2, cores, BLOCK, BLOCK)
    return pl.pallas_call(
        functools.partial(main_kernel, geo),
        out_shape=jax.ShapeDtypeStruct(out_shape, BF16),
        in_specs=[pl.BlockSpec(memory_space=pltpu.HBM)] * (len(args) + len(tables)),
        out_specs=pl.BlockSpec(memory_space=vmem if geo.scatter else pltpu.HBM),
        scratch_shapes=[
            vmem((geo.cols, geo.levels, geo.taken, features), BF16),
            vmem((2, geo.cols, geo.rows), jnp.int32),
            vmem((cores, 3, features, width), BF16),
            vmem((cores, width, features), BF16),
            vmem((cores, features, units), BF16),
            vmem((cores, units, features), BF16),
            *[vmem(one.shape, one.dtype) for one in args[6:]],
            *[vmem(one.shape, one.dtype) for one in tables],
            vmem((cores, fold_rows, features), BF16),
            vmem((windows, geo.half, features), BF16),
            vmem((windows, geo.half, features), BF16),
            vmem((windows, geo.half, features), BF16),
            vmem((geo.tokens, KEYS), F32),
            vmem((geo.tokens, cores * units), BF16),
            vmem((geo.levels - 1, cores * geo.heads * LEVEL_SLOTS, BLOCK), F32),
            vmem((geo.levels - 1, cores * geo.heads * geo.pixels, BLOCK), F32),
            vmem((cores, 3, windows, geo.half, width), BF16),
            vmem((2 * geo.pixels, features), BF16),
            vmem((windows, geo.tokens, features), F32),
            vmem((geo.pixels, BLOCK), F32),
            vmem((geo.slots, geo.pixels, BLOCK), F32),
            vmem((windows, 2, cores, BLOCK, BLOCK), BF16),
            vmem((BLOCK, BLOCK), F32),
            dma((geo.taken // 4 + 15,)),
            dma((6,)),
            dma((6,)),
            dma((windows,)),
            dma((windows,)),
            dma((windows, 2, cores)),
            dma((geo.bands, 2)),
        ],
        compiler_params=pltpu.CompilerParams(
            collective_id=0, has_side_effects=True, vmem_limit_bytes=30 * 2**20
        ),
    )(*[pltpu.with_memory_space_constraint(one, pltpu.HBM) for one in (*args, *tables)])


def assemble_kernel(isobars, run, got_ref, out_ref):
    bands = got_ref.shape[0]
    half_lat = WIN_LAT // 2
    groups = (isobars + 1) // 2
    rows = groups * 16
    whole_run = out_ref.shape[-1]
    tiles = whole_run // BLOCK
    extra = half_lat * run - BLOCK
    lane = lax.broadcasted_iota(jnp.int32, (rows, BLOCK), 1)

    @pl.loop(0, 2)
    def _(ih):
        for r in range(half_lat):
            out = [jnp.zeros((rows, BLOCK), F32) for _ in range(tiles)]
            for s in range(bands):
                base = (s * run + whole_run - run // 2) % whole_run
                piece = got_ref[s, ih].astype(F32)
                whole = min(run, BLOCK - r * run)
                parts = [(pltpu.roll(piece[:rows], (base - r * run) % BLOCK, 1), base, base + whole)]
                if whole < run:
                    rest = piece[rows:]
                    moved = [
                        pltpu.roll(rest, (base + whole - extra * k) % BLOCK, 1) for k in range(groups)
                    ]
                    parts.append((jnp.concatenate(moved, axis=0), base + whole, base + run))
                for value, low, high in parts:
                    spans = [(low, min(high, whole_run)), (max(low, whole_run) - whole_run, high - whole_run)]
                    for low, high in spans:
                        if high <= low:
                            continue
                        for t in range(low // BLOCK, (high - 1) // BLOCK + 1):
                            at = lane + t * BLOCK
                            out[t] = jnp.where(jnp.logical_and(at >= low, at < high), value, out[t])
            for t in range(tiles):
                value = out[t].reshape(2 * groups, 8, BLOCK)[:isobars]
                for flag in range(2):
                    top = ((half_lat if flag == 0 else 0) + r) * SQUARE_SPAN

                    @pl.when(ih == flag)
                    def _():
                        for v in range(2):
                            out_ref[v, :, top : top + SQUARE_SPAN, t * BLOCK : (t + 1) * BLOCK] = value[
                                :, v * SQUARE_SPAN : (v + 1) * SQUARE_SPAN
                            ]


def assemble(got, columns, isobars):
    bands = got.shape[0]
    run = columns * SQUARE_SPAN
    shape = (TARGET_QUANTITY // 2, isobars, WIN_LAT * SQUARE_SPAN, bands * run)
    return pl.pallas_call(
        functools.partial(assemble_kernel, isobars, run),
        out_shape=jax.ShapeDtypeStruct(shape, F32),
        compiler_params=pltpu.CompilerParams(vmem_limit_bytes=40 * 2**20),
    )(got)


def exchange(pieces, geo):
    half_lat = WIN_LAT // 2
    run = geo.cols * SQUARE_SPAN
    quantities = TARGET_QUANTITY // geo.cores
    rows = geo.slots * quantities * SQUARE_SPAN
    extra = half_lat * run - BLOCK
    lead = pieces.shape[:3]
    main = pieces[:, :, :, :rows].reshape(*lead, geo.slots, quantities, SQUARE_SPAN, BLOCK)
    rest = pieces[:, :, :, rows:, : extra * (geo.slots // 2)]
    rest = rest.reshape(*lead, 2, quantities, SQUARE_SPAN, geo.slots // 2, extra)
    rest = jnp.moveaxis(rest, 6, 3).reshape(*lead, geo.slots, quantities, SQUARE_SPAN, extra)
    maps = jnp.concatenate([main, rest], axis=-1)[:, :, :, : geo.isobars]
    maps = maps.reshape(*lead, geo.isobars, quantities, SQUARE_SPAN, half_lat, run)
    maps = jnp.transpose(maps, (2, 4, 3, 0, 1, 6, 5, 7))
    maps = maps.reshape(TARGET_QUANTITY, geo.isobars, geo.row_count * SQUARE_SPAN, run)
    maps = lax.all_to_all(maps, "var", split_axis=0, concat_axis=2, tiled=True)
    maps = jnp.roll(maps, half_lat * SQUARE_SPAN, 2)
    maps = lax.all_to_all(maps, "grid", split_axis=2, concat_axis=3, tiled=True)
    return jnp.roll(maps, -(run // 2), 3).astype(F32)


def local(
    tokens,
    key_mask,
    w_qkv,
    w_proj,
    w_up,
    w_down,
    level_query,
    w_dec_q,
    w_dec_kv,
    w_dec_o,
    decode_matrix,
):
    geo = Geometry(
        tokens, w_proj, level_query, decode_matrix, lax.axis_size("var"), lax.axis_size("grid")
    )
    pieces = forecast(
        geo,
        jnp.transpose(tokens, (1, 2, 0, 3)),
        key_mask.T,
        w_qkv,
        w_proj,
        w_up,
        w_down,
        level_query,
        w_dec_q,
        w_dec_kv,
        w_dec_o,
        decode_matrix.T,
    )
    if geo.scatter:
        return assemble(pieces, geo.cols, geo.isobars)
    return exchange(pieces, geo)


def solution(mesh):
    placed = (
        P("group", "grid", None, None),
        P("group", "grid"),
        P(None, None, "var"),
        P("var", None),
        P(None, "var"),
        P("var", None),
        P(),
        P(None, "var"),
        P(None, None, "var"),
        P("var", None),
        P(),
    )
    return jax.shard_map(
        local,
        mesh=mesh,
        in_specs=placed,
        out_specs=P("var", "group", "grid", None),
        check_vma=False,
    )
```

```python
import functools

import jax
import jax.numpy as jnp
import numpy as np
from jax import lax
from jax.experimental import pallas as pl
from jax.experimental.pallas import tpu as pltpu
from jax.sharding import PartitionSpec as P

HD = 64
TARGET_QUANTITY = 4
SQUARE_SPAN = 4
WIN_LAT = 6
EPSILON = 1e-05
BLOCK = 128
KEYS = 256
CHUNK = 256
LEVEL_SLOTS = 16
ORDER = "abaabbbbaaabbbbabaabbbb"
MESH = pl.DeviceIdType.MESH
NT = (((1,), (1,)), ((), ()))
F32 = jnp.float32
BF16 = jnp.bfloat16


def layer_norm(values):
    center = values - jnp.mean(values, axis=-1, keepdims=True)
    spread = jnp.mean(center * center, axis=-1, keepdims=True)
    return center * lax.rsqrt(spread + EPSILON)


def lane_bases(bands, run):
    return [(s * run + bands * run - run // 2) % (bands * run) for s in range(bands)]


class Geometry:
    def __init__(self, tokens, w_proj, level_query, decode_matrix, cores, bands):
        self.rows, self.cols, self.levels, self.features = tokens.shape
        self.cores, self.bands = cores, bands
        self.half_cols = self.cols // 2
        self.row_count = self.rows // cores
        self.windows = self.row_count // WIN_LAT
        self.taken = 8 * (-(-(self.row_count + WIN_LAT // 2) // 8))
        self.half_patches = WIN_LAT * self.half_cols
        self.half = 16 * (-(-(self.levels * self.half_patches) // 16))
        self.tokens = 2 * self.half
        self.patches = 2 * self.half_patches
        self.width = w_proj.shape[0]
        self.heads = self.width // HD
        self.isobars = level_query.shape[0]
        self.slots = self.isobars + self.isobars % 2
        self.pixels = decode_matrix.shape[1]
        self.run = self.cols * SQUARE_SPAN
        self.extra = WIN_LAT // 2 * self.run - BLOCK
        self.bases = lane_bases(bands, self.run)
        covered = [(base + lane) % BLOCK for base in self.bases for lane in range(self.extra)]
        self.scatter = (
            bands * WIN_LAT == self.rows
            and (bands * self.run) % BLOCK == 0
            and self.extra * (self.slots // 2) <= BLOCK
            and sorted(covered) == list(range(BLOCK))
        )

    def place(self, half, level, r, c):
        return half * self.half + level * self.half_patches + r * self.half_cols + c

    def each(self):
        for half in range(2):
            for level in range(self.levels):
                for r in range(WIN_LAT):
                    for c in range(self.half_cols):
                        yield half, level, r, c

    def gather_table(self):
        table = np.zeros((self.windows, self.half, self.half_cols * self.levels * self.taken), np.float32)
        for w in range(self.windows):
            for half, level, r, c in self.each():
                if half == 0:
                    source = (c * self.levels + level) * self.taken + WIN_LAT * w + WIN_LAT // 2 + r
                    table[w, self.place(0, level, r, c), source] = 1.0
        return table.reshape(self.windows * self.half, -1)

    def order_table(self):
        table = np.zeros((self.levels * BLOCK, self.tokens), np.float32)
        for half, level, r, c in self.each():
            patch = r * self.cols + (1 - half) * self.half_cols + c
            table[level * BLOCK + patch, self.place(half, level, r, c)] = 1.0
            if level > 0:
                table[level * BLOCK + patch, self.place(half, 0, r, c)] = -1.0
        return table

    def position_table(self):
        table = np.full((8, KEYS), -1, np.int32)
        table[0] = 0
        for half, level, r, c in self.each():
            at = self.place(half, level, r, c)
            table[0, at] = r
            table[1 + half, at] = c + half * self.half_cols
        return table

    def pixel_table(self):
        table = np.zeros((self.pixels, self.pixels), np.float32)
        own = TARGET_QUANTITY // self.cores
        for v in range(TARGET_QUANTITY):
            for a in range(SQUARE_SPAN):
                for b in range(SQUARE_SPAN):
                    target = ((v // own * SQUARE_SPAN + b) * own + v % own) * SQUARE_SPAN + a
                    table[target, (v * SQUARE_SPAN + a) * SQUARE_SPAN + b] = 1.0
        return table

    def pick_table(self):
        half_lat = WIN_LAT // 2
        run = self.cols * SQUARE_SPAN
        extra = half_lat * run - BLOCK
        picks = np.zeros((SQUARE_SPAN, BLOCK, 4 * BLOCK), np.float32)
        for ih in range(2):
            for q in range(half_lat * run):
                r, rest = divmod(q, run)
                column, b = divmod(rest, SQUARE_SPAN)
                source = (half_lat * ih + r) * self.cols + column
                if q < BLOCK:
                    picks[b, source, ih * BLOCK + q] = 1.0
                else:
                    for k in range(self.slots // 2):
                        picks[b, source, (2 + ih) * BLOCK + extra * k + q - BLOCK] = 1.0
        return picks


def fold_decoder(lq, wq, wkv_ref, wo, dm, perm, out_ref):
    width = wq.shape[1]
    heads = width // HD
    dquery = jnp.dot(lq, wq, preferred_element_type=F32) * HD ** (-0.5)
    d_hi = dquery.astype(BF16)
    d_lo = (dquery - d_hi.astype(F32)).astype(BF16)
    count = LEVEL_SLOTS * heads
    row = lax.broadcasted_iota(jnp.int32, (count, dquery.shape[0]), 0)
    slot = lax.broadcasted_iota(jnp.int32, (count, dquery.shape[0]), 1)
    spread = (row // heads == slot).astype(F32).astype(BF16)
    row = lax.broadcasted_iota(jnp.int32, (count, width), 0)
    mine = row % heads == lax.broadcasted_iota(jnp.int32, (count, width), 1) // HD
    q_hi = jnp.dot(spread, d_hi, preferred_element_type=F32)
    q_hi = jnp.where(mine, q_hi, 0.0).astype(BF16)
    q_lo = jnp.dot(spread, d_lo, preferred_element_type=F32)
    q_lo = jnp.where(mine, q_lo, 0.0).astype(BF16)
    wk = wkv_ref[0]
    g = lax.dot_general(q_hi, wk, NT, preferred_element_type=F32)
    g = g + lax.dot_general(q_lo, wk, NT, preferred_element_type=F32)
    g_hi = g.astype(BF16)
    out_ref[0, 0:count, :] = g_hi
    out_ref[0, count : 2 * count, :] = (g - g_hi.astype(F32)).astype(BF16)
    dm_hi = dm.astype(BF16)
    dm_lo = (dm - dm_hi.astype(F32)).astype(BF16)
    dm_hi = jnp.dot(perm, dm_hi, preferred_element_type=F32).astype(BF16)
    dm_lo = jnp.dot(perm, dm_lo, preferred_element_type=F32).astype(BF16)
    m_t = lax.dot_general(dm_hi, wo, NT, preferred_element_type=F32)
    m_t = m_t + lax.dot_general(dm_lo, wo, NT, preferred_element_type=F32)
    pixels = m_t.shape[0]
    stacked = jnp.concatenate([m_t] * heads, axis=0)
    row_head = lax.broadcasted_iota(jnp.int32, stacked.shape, 0) // pixels
    lane_head = lax.broadcasted_iota(jnp.int32, stacked.shape, 1) // HD
    stacked = jnp.where(row_head == lane_head, stacked, 0.0)
    s_hi = stacked.astype(BF16)
    s_lo = (stacked - s_hi.astype(F32)).astype(BF16)
    wv = wkv_ref[1]
    n_t = lax.dot_general(s_hi, wv, NT, preferred_element_type=F32)
    n_t = n_t + lax.dot_general(s_lo, wv, NT, preferred_element_type=F32)
    out_ref[0, 2 * count :, :] = n_t.astype(BF16)


def main_kernel(
    geo,
    tok_ref,
    mask_ref,
    wqkv_ref,
    wproj_ref,
    wup_ref,
    wdown_ref,
    lq_ref,
    wq_ref,
    wkv_ref,
    wo_ref,
    dm_ref,
    gather_ref,
    order_ref,
    position_ref,
    perm_ref,
    pick_ref,
    out_ref,
    raw,
    marks,
    qkv,
    proj,
    up,
    down,
    lq,
    wq,
    wkv,
    wo,
    dm,
    gather,
    order,
    position,
    perm,
    pick,
    fold,
    first,
    own,
    halo,
    differs,
    hid,
    dw,
    du,
    ready,
    fold_base,
    x_one,
    base_pix,
    pix,
    pieces,
    checked,
    load_sem,
    weight_send,
    weight_recv,
    halo_send,
    halo_recv,
    piece_send,
    piece_recv,
):
    group, grid, var = (lax.axis_index(name) for name in ("group", "grid", "var"))
    bands, cores, windows, half = geo.bands, geo.cores, geo.windows, geo.half
    features, levels, width, heads = geo.features, geo.levels, geo.width, geo.heads
    sibling = (group, grid, lax.rem(var + 1, cores))

    def turn(step, column=grid):
        near = column * cores // bands == var
        rest = lax.rem(step + column + windows - 2, windows - 1)
        return jnp.where(near, jnp.where(step == 0, windows - 1, rest), step)

    east_grid = lax.rem(grid + 1, bands)
    west = (group, lax.rem(grid + bands - 1, bands), var)
    east = (group, east_grid, var)
    barrier = pltpu.get_barrier_semaphore()
    if geo.scatter:
        peers = bands * cores
        me = grid * cores + var

        @pl.loop(1, peers)
        def _(step):
            peer = lax.rem(me + step, peers)
            pl.semaphore_signal(
                barrier, inc=1, device_id=(group, peer // cores, lax.rem(peer, cores)), device_id_type=MESH
            )

        greeted = peers - 1
    else:
        for peer in (sibling, west, east):
            pl.semaphore_signal(barrier, inc=1, device_id=peer, device_id_type=MESH)
        greeted = 3

    loads = []

    def load(source, target):
        copy = pltpu.make_async_copy(source, target, load_sem.at[len(loads)])
        copy.start()
        loads.append(copy)
        return copy

    gather_load = load(gather_ref, gather)
    tiles = geo.rows // 8
    first_tile = var * (geo.row_count // 8)
    slabs = []
    for s in range(geo.taken // 8):
        tile = lax.rem(first_tile + s, tiles)
        for h in (0, 1):
            some = slice(h * geo.half_cols, (h + 1) * geo.half_cols)
            slabs.append(
                load(
                    tok_ref.at[some, :, pl.ds(pl.multiple_of(tile * 8, 8), 8), :],
                    raw.at[some, :, 8 * s : 8 * s + 8, :],
                )
            )
    fold_loads = [
        load(a, b)
        for a, b in ((lq_ref, lq), (wq_ref, wq), (wkv_ref, wkv), (wo_ref, wo), (dm_ref, dm), (perm_ref, perm))
    ]
    late_loads = [
        load(a, b)
        for a, b in (
            (mask_ref, marks.at[0]),
            (wqkv_ref, qkv.at[0]),
            (wproj_ref, proj.at[0]),
            (wup_ref, up.at[0]),
            (wdown_ref, down.at[0]),
            (position_ref, position),
            (order_ref, order),
            (pick_ref, pick),
        )
    ]

    depth = geo.half_cols * levels * geo.taken

    def collect(h, w, target):
        slab = raw[h * geo.half_cols : (h + 1) * geo.half_cols].reshape(depth, features)
        picked = gather[pl.ds(pl.multiple_of(w * half, 16), half), :]
        target[w] = jnp.dot(picked, slab, preferred_element_type=F32).astype(BF16)

    gather_load.wait()
    for copy in slabs[1::2]:
        copy.wait()
    collect(1, turn(0, east_grid), first)
    pl.semaphore_wait(barrier, greeted)

    def remote(source, target, send, recv, peer):
        copy = pltpu.make_async_remote_copy(
            src_ref=source, dst_ref=target, send_sem=send, recv_sem=recv, device_id=peer, device_id_type=MESH
        )
        copy.start()
        return copy

    copies = [remote(mask_ref, marks.at[1], weight_send.at[0], weight_recv.at[0], east)]
    halos = []

    def pass_on(step):
        w = turn(step, east_grid)
        halos.append(remote(first.at[w], halo.at[w], halo_send.at[w], halo_recv.at[w], east))

    pass_on(0)
    for n, (source, target) in enumerate(((wqkv_ref, qkv), (wproj_ref, proj), (wup_ref, up), (wdown_ref, down))):
        copies.append(remote(source, target.at[1], weight_send.at[n + 1], weight_recv.at[n + 1], sibling))

    for step in range(1, windows):
        collect(1, turn(step, east_grid), first)
    for copy in slabs[0::2]:
        copy.wait()
    for step in range(windows):
        collect(0, turn(step), own)
    for step in range(1, windows):
        pass_on(step)
    for copy in fold_loads:
        copy.wait()
    fold_decoder(lq[...], wq[...], wkv, wo[...], dm[...], perm[...], fold)

    tokens = geo.tokens
    q_pos = lax.broadcasted_iota(jnp.int32, (tokens, KEYS), 0)
    k_pos = lax.broadcasted_iota(jnp.int32, (tokens, KEYS), 1)
    diagonal = q_pos == k_pos

    def region_of(pos):
        pos = jnp.where(pos >= half, pos - half, pos)
        for level in range(levels - 1, 0, -1):
            start = geo.half_patches * level
            pos = jnp.where(pos >= start, pos - start, pos)
        return pos >= geo.half_patches // 2

    differs[...] = jnp.where(region_of(q_pos) != region_of(k_pos), -1e30, 0.0)
    lane_head = lax.broadcasted_iota(jnp.int32, (tokens, width), 1) // HD
    lane_head_keys = lax.broadcasted_iota(jnp.int32, (KEYS, width), 1) // HD

    for copy in late_loads:
        copy.wait()
    copies.append(remote(fold.at[0], fold.at[1], weight_send.at[5], weight_recv.at[5], sibling))

    count = heads * LEVEL_SLOTS
    pixels = geo.pixels
    row_size = pixels // cores // SQUARE_SPAN
    rows = geo.slots * row_size
    half_lat = WIN_LAT // 2
    extra = half_lat * geo.cols * SQUARE_SPAN - BLOCK
    pix[geo.isobars :] = jnp.zeros((geo.slots - geo.isobars, pixels, BLOCK), F32)
    units = up.shape[2]

    def piece_copy(w, ih, core, action):
        band = lax.rem(var * windows + w + ih, bands)
        here = jnp.logical_and(band == grid, core == var)
        source, target = pieces.at[w, ih, core], out_ref.at[grid, ih]

        @pl.when(here)
        def _():
            if action == "start":
                pltpu.make_async_copy(source, target, piece_recv.at[grid, ih]).start()

        @pl.when(jnp.logical_not(here))
        def _():
            if action == "start":
                pltpu.make_async_remote_copy(
                    src_ref=source,
                    dst_ref=target,
                    send_sem=piece_send.at[w, ih, core],
                    recv_sem=piece_recv.at[grid, ih],
                    device_id=(group, band, core),
                    device_id_type=MESH,
                ).start()
            else:
                pltpu.make_async_copy(source, source, piece_send.at[w, ih, core]).wait()

    def arrive(w):
        pltpu.make_async_copy(halo.at[w], halo.at[w], halo_recv.at[w]).wait()

    def send(w, some=range(cores)):
        for core in some:
            checked[...] = pieces[w, :, core].astype(F32).max(axis=0)
        if geo.scatter:
            for core in some:
                for ih in range(2):
                    piece_copy(w, ih, core, "start")

    def attend(w):
        x = jnp.concatenate([own[w], halo[w]], axis=0).astype(F32)
        n1 = layer_norm(x[half:]).astype(BF16)
        target = position[0:1, :] + (var * geo.row_count + WIN_LAT * w + half_lat)
        target = jnp.where(target >= geo.rows, target - geo.rows, target)
        there = lax.broadcasted_iota(jnp.int32, (geo.rows, KEYS), 0) == target
        there = there.astype(F32).astype(BF16)
        opened = jnp.zeros((1, KEYS), F32)
        column = lax.broadcasted_iota(jnp.int32, (geo.cols, KEYS), 0)
        for h in range(2):
            seen = (marks[h] > 0).astype(F32).astype(BF16)
            seen = jnp.dot(seen, there, preferred_element_type=F32)
            seen = jnp.where(column == position[1 + h : 2 + h, :], seen, 0.0)
            opened = opened + jnp.sum(seen, axis=0, keepdims=True)
        allowed = jnp.logical_or(jnp.broadcast_to(opened, diagonal.shape) > 0.5, diagonal)
        cut = jnp.logical_and(var == cores - 1, w == windows - 1)
        bias = jnp.where(allowed, 0.0, -1e30) + differs[...] * jnp.where(cut, 1.0, 0.0)
        yield
        scores, values = [], []
        for s in range(cores):
            q, k, v = (
                jnp.concatenate(
                    [ready[s, i, w], jnp.dot(n1, qkv[s, i], preferred_element_type=F32).astype(BF16)], axis=0
                )
                for i in range(3)
            )
            q = q * jnp.asarray(HD ** (-0.5), BF16)
            tail = jnp.zeros((KEYS - tokens, width), BF16)
            k = jnp.concatenate([k, tail], axis=0)
            values.append(jnp.concatenate([v, tail], axis=0))
            q_all = jnp.concatenate(
                [jnp.where(lane_head == h, q, jnp.zeros_like(q)) for h in range(heads)], axis=0
            )
            yield
            scores.append(lax.dot_general(q_all, k, NT, preferred_element_type=F32))
            yield
        attended = x
        for s in range(cores):
            weights = []
            for h in range(heads):
                one = scores[s][h * tokens : (h + 1) * tokens] + bias
                peak = jnp.max(one, axis=-1, keepdims=True)
                e = jnp.exp(one - peak)
                total = jnp.sum(e, axis=-1, keepdims=True)
                weights.append((e * (1.0 / total)).astype(BF16))
            weights = jnp.concatenate(weights, axis=1)
            v = values[s]
            v_all = jnp.concatenate(
                [jnp.where(lane_head_keys == h, v, jnp.zeros_like(v)) for h in range(heads)], axis=0
            )
            context = jnp.dot(weights, v_all, preferred_element_type=F32).astype(BF16)
            yield
            attended = attended + jnp.dot(context, proj[s], preferred_element_type=F32)
            if s == cores - 1:
                x_one[w] = attended
            yield

    def finish(w):
        n2 = layer_norm(x_one[w]).astype(BF16)
        yield
        for s in range(cores):
            for c in range(0, units, CHUNK):
                one = jnp.dot(n2, up[s, :, c : c + CHUNK], preferred_element_type=F32)
                one = 0.5 * one * (1.0 + lax.erf(one * 2.0 ** (-0.5)))
                hid[:, s * units + c : s * units + c + CHUNK] = one.astype(BF16)
                yield
        latent = x_one[w] + jnp.dot(
            hid[...], down[...].reshape(cores * units, features), preferred_element_type=F32
        )
        yield
        n3 = layer_norm(latent.astype(BF16).astype(F32)).astype(BF16)
        n3 = jnp.dot(order[...], n3, preferred_element_type=F32).astype(BF16)
        n3, others = n3[:BLOCK], n3[BLOCK:]
        yield
        base = lax.dot_general(fold_base[...], n3, NT, preferred_element_type=F32)
        base_pix[...] = base[:pixels] + base[pixels:]
        for s in range(cores):
            g = lax.dot_general(fold[s, 0 : 2 * count, :], others, NT, preferred_element_type=F32)
            g = g[:count] + g[count:]
            scores = [jnp.zeros((count, BLOCK), F32)]
            scores += [g[:, j * BLOCK : (j + 1) * BLOCK] for j in range(levels - 1)]
            peak = functools.reduce(jnp.maximum, scores)
            e = [jnp.exp(one - peak) for one in scores]
            inverse = 1.0 / sum(e)
            u = lax.dot_general(fold[s, 2 * count :, :], others, NT, preferred_element_type=F32)
            for j in range(levels - 1):
                dw[j, s * count : (s + 1) * count, :] = e[j + 1] * inverse
                du[j, s * heads * pixels : (s + 1) * heads * pixels, :] = u[:, j * BLOCK : (j + 1) * BLOCK]
        yield

    def paint(w):
        low = pixels // cores
        lane = lax.broadcasted_iota(jnp.int32, (2 * row_size, BLOCK), 1) - lane_base
        lane = jnp.where(lane < 0, lane + BLOCK, lane)
        for core in range(cores):
            top = core * low
            for first_level in range(0, geo.isobars, 5):
                some = range(first_level, min(first_level + 5, geo.isobars))
                totals = [base_pix[top : top + low, :] for _ in some]
                for s in range(cores):
                    for h in range(heads):
                        for j in range(levels - 1):
                            at = (s * heads + h) * pixels + top
                            value = du[j, at : at + low, :]
                            for n, level in enumerate(some):
                                row = s * count + level * heads + h
                                totals[n] = totals[n] + dw[j, row : row + 1, :] * value
                for n, level in enumerate(some):
                    pix[level, top : top + low, :] = totals[n]
            total = jnp.zeros((rows, 4 * BLOCK), F32)
            for b in range(SQUARE_SPAN):
                at = top + b * row_size
                part = pix[:, at : at + row_size, :].reshape(rows, BLOCK)
                total = total + jnp.dot(part.astype(BF16), pick[b], preferred_element_type=F32)
            for ih in range(2):
                left = jnp.zeros((2 * row_size, BLOCK), F32)
                for k in range(geo.slots // 2):
                    at = slice(2 * row_size * k, 2 * row_size * (k + 1))
                    inside = jnp.logical_and(lane >= extra * k, lane < extra * (k + 1))
                    left = jnp.where(inside, total[at, (2 + ih) * BLOCK : (3 + ih) * BLOCK], left)
                main = total[:, ih * BLOCK : (ih + 1) * BLOCK]
                pieces[w, ih, core] = jnp.concatenate([main, left], axis=0).astype(BF16)
            yield

    def run(order="", **steps):
        for name in order:
            next(steps[name])

    mask_copy, qkv_copy, proj_copy, up_copy, down_copy, fold_copy = copies
    for copy in (mask_copy, qkv_copy, proj_copy):
        copy.wait()
    lane_base = lax.rem(grid * geo.run + bands * geo.run - geo.run // 2, BLOCK) if geo.scatter else 0
    if geo.scatter:
        for b in range(SQUARE_SPAN):
            for part in range(4):
                lanes = slice(part * BLOCK, (part + 1) * BLOCK)
                pick[b, :, lanes] = pltpu.roll(pick[b, :, lanes].astype(F32), lane_base, 1).astype(BF16)
    n_own = layer_norm(own[...].reshape(windows * half, features).astype(F32)).astype(BF16)
    for s in range(cores):
        for i in range(3):
            one = jnp.dot(n_own, qkv[s, i], preferred_element_type=F32).astype(BF16)
            ready[s, i] = one.reshape(windows, half, width)
    arrive(turn(0))
    run("a" * ORDER.count("a"), a=attend(turn(0)))
    for copy in (up_copy, down_copy, fold_copy):
        copy.wait()
    whole = jnp.zeros((pixels, features), F32)
    for s in range(cores):
        for h in range(heads):
            top = 2 * count + h * pixels
            whole = whole + fold[s, top : top + pixels, :].astype(F32)
    whole_hi = whole.astype(BF16)
    fold_base[0:pixels, :] = whole_hi
    fold_base[pixels:, :] = (whole - whole_hi.astype(F32)).astype(BF16)

    last = windows - 1

    def complete(w):
        yield from finish(w)
        yield from paint(w)

    @pl.loop(0, last)
    def _(step):
        arrive(turn(step + 1))
        run(ORDER, a=attend(turn(step + 1)), b=complete(turn(step)))
        send(turn(step))

    finishing = complete(turn(last))
    run("b" * (ORDER.count("b") - cores), b=finishing)
    for core in range(cores):
        next(finishing)
        send(turn(last), (core,))

    for copy in halos:
        copy.wait_send()
    if geo.scatter:

        @pl.loop(0, bands)
        def _(s):
            for ih in range(2):
                target = out_ref.at[s, ih]
                pltpu.make_async_copy(target, target, piece_recv.at[s, ih]).wait()

        @pl.loop(0, windows)
        def _(w):
            for ih in range(2):
                for core in range(cores):
                    piece_copy(w, ih, core, "finish")

    else:
        copy = pltpu.make_async_copy(pieces, out_ref, load_sem.at[0])
        copy.start()
        copy.wait()


def forecast(geo, *args):
    tables = (
        jnp.asarray(geo.gather_table(), BF16),
        jnp.asarray(geo.order_table(), BF16),
        jnp.asarray(geo.position_table(), jnp.int32),
        jnp.asarray(geo.pixel_table(), BF16),
        jnp.asarray(geo.pick_table(), BF16),
    )
    features, width, cores, windows = geo.features, geo.width, geo.cores, geo.windows
    units = args[4].shape[1]
    fold_rows = geo.heads * (2 * LEVEL_SLOTS + geo.pixels)
    vmem = pltpu.VMEM
    dma = pltpu.SemaphoreType.DMA
    if geo.scatter:
        out_shape = (geo.bands, 2, BLOCK, BLOCK)
    else:
        out_shape = (windows, 2, cores, BLOCK, BLOCK)
    return pl.pallas_call(
        functools.partial(main_kernel, geo),
        out_shape=jax.ShapeDtypeStruct(out_shape, BF16),
        in_specs=[pl.BlockSpec(memory_space=pltpu.HBM)] * (len(args) + len(tables)),
        out_specs=pl.BlockSpec(memory_space=vmem if geo.scatter else pltpu.HBM),
        scratch_shapes=[
            vmem((geo.cols, geo.levels, geo.taken, features), BF16),
            vmem((2, geo.cols, geo.rows), jnp.int32),
            vmem((cores, 3, features, width), BF16),
            vmem((cores, width, features), BF16),
            vmem((cores, features, units), BF16),
            vmem((cores, units, features), BF16),
            *[vmem(one.shape, one.dtype) for one in args[6:]],
            *[vmem(one.shape, one.dtype) for one in tables],
            vmem((cores, fold_rows, features), BF16),
            vmem((windows, geo.half, features), BF16),
            vmem((windows, geo.half, features), BF16),
            vmem((windows, geo.half, features), BF16),
            vmem((geo.tokens, KEYS), F32),
            vmem((geo.tokens, cores * units), BF16),
            vmem((geo.levels - 1, cores * geo.heads * LEVEL_SLOTS, BLOCK), F32),
            vmem((geo.levels - 1, cores * geo.heads * geo.pixels, BLOCK), F32),
            vmem((cores, 3, windows, geo.half, width), BF16),
            vmem((2 * geo.pixels, features), BF16),
            vmem((windows, geo.tokens, features), F32),
            vmem((geo.pixels, BLOCK), F32),
            vmem((geo.slots, geo.pixels, BLOCK), F32),
            vmem((windows, 2, cores, BLOCK, BLOCK), BF16),
            vmem((BLOCK, BLOCK), F32),
            dma((geo.taken // 4 + 15,)),
            dma((6,)),
            dma((6,)),
            dma((windows,)),
            dma((windows,)),
            dma((windows, 2, cores)),
            dma((geo.bands, 2)),
        ],
        compiler_params=pltpu.CompilerParams(
            collective_id=0, has_side_effects=True, vmem_limit_bytes=30 * 2**20
        ),
    )(*[pltpu.with_memory_space_constraint(one, pltpu.HBM) for one in (*args, *tables)])


def assemble_kernel(isobars, run, got_ref, out_ref, out, sems):
    bands = got_ref.shape[0]
    half_lat = WIN_LAT // 2
    groups = (isobars + 1) // 2
    tiles = out.shape[-1] // BLOCK
    extra = half_lat * run - BLOCK
    bases = lane_bases(bands, run)
    lane = lax.broadcasted_iota(jnp.int32, (1, BLOCK), 1)
    sublane = lax.broadcasted_iota(jnp.int32, (1, 8, BLOCK), 1)

    def around(start, length):
        start = start % BLOCK
        if start + length <= BLOCK:
            return jnp.logical_and(lane >= start, lane < start + length)
        return jnp.logical_or(lane >= start, lane < start + length - BLOCK)

    def put(merged, value, start, length):
        while length > 0:
            start = start % (tiles * BLOCK)
            tile, part = start // BLOCK, min(length, BLOCK - start % BLOCK)
            old = merged[tile]
            merged[tile] = value if old is None else jnp.where(around(start, part), value, old)
            start, length = start + part, length - part

    copies = []
    middle = (groups + 1) // 2
    for first, last in ((0, middle), (middle, groups)):
        low, high = 2 * first, min(2 * last, isobars)
        found = {}
        for ih in range(2):
            pieces = [got_ref[s, ih, 16 * first : 16 * last, :].astype(F32) for s in range(bands)]
            rests = [got_ref[s, ih, 16 * groups : 16 * groups + 16, :].astype(F32) for s in range(bands)]
            left = []
            for k in range(first, last):
                one = rests[0]
                for s in range(1, bands):
                    one = jnp.where(around(bases[s] + extra * k, extra), rests[s], one)
                left.append(pltpu.roll(one, (-extra * k) % BLOCK, 1) if k > 0 else one)
            left = jnp.concatenate(left, axis=0)
            for r in range(half_lat):
                merged = [None] * tiles
                for s in range(bands):
                    put(merged, pieces[s], bases[s] + run * r, min(run, BLOCK - run * r))
                if run * (r + 1) > BLOCK:
                    for s in range(bands):
                        put(merged, left, bases[s] + BLOCK, run * (r + 1) - BLOCK)
                if r > 0:
                    merged = [pltpu.roll(one, BLOCK - run * r, 1) for one in merged]
                    merged = [
                        jnp.where(lane < BLOCK - run * r, merged[t], merged[(t + 1) % tiles])
                        for t in range(tiles)
                    ]
                found[(1 - ih) * half_lat + r] = merged
        for top in range(0, 2 * half_lat, 2):
            for t in range(tiles):
                upper = found[top][t].reshape(-1, 8, BLOCK)
                lower = found[top + 1][t].reshape(-1, 8, BLOCK)
                some = (
                    jnp.where(sublane < 4, upper, pltpu.roll(lower, 4, 1)),
                    jnp.where(sublane < 4, pltpu.roll(upper, 4, 1), lower),
                )
                for v in range(2):
                    out[v, low:high, 4 * top : 4 * top + 8, t * BLOCK : (t + 1) * BLOCK] = some[v][: high - low]
        for v in range(2):
            copy = pltpu.make_async_copy(
                out.at[v, low:high], out_ref.at[v, low:high], sems.at[len(copies)]
            )
            copy.start()
            copies.append(copy)
    for copy in copies:
        copy.wait()


def assemble(got, geo):
    shape = (TARGET_QUANTITY // geo.cores, geo.isobars, WIN_LAT * SQUARE_SPAN, geo.bands * geo.run)
    return pl.pallas_call(
        functools.partial(assemble_kernel, geo.isobars, geo.run),
        out_shape=jax.ShapeDtypeStruct(shape, F32),
        out_specs=pl.BlockSpec(memory_space=pltpu.HBM),
        scratch_shapes=[pltpu.VMEM(shape, F32), pltpu.SemaphoreType.DMA((4,))],
        compiler_params=pltpu.CompilerParams(vmem_limit_bytes=40 * 2**20),
    )(got)


def exchange(pieces, geo):
    half_lat = WIN_LAT // 2
    run = geo.cols * SQUARE_SPAN
    quantities = TARGET_QUANTITY // geo.cores
    rows = geo.slots * quantities * SQUARE_SPAN
    extra = half_lat * run - BLOCK
    lead = pieces.shape[:3]
    main = pieces[:, :, :, :rows].reshape(*lead, geo.slots, quantities, SQUARE_SPAN, BLOCK)
    rest = pieces[:, :, :, rows:, : extra * (geo.slots // 2)]
    rest = rest.reshape(*lead, 2, quantities, SQUARE_SPAN, geo.slots // 2, extra)
    rest = jnp.moveaxis(rest, 6, 3).reshape(*lead, geo.slots, quantities, SQUARE_SPAN, extra)
    maps = jnp.concatenate([main, rest], axis=-1)[:, :, :, : geo.isobars]
    maps = maps.reshape(*lead, geo.isobars, quantities, SQUARE_SPAN, half_lat, run)
    maps = jnp.transpose(maps, (2, 4, 3, 0, 1, 6, 5, 7))
    maps = maps.reshape(TARGET_QUANTITY, geo.isobars, geo.row_count * SQUARE_SPAN, run)
    maps = lax.all_to_all(maps, "var", split_axis=0, concat_axis=2, tiled=True)
    maps = jnp.roll(maps, half_lat * SQUARE_SPAN, 2)
    maps = lax.all_to_all(maps, "grid", split_axis=2, concat_axis=3, tiled=True)
    return jnp.roll(maps, -(run // 2), 3).astype(F32)


def local(
    tokens,
    key_mask,
    w_qkv,
    w_proj,
    w_up,
    w_down,
    level_query,
    w_dec_q,
    w_dec_kv,
    w_dec_o,
    decode_matrix,
):
    geo = Geometry(
        tokens, w_proj, level_query, decode_matrix, lax.axis_size("var"), lax.axis_size("grid")
    )
    pieces = forecast(
        geo,
        jnp.transpose(tokens, (1, 2, 0, 3)),
        key_mask.T,
        w_qkv,
        w_proj,
        w_up,
        w_down,
        level_query,
        w_dec_q,
        w_dec_kv,
        w_dec_o,
        decode_matrix.T,
    )
    if geo.scatter:
        return assemble(pieces, geo)
    return exchange(pieces, geo)


def solution(mesh):
    placed = (
        P("group", "grid", None, None),
        P("group", "grid"),
        P(None, None, "var"),
        P("var", None),
        P(None, "var"),
        P("var", None),
        P(),
        P(None, "var"),
        P(None, None, "var"),
        P("var", None),
        P(),
    )
    return jax.shard_map(
        local,
        mesh=mesh,
        in_specs=placed,
        out_specs=P("var", "group", "grid", None),
        check_vma=False,
    )
```

```python
import functools

import jax
import jax.numpy as jnp
import numpy as np
from jax import lax
from jax.experimental import pallas as pl
from jax.experimental.pallas import tpu as pltpu
from jax.sharding import PartitionSpec as P

HD = 64
TARGET_QUANTITY = 4
SQUARE_SPAN = 4
WIN_LAT = 6
EPSILON = 1e-05
BLOCK = 128
KEYS = 256
CHUNK = 256
LEVEL_SLOTS = 16
ORDER = "aabaabbbbaabbbbabababbb"
MESH = pl.DeviceIdType.MESH
NT = (((1,), (1,)), ((), ()))
F32 = jnp.float32
BF16 = jnp.bfloat16


def layer_norm(values):
    center = values - jnp.mean(values, axis=-1, keepdims=True)
    spread = jnp.mean(center * center, axis=-1, keepdims=True)
    return center * lax.rsqrt(spread + EPSILON)


def lane_bases(bands, run):
    return [(s * run + bands * run - run // 2) % (bands * run) for s in range(bands)]


class Geometry:
    def __init__(self, tokens, w_proj, level_query, decode_matrix, cores, bands):
        self.rows, self.cols, self.levels, self.features = tokens.shape
        self.cores, self.bands = cores, bands
        self.half_cols = self.cols // 2
        self.row_count = self.rows // cores
        self.windows = self.row_count // WIN_LAT
        self.taken = 8 * (-(-(self.row_count + WIN_LAT // 2) // 8))
        self.half_patches = WIN_LAT * self.half_cols
        self.half = 16 * (-(-(self.levels * self.half_patches) // 16))
        self.tokens = 2 * self.half
        self.patches = 2 * self.half_patches
        self.width = w_proj.shape[0]
        self.heads = self.width // HD
        self.isobars = level_query.shape[0]
        self.slots = self.isobars + self.isobars % 2
        self.pixels = decode_matrix.shape[1]
        self.run = self.cols * SQUARE_SPAN
        self.extra = WIN_LAT // 2 * self.run - BLOCK
        self.bases = lane_bases(bands, self.run)
        covered = [(base + lane) % BLOCK for base in self.bases for lane in range(self.extra)]
        self.scatter = (
            bands * WIN_LAT == self.rows
            and (bands * self.run) % BLOCK == 0
            and self.extra * (self.slots // 2) <= BLOCK
            and sorted(covered) == list(range(BLOCK))
        )

    def place(self, half, level, r, c):
        return half * self.half + level * self.half_patches + r * self.half_cols + c

    def each(self):
        for half in range(2):
            for level in range(self.levels):
                for r in range(WIN_LAT):
                    for c in range(self.half_cols):
                        yield half, level, r, c

    def order_table(self):
        table = np.zeros((self.levels * BLOCK, self.tokens), np.float32)
        for half, level, r, c in self.each():
            patch = r * self.cols + (1 - half) * self.half_cols + c
            table[level * BLOCK + patch, self.place(half, level, r, c)] = 1.0
            if level > 0:
                table[level * BLOCK + patch, self.place(half, 0, r, c)] = -1.0
        return table

    def position_table(self):
        table = np.full((8, KEYS), -1, np.int32)
        table[0] = 0
        for half, level, r, c in self.each():
            at = self.place(half, level, r, c)
            table[0, at] = r
            table[1 + half, at] = c + half * self.half_cols
        return table

    def pixel_table(self):
        table = np.zeros((self.pixels, self.pixels), np.float32)
        own = TARGET_QUANTITY // self.cores
        for v in range(TARGET_QUANTITY):
            for a in range(SQUARE_SPAN):
                for b in range(SQUARE_SPAN):
                    target = ((v // own * SQUARE_SPAN + b) * own + v % own) * SQUARE_SPAN + a
                    table[target, (v * SQUARE_SPAN + a) * SQUARE_SPAN + b] = 1.0
        return table

    def pick_table(self):
        half_lat = WIN_LAT // 2
        run = self.cols * SQUARE_SPAN
        extra = half_lat * run - BLOCK
        picks = np.zeros((SQUARE_SPAN, BLOCK, 4 * BLOCK), np.float32)
        for ih in range(2):
            for q in range(half_lat * run):
                r, rest = divmod(q, run)
                column, b = divmod(rest, SQUARE_SPAN)
                source = (half_lat * ih + r) * self.cols + column
                if q < BLOCK:
                    picks[b, source, ih * BLOCK + q] = 1.0
                else:
                    for k in range(self.slots // 2):
                        picks[b, source, (2 + ih) * BLOCK + extra * k + q - BLOCK] = 1.0
        return picks


def fold_decoder(lq, wq, wkv_ref, wo, dm, perm, out_ref):
    width = wq.shape[1]
    heads = width // HD
    dquery = jnp.dot(lq, wq, preferred_element_type=F32) * HD ** (-0.5)
    d_hi = dquery.astype(BF16)
    d_lo = (dquery - d_hi.astype(F32)).astype(BF16)
    count = LEVEL_SLOTS * heads
    row = lax.broadcasted_iota(jnp.int32, (count, dquery.shape[0]), 0)
    slot = lax.broadcasted_iota(jnp.int32, (count, dquery.shape[0]), 1)
    spread = (row // heads == slot).astype(F32).astype(BF16)
    row = lax.broadcasted_iota(jnp.int32, (count, width), 0)
    mine = row % heads == lax.broadcasted_iota(jnp.int32, (count, width), 1) // HD
    q_hi = jnp.dot(spread, d_hi, preferred_element_type=F32)
    q_hi = jnp.where(mine, q_hi, 0.0).astype(BF16)
    q_lo = jnp.dot(spread, d_lo, preferred_element_type=F32)
    q_lo = jnp.where(mine, q_lo, 0.0).astype(BF16)
    wk = wkv_ref[0]
    g = lax.dot_general(q_hi, wk, NT, preferred_element_type=F32)
    g = g + lax.dot_general(q_lo, wk, NT, preferred_element_type=F32)
    g_hi = g.astype(BF16)
    out_ref[0, 0:count, :] = g_hi
    out_ref[0, count : 2 * count, :] = (g - g_hi.astype(F32)).astype(BF16)
    dm_hi = dm.astype(BF16)
    dm_lo = (dm - dm_hi.astype(F32)).astype(BF16)
    dm_hi = jnp.dot(perm, dm_hi, preferred_element_type=F32).astype(BF16)
    dm_lo = jnp.dot(perm, dm_lo, preferred_element_type=F32).astype(BF16)
    m_t = lax.dot_general(dm_hi, wo, NT, preferred_element_type=F32)
    m_t = m_t + lax.dot_general(dm_lo, wo, NT, preferred_element_type=F32)
    pixels = m_t.shape[0]
    stacked = jnp.concatenate([m_t] * heads, axis=0)
    row_head = lax.broadcasted_iota(jnp.int32, stacked.shape, 0) // pixels
    lane_head = lax.broadcasted_iota(jnp.int32, stacked.shape, 1) // HD
    stacked = jnp.where(row_head == lane_head, stacked, 0.0)
    s_hi = stacked.astype(BF16)
    s_lo = (stacked - s_hi.astype(F32)).astype(BF16)
    wv = wkv_ref[1]
    n_t = lax.dot_general(s_hi, wv, NT, preferred_element_type=F32)
    n_t = n_t + lax.dot_general(s_lo, wv, NT, preferred_element_type=F32)
    out_ref[0, 2 * count :, :] = n_t.astype(BF16)


def main_kernel(
    geo,
    tok_ref,
    mask_ref,
    wqkv_ref,
    wproj_ref,
    wup_ref,
    wdown_ref,
    lq_ref,
    wq_ref,
    wkv_ref,
    wo_ref,
    dm_ref,
    order_ref,
    position_ref,
    perm_ref,
    pick_ref,
    out_ref,
    raw,
    marks,
    qkv,
    proj,
    up,
    down,
    lq,
    wq,
    wkv,
    wo,
    dm,
    order,
    position,
    perm,
    pick,
    fold,
    first,
    own,
    halo,
    differs,
    hid,
    dw,
    du,
    ready,
    fold_base,
    x_one,
    base_pix,
    pix,
    pieces,
    checked,
    load_sem,
    weight_send,
    weight_recv,
    halo_send,
    halo_recv,
    piece_send,
    piece_recv,
):
    group, grid, var = (lax.axis_index(name) for name in ("group", "grid", "var"))
    bands, cores, windows, half = geo.bands, geo.cores, geo.windows, geo.half
    features, levels, width, heads = geo.features, geo.levels, geo.width, geo.heads
    sibling = (group, grid, lax.rem(var + 1, cores))

    def turn(step, column=grid):
        near = column * cores // bands == var
        rest = lax.rem(step + column + windows - 2, windows - 1)
        return jnp.where(near, jnp.where(step == 0, windows - 1, rest), step)

    east_grid = lax.rem(grid + 1, bands)
    west = (group, lax.rem(grid + bands - 1, bands), var)
    east = (group, east_grid, var)
    barrier = pltpu.get_barrier_semaphore()
    if geo.scatter:
        peers = bands * cores
        me = grid * cores + var

        @pl.loop(1, peers)
        def _(step):
            peer = lax.rem(me + step, peers)
            pl.semaphore_signal(
                barrier, inc=1, device_id=(group, peer // cores, lax.rem(peer, cores)), device_id_type=MESH
            )

        greeted = peers - 1
    else:
        for peer in (sibling, west, east):
            pl.semaphore_signal(barrier, inc=1, device_id=peer, device_id_type=MESH)
        greeted = 3

    loads = []

    def load(source, target):
        copy = pltpu.make_async_copy(source, target, load_sem.at[len(loads)])
        copy.start()
        loads.append(copy)
        return copy

    tiles = geo.rows // 8
    first_tile = var * (geo.row_count // 8)
    slabs = []
    for h in (1, 0):
        for s in range(geo.taken // 8):
            tile = lax.rem(first_tile + s, tiles)
            some = slice(h * geo.half_cols, (h + 1) * geo.half_cols)
            slabs.append(
                load(
                    tok_ref.at[some, :, pl.ds(pl.multiple_of(tile * 8, 8), 8), :],
                    raw.at[some, :, 8 * s : 8 * s + 8, :],
                )
            )
    fold_loads = [
        load(a, b)
        for a, b in ((lq_ref, lq), (wq_ref, wq), (wkv_ref, wkv), (wo_ref, wo), (dm_ref, dm), (perm_ref, perm))
    ]
    late_loads = [
        load(a, b)
        for a, b in (
            (mask_ref, marks.at[0]),
            (wqkv_ref, qkv.at[0]),
            (wproj_ref, proj.at[0]),
            (wup_ref, up.at[0]),
            (wdown_ref, down.at[0]),
            (position_ref, position),
            (order_ref, order),
            (pick_ref, pick),
        )
    ]

    depth = geo.half_cols * levels * geo.taken

    at = lax.broadcasted_iota(jnp.int32, (half, depth), 0)
    level = sum(jnp.where(at >= geo.half_patches * n, 1, 0) for n in range(1, levels))
    at = at - geo.half_patches * level
    row = sum(jnp.where(at >= geo.half_cols * n, 1, 0) for n in range(1, WIN_LAT + 1))
    wanted = ((at - geo.half_cols * row) * levels + level) * geo.taken + row + WIN_LAT // 2
    wanted = jnp.where(row < WIN_LAT, wanted, depth * 2)
    wanted = lax.broadcasted_iota(jnp.int32, (half, depth), 1) - wanted

    def collect(h, w, target):
        slab = raw[h * geo.half_cols : (h + 1) * geo.half_cols].reshape(depth, features)
        picked = (wanted == WIN_LAT * w).astype(F32).astype(BF16)
        target[w] = jnp.dot(picked, slab, preferred_element_type=F32).astype(BF16)

    for copy in slabs[: len(slabs) // 2]:
        copy.wait()
    collect(1, turn(0, east_grid), first)
    pl.semaphore_wait(barrier, greeted)

    def remote(source, target, send, recv, peer):
        copy = pltpu.make_async_remote_copy(
            src_ref=source, dst_ref=target, send_sem=send, recv_sem=recv, device_id=peer, device_id_type=MESH
        )
        copy.start()
        return copy

    copies = [remote(mask_ref, marks.at[1], weight_send.at[0], weight_recv.at[0], east)]
    halos = []

    def pass_on(step):
        w = turn(step, east_grid)
        halos.append(remote(first.at[w], halo.at[w], halo_send.at[w], halo_recv.at[w], east))

    pass_on(0)
    for n, (source, target) in enumerate(((wqkv_ref, qkv), (wproj_ref, proj), (wup_ref, up), (wdown_ref, down))):
        copies.append(remote(source, target.at[1], weight_send.at[n + 1], weight_recv.at[n + 1], sibling))

    for step in range(1, windows):
        collect(1, turn(step, east_grid), first)
    for copy in slabs[len(slabs) // 2 :]:
        copy.wait()
    for step in range(windows):
        collect(0, turn(step), own)
    for step in range(1, windows):
        pass_on(step)
    for copy in fold_loads:
        copy.wait()
    fold_decoder(lq[...], wq[...], wkv, wo[...], dm[...], perm[...], fold)

    tokens = geo.tokens
    q_pos = lax.broadcasted_iota(jnp.int32, (tokens, KEYS), 0)
    k_pos = lax.broadcasted_iota(jnp.int32, (tokens, KEYS), 1)
    diagonal = q_pos == k_pos

    def region_of(pos):
        pos = jnp.where(pos >= half, pos - half, pos)
        for level in range(levels - 1, 0, -1):
            start = geo.half_patches * level
            pos = jnp.where(pos >= start, pos - start, pos)
        return pos >= geo.half_patches // 2

    differs[...] = jnp.where(region_of(q_pos) != region_of(k_pos), -1e30, 0.0)
    lane_head = lax.broadcasted_iota(jnp.int32, (tokens, width), 1) // HD
    lane_head_keys = lax.broadcasted_iota(jnp.int32, (KEYS, width), 1) // HD

    for copy in late_loads:
        copy.wait()
    copies.append(remote(fold.at[0], fold.at[1], weight_send.at[5], weight_recv.at[5], sibling))

    count = heads * LEVEL_SLOTS
    pixels = geo.pixels
    row_size = pixels // cores // SQUARE_SPAN
    rows = geo.slots * row_size
    half_lat = WIN_LAT // 2
    extra = half_lat * geo.cols * SQUARE_SPAN - BLOCK
    pix[geo.isobars :] = jnp.zeros((geo.slots - geo.isobars, pixels, BLOCK), F32)
    units = up.shape[2]

    def piece_copy(w, ih, core, action):
        band = lax.rem(var * windows + w + ih, bands)
        here = jnp.logical_and(band == grid, core == var)
        source, target = pieces.at[w, ih, core], out_ref.at[grid, ih]

        @pl.when(here)
        def _():
            if action == "start":
                pltpu.make_async_copy(source, target, piece_recv.at[grid, ih]).start()

        @pl.when(jnp.logical_not(here))
        def _():
            if action == "start":
                pltpu.make_async_remote_copy(
                    src_ref=source,
                    dst_ref=target,
                    send_sem=piece_send.at[w, ih, core],
                    recv_sem=piece_recv.at[grid, ih],
                    device_id=(group, band, core),
                    device_id_type=MESH,
                ).start()
            else:
                pltpu.make_async_copy(source, source, piece_send.at[w, ih, core]).wait()

    def arrive(w):
        pltpu.make_async_copy(halo.at[w], halo.at[w], halo_recv.at[w]).wait()

    def send(w, some=range(cores)):
        for core in some:
            checked[...] = pieces[w, :, core].astype(F32).max(axis=0)
        if geo.scatter:
            for core in some:
                for ih in range(2):
                    piece_copy(w, ih, core, "start")

    def attend(w):
        x = jnp.concatenate([own[w], halo[w]], axis=0).astype(F32)
        n1 = layer_norm(x[half:]).astype(BF16)
        target = position[0:1, :] + (var * geo.row_count + WIN_LAT * w + half_lat)
        target = jnp.where(target >= geo.rows, target - geo.rows, target)
        there = lax.broadcasted_iota(jnp.int32, (geo.rows, KEYS), 0) == target
        there = there.astype(F32).astype(BF16)
        opened = jnp.zeros((1, KEYS), F32)
        column = lax.broadcasted_iota(jnp.int32, (geo.cols, KEYS), 0)
        for h in range(2):
            seen = (marks[h] > 0).astype(F32).astype(BF16)
            seen = jnp.dot(seen, there, preferred_element_type=F32)
            seen = jnp.where(column == position[1 + h : 2 + h, :], seen, 0.0)
            opened = opened + jnp.sum(seen, axis=0, keepdims=True)
        allowed = jnp.logical_or(jnp.broadcast_to(opened, diagonal.shape) > 0.5, diagonal)
        cut = jnp.logical_and(var == cores - 1, w == windows - 1)
        bias = jnp.where(allowed, 0.0, -1e30) + differs[...] * jnp.where(cut, 1.0, 0.0)
        yield
        scores, values = [], []
        for s in range(cores):
            q, k, v = (
                jnp.concatenate(
                    [ready[s, i, w], jnp.dot(n1, qkv[s, i], preferred_element_type=F32).astype(BF16)], axis=0
                )
                for i in range(3)
            )
            q = q * jnp.asarray(HD ** (-0.5), BF16)
            tail = jnp.zeros((KEYS - tokens, width), BF16)
            k = jnp.concatenate([k, tail], axis=0)
            values.append(jnp.concatenate([v, tail], axis=0))
            q_all = jnp.concatenate(
                [jnp.where(lane_head == h, q, jnp.zeros_like(q)) for h in range(heads)], axis=0
            )
            yield
            scores.append(lax.dot_general(q_all, k, NT, preferred_element_type=F32))
            yield
        attended = x
        for s in range(cores):
            weights = []
            for h in range(heads):
                one = scores[s][h * tokens : (h + 1) * tokens] + bias
                peak = jnp.max(one, axis=-1, keepdims=True)
                e = jnp.exp(one - peak)
                total = jnp.sum(e, axis=-1, keepdims=True)
                weights.append((e * (1.0 / total)).astype(BF16))
            weights = jnp.concatenate(weights, axis=1)
            v = values[s]
            v_all = jnp.concatenate(
                [jnp.where(lane_head_keys == h, v, jnp.zeros_like(v)) for h in range(heads)], axis=0
            )
            context = jnp.dot(weights, v_all, preferred_element_type=F32).astype(BF16)
            yield
            attended = attended + jnp.dot(context, proj[s], preferred_element_type=F32)
            if s == cores - 1:
                x_one[w] = attended
            yield

    def finish(w):
        n2 = layer_norm(x_one[w]).astype(BF16)
        yield
        for s in range(cores):
            for c in range(0, units, CHUNK):
                one = jnp.dot(n2, up[s, :, c : c + CHUNK], preferred_element_type=F32)
                one = 0.5 * one * (1.0 + lax.erf(one * 2.0 ** (-0.5)))
                hid[:, s * units + c : s * units + c + CHUNK] = one.astype(BF16)
                yield
        latent = x_one[w] + jnp.dot(
            hid[...], down[...].reshape(cores * units, features), preferred_element_type=F32
        )
        yield
        n3 = layer_norm(latent.astype(BF16).astype(F32)).astype(BF16)
        n3 = jnp.dot(order[...], n3, preferred_element_type=F32).astype(BF16)
        n3, others = n3[:BLOCK], n3[BLOCK:]
        yield
        base = lax.dot_general(fold_base[...], n3, NT, preferred_element_type=F32)
        base_pix[...] = base[:pixels] + base[pixels:]
        for s in range(cores):
            g = lax.dot_general(fold[s, 0 : 2 * count, :], others, NT, preferred_element_type=F32)
            g = g[:count] + g[count:]
            scores = [jnp.zeros((count, BLOCK), F32)]
            scores += [g[:, j * BLOCK : (j + 1) * BLOCK] for j in range(levels - 1)]
            peak = functools.reduce(jnp.maximum, scores)
            e = [jnp.exp(one - peak) for one in scores]
            inverse = 1.0 / sum(e)
            u = lax.dot_general(fold[s, 2 * count :, :], others, NT, preferred_element_type=F32)
            for j in range(levels - 1):
                dw[j, s * count : (s + 1) * count, :] = e[j + 1] * inverse
                du[j, s * heads * pixels : (s + 1) * heads * pixels, :] = u[:, j * BLOCK : (j + 1) * BLOCK]
        yield

    def paint(w):
        low = pixels // cores
        lane = lax.broadcasted_iota(jnp.int32, (2 * row_size, BLOCK), 1) - lane_base
        lane = jnp.where(lane < 0, lane + BLOCK, lane)
        for core in range(cores):
            top = core * low
            for first_level in range(0, geo.isobars, 5):
                some = range(first_level, min(first_level + 5, geo.isobars))
                totals = [base_pix[top : top + low, :] for _ in some]
                for s in range(cores):
                    for h in range(heads):
                        for j in range(levels - 1):
                            at = (s * heads + h) * pixels + top
                            value = du[j, at : at + low, :]
                            for n, level in enumerate(some):
                                row = s * count + level * heads + h
                                totals[n] = totals[n] + dw[j, row : row + 1, :] * value
                for n, level in enumerate(some):
                    pix[level, top : top + low, :] = totals[n]
            total = jnp.zeros((rows, 4 * BLOCK), F32)
            for b in range(SQUARE_SPAN):
                at = top + b * row_size
                part = pix[:, at : at + row_size, :].reshape(rows, BLOCK)
                total = total + jnp.dot(part.astype(BF16), pick[b], preferred_element_type=F32)
            for ih in range(2):
                left = jnp.zeros((2 * row_size, BLOCK), F32)
                for k in range(geo.slots // 2):
                    at = slice(2 * row_size * k, 2 * row_size * (k + 1))
                    inside = jnp.logical_and(lane >= extra * k, lane < extra * (k + 1))
                    left = jnp.where(inside, total[at, (2 + ih) * BLOCK : (3 + ih) * BLOCK], left)
                main = total[:, ih * BLOCK : (ih + 1) * BLOCK]
                pieces[w, ih, core] = jnp.concatenate([main, left], axis=0).astype(BF16)
            yield

    def run(order="", **steps):
        for name in order:
            next(steps[name])

    mask_copy, qkv_copy, proj_copy, up_copy, down_copy, fold_copy = copies
    for copy in (mask_copy, qkv_copy, proj_copy):
        copy.wait()
    lane_base = lax.rem(grid * geo.run + bands * geo.run - geo.run // 2, BLOCK) if geo.scatter else 0
    if geo.scatter:
        for b in range(SQUARE_SPAN):
            for part in range(4):
                lanes = slice(part * BLOCK, (part + 1) * BLOCK)
                pick[b, :, lanes] = pltpu.roll(pick[b, :, lanes].astype(F32), lane_base, 1).astype(BF16)
    n_own = layer_norm(own[...].reshape(windows * half, features).astype(F32)).astype(BF16)
    for s in range(cores):
        for i in range(3):
            one = jnp.dot(n_own, qkv[s, i], preferred_element_type=F32).astype(BF16)
            ready[s, i] = one.reshape(windows, half, width)
    arrive(turn(0))
    run("a" * ORDER.count("a"), a=attend(turn(0)))
    for copy in (up_copy, down_copy, fold_copy):
        copy.wait()
    whole = jnp.zeros((pixels, features), F32)
    for s in range(cores):
        for h in range(heads):
            top = 2 * count + h * pixels
            whole = whole + fold[s, top : top + pixels, :].astype(F32)
    whole_hi = whole.astype(BF16)
    fold_base[0:pixels, :] = whole_hi
    fold_base[pixels:, :] = (whole - whole_hi.astype(F32)).astype(BF16)

    last = windows - 1

    def complete(w):
        yield from finish(w)
        yield from paint(w)

    @pl.loop(0, last)
    def _(step):
        arrive(turn(step + 1))
        run(ORDER, a=attend(turn(step + 1)), b=complete(turn(step)))
        send(turn(step))

    finishing = complete(turn(last))
    run("b" * (ORDER.count("b") - cores), b=finishing)
    for core in range(cores):
        next(finishing)
        send(turn(last), (core,))

    for copy in halos:
        copy.wait_send()
    if geo.scatter:

        @pl.loop(0, bands)
        def _(s):
            for ih in range(2):
                target = out_ref.at[s, ih]
                pltpu.make_async_copy(target, target, piece_recv.at[s, ih]).wait()

        @pl.loop(0, windows)
        def _(w):
            for ih in range(2):
                for core in range(cores):
                    piece_copy(w, ih, core, "finish")

    else:
        copy = pltpu.make_async_copy(pieces, out_ref, load_sem.at[0])
        copy.start()
        copy.wait()


def forecast(geo, *args):
    tables = (
        jnp.asarray(geo.order_table(), BF16),
        jnp.asarray(geo.position_table(), jnp.int32),
        jnp.asarray(geo.pixel_table(), BF16),
        jnp.asarray(geo.pick_table(), BF16),
    )
    features, width, cores, windows = geo.features, geo.width, geo.cores, geo.windows
    units = args[4].shape[1]
    fold_rows = geo.heads * (2 * LEVEL_SLOTS + geo.pixels)
    vmem = pltpu.VMEM
    dma = pltpu.SemaphoreType.DMA
    if geo.scatter:
        out_shape = (geo.bands, 2, BLOCK, BLOCK)
    else:
        out_shape = (windows, 2, cores, BLOCK, BLOCK)
    return pl.pallas_call(
        functools.partial(main_kernel, geo),
        out_shape=jax.ShapeDtypeStruct(out_shape, BF16),
        in_specs=[pl.BlockSpec(memory_space=pltpu.HBM)] * (len(args) + len(tables)),
        out_specs=pl.BlockSpec(memory_space=vmem if geo.scatter else pltpu.HBM),
        scratch_shapes=[
            vmem((geo.cols, geo.levels, geo.taken, features), BF16),
            vmem((2, geo.cols, geo.rows), jnp.int32),
            vmem((cores, 3, features, width), BF16),
            vmem((cores, width, features), BF16),
            vmem((cores, features, units), BF16),
            vmem((cores, units, features), BF16),
            *[vmem(one.shape, one.dtype) for one in args[6:]],
            *[vmem(one.shape, one.dtype) for one in tables],
            vmem((cores, fold_rows, features), BF16),
            vmem((windows, geo.half, features), BF16),
            vmem((windows, geo.half, features), BF16),
            vmem((windows, geo.half, features), BF16),
            vmem((geo.tokens, KEYS), F32),
            vmem((geo.tokens, cores * units), BF16),
            vmem((geo.levels - 1, cores * geo.heads * LEVEL_SLOTS, BLOCK), F32),
            vmem((geo.levels - 1, cores * geo.heads * geo.pixels, BLOCK), F32),
            vmem((cores, 3, windows, geo.half, width), BF16),
            vmem((2 * geo.pixels, features), BF16),
            vmem((windows, geo.tokens, features), F32),
            vmem((geo.pixels, BLOCK), F32),
            vmem((geo.slots, geo.pixels, BLOCK), F32),
            vmem((windows, 2, cores, BLOCK, BLOCK), BF16),
            vmem((BLOCK, BLOCK), F32),
            dma((geo.taken // 4 + 15,)),
            dma((6,)),
            dma((6,)),
            dma((windows,)),
            dma((windows,)),
            dma((windows, 2, cores)),
            dma((geo.bands, 2)),
        ],
        compiler_params=pltpu.CompilerParams(
            collective_id=0, has_side_effects=True, vmem_limit_bytes=30 * 2**20
        ),
    )(*[pltpu.with_memory_space_constraint(one, pltpu.HBM) for one in (*args, *tables)])


def assemble_kernel(isobars, run, got_ref, out_ref, out, sems):
    bands = got_ref.shape[0]
    half_lat = WIN_LAT // 2
    groups = (isobars + 1) // 2
    tiles = out.shape[-1] // BLOCK
    extra = half_lat * run - BLOCK
    bases = lane_bases(bands, run)
    lane = lax.broadcasted_iota(jnp.int32, (1, BLOCK), 1)
    sublane = lax.broadcasted_iota(jnp.int32, (1, 8, BLOCK), 1)

    def around(start, length):
        start = start % BLOCK
        if start + length <= BLOCK:
            return jnp.logical_and(lane >= start, lane < start + length)
        return jnp.logical_or(lane >= start, lane < start + length - BLOCK)

    def put(merged, value, start, length):
        while length > 0:
            start = start % (tiles * BLOCK)
            tile, part = start // BLOCK, min(length, BLOCK - start % BLOCK)
            old = merged[tile]
            merged[tile] = value if old is None else jnp.where(around(start, part), value, old)
            start, length = start + part, length - part

    copies = []
    middle = (groups + 1) // 2
    for first, last in ((0, middle), (middle, groups)):
        low, high = 2 * first, min(2 * last, isobars)
        found = {}
        for ih in range(2):
            pieces = [got_ref[s, ih, 16 * first : 16 * last, :].astype(F32) for s in range(bands)]
            rests = [got_ref[s, ih, 16 * groups : 16 * groups + 16, :].astype(F32) for s in range(bands)]
            left = []
            for k in range(first, last):
                one = rests[0]
                for s in range(1, bands):
                    one = jnp.where(around(bases[s] + extra * k, extra), rests[s], one)
                left.append(pltpu.roll(one, (-extra * k) % BLOCK, 1) if k > 0 else one)
            left = jnp.concatenate(left, axis=0)
            for r in range(half_lat):
                merged = [None] * tiles
                for s in range(bands):
                    put(merged, pieces[s], bases[s] + run * r, min(run, BLOCK - run * r))
                if run * (r + 1) > BLOCK:
                    for s in range(bands):
                        put(merged, left, bases[s] + BLOCK, run * (r + 1) - BLOCK)
                if r > 0:
                    merged = [pltpu.roll(one, BLOCK - run * r, 1) for one in merged]
                    merged = [
                        jnp.where(lane < BLOCK - run * r, merged[t], merged[(t + 1) % tiles])
                        for t in range(tiles)
                    ]
                found[(1 - ih) * half_lat + r] = merged
        for top in range(0, 2 * half_lat, 2):
            for t in range(tiles):
                upper = found[top][t].reshape(-1, 8, BLOCK)
                lower = found[top + 1][t].reshape(-1, 8, BLOCK)
                some = (
                    jnp.where(sublane < 4, upper, pltpu.roll(lower, 4, 1)),
                    jnp.where(sublane < 4, pltpu.roll(upper, 4, 1), lower),
                )
                for v in range(2):
                    out[v, low:high, 4 * top : 4 * top + 8, t * BLOCK : (t + 1) * BLOCK] = some[v][: high - low]
        for v in range(2):
            copy = pltpu.make_async_copy(
                out.at[v, low:high], out_ref.at[v, low:high], sems.at[len(copies)]
            )
            copy.start()
            copies.append(copy)
    for copy in copies:
        copy.wait()


def assemble(got, geo):
    shape = (TARGET_QUANTITY // geo.cores, geo.isobars, WIN_LAT * SQUARE_SPAN, geo.bands * geo.run)
    return pl.pallas_call(
        functools.partial(assemble_kernel, geo.isobars, geo.run),
        out_shape=jax.ShapeDtypeStruct(shape, F32),
        out_specs=pl.BlockSpec(memory_space=pltpu.HBM),
        scratch_shapes=[pltpu.VMEM(shape, F32), pltpu.SemaphoreType.DMA((4,))],
        compiler_params=pltpu.CompilerParams(vmem_limit_bytes=40 * 2**20),
    )(got)


def exchange(pieces, geo):
    half_lat = WIN_LAT // 2
    run = geo.cols * SQUARE_SPAN
    quantities = TARGET_QUANTITY // geo.cores
    rows = geo.slots * quantities * SQUARE_SPAN
    extra = half_lat * run - BLOCK
    lead = pieces.shape[:3]
    main = pieces[:, :, :, :rows].reshape(*lead, geo.slots, quantities, SQUARE_SPAN, BLOCK)
    rest = pieces[:, :, :, rows:, : extra * (geo.slots // 2)]
    rest = rest.reshape(*lead, 2, quantities, SQUARE_SPAN, geo.slots // 2, extra)
    rest = jnp.moveaxis(rest, 6, 3).reshape(*lead, geo.slots, quantities, SQUARE_SPAN, extra)
    maps = jnp.concatenate([main, rest], axis=-1)[:, :, :, : geo.isobars]
    maps = maps.reshape(*lead, geo.isobars, quantities, SQUARE_SPAN, half_lat, run)
    maps = jnp.transpose(maps, (2, 4, 3, 0, 1, 6, 5, 7))
    maps = maps.reshape(TARGET_QUANTITY, geo.isobars, geo.row_count * SQUARE_SPAN, run)
    maps = lax.all_to_all(maps, "var", split_axis=0, concat_axis=2, tiled=True)
    maps = jnp.roll(maps, half_lat * SQUARE_SPAN, 2)
    maps = lax.all_to_all(maps, "grid", split_axis=2, concat_axis=3, tiled=True)
    return jnp.roll(maps, -(run // 2), 3).astype(F32)


def local(
    tokens,
    key_mask,
    w_qkv,
    w_proj,
    w_up,
    w_down,
    level_query,
    w_dec_q,
    w_dec_kv,
    w_dec_o,
    decode_matrix,
):
    geo = Geometry(
        tokens, w_proj, level_query, decode_matrix, lax.axis_size("var"), lax.axis_size("grid")
    )
    pieces = forecast(
        geo,
        jnp.transpose(tokens, (1, 2, 0, 3)),
        key_mask.T,
        w_qkv,
        w_proj,
        w_up,
        w_down,
        level_query,
        w_dec_q,
        w_dec_kv,
        w_dec_o,
        decode_matrix.T,
    )
    if geo.scatter:
        return assemble(pieces, geo)
    return exchange(pieces, geo)


def solution(mesh):
    placed = (
        P("group", "grid", None, None),
        P("group", "grid"),
        P(None, None, "var"),
        P("var", None),
        P(None, "var"),
        P("var", None),
        P(),
        P(None, "var"),
        P(None, None, "var"),
        P("var", None),
        P(),
    )
    return jax.shard_map(
        local,
        mesh=mesh,
        in_specs=placed,
        out_specs=P("var", "group", "grid", None),
        check_vma=False,
    )
```

```python
import functools

import jax
import jax.numpy as jnp
import numpy as np
from jax import lax
from jax.experimental import pallas as pl
from jax.experimental.pallas import tpu as pltpu
from jax.sharding import PartitionSpec as P

HD = 64
TARGET_QUANTITY = 4
SQUARE_SPAN = 4
WIN_LAT = 6
EPSILON = 1e-05
BLOCK = 128
KEYS = 256
CHUNK = 256
LEVEL_SLOTS = 16
ORDER = "aabaabbbbaabbbbabababbb"
MESH = pl.DeviceIdType.MESH
NT = (((1,), (1,)), ((), ()))
F32 = jnp.float32
BF16 = jnp.bfloat16


def layer_norm(values):
    center = values - jnp.mean(values, axis=-1, keepdims=True)
    spread = jnp.mean(center * center, axis=-1, keepdims=True)
    return center * lax.rsqrt(spread + EPSILON)


def lane_bases(bands, run):
    return [(s * run + bands * run - run // 2) % (bands * run) for s in range(bands)]


class Geometry:
    def __init__(self, tokens, w_proj, level_query, decode_matrix, cores, bands):
        self.rows, self.cols, self.levels, self.features = tokens.shape
        self.cores, self.bands = cores, bands
        self.half_cols = self.cols // 2
        self.row_count = self.rows // cores
        self.windows = self.row_count // WIN_LAT
        self.taken = 8 * (-(-(self.row_count + WIN_LAT // 2) // 8))
        self.half_patches = WIN_LAT * self.half_cols
        self.half = 16 * (-(-(self.levels * self.half_patches) // 16))
        self.tokens = 2 * self.half
        self.patches = 2 * self.half_patches
        self.width = w_proj.shape[0]
        self.heads = self.width // HD
        self.isobars = level_query.shape[0]
        self.slots = self.isobars + self.isobars % 2
        self.pixels = decode_matrix.shape[1]
        self.run = self.cols * SQUARE_SPAN
        self.extra = WIN_LAT // 2 * self.run - BLOCK
        self.bases = lane_bases(bands, self.run)
        covered = [(base + lane) % BLOCK for base in self.bases for lane in range(self.extra)]
        self.scatter = (
            bands * WIN_LAT == self.rows
            and (bands * self.run) % BLOCK == 0
            and self.extra * (self.slots // 2) <= BLOCK
            and sorted(covered) == list(range(BLOCK))
        )

    def place(self, half, level, r, c):
        return half * self.half + level * self.half_patches + r * self.half_cols + c

    def each(self):
        for half in range(2):
            for level in range(self.levels):
                for r in range(WIN_LAT):
                    for c in range(self.half_cols):
                        yield half, level, r, c

    def order_table(self):
        table = np.zeros((self.levels * BLOCK, self.tokens), np.float32)
        for half, level, r, c in self.each():
            patch = r * self.cols + (1 - half) * self.half_cols + c
            table[level * BLOCK + patch, self.place(half, level, r, c)] = 1.0
            if level > 0:
                table[level * BLOCK + patch, self.place(half, 0, r, c)] = -1.0
        return table

    def position_table(self):
        table = np.full((8, KEYS), -1, np.int32)
        table[0] = 0
        for half, level, r, c in self.each():
            at = self.place(half, level, r, c)
            table[0, at] = r
            table[1 + half, at] = c + half * self.half_cols
        return table

    def pixel_table(self):
        table = np.zeros((self.pixels, self.pixels), np.float32)
        own = TARGET_QUANTITY // self.cores
        for v in range(TARGET_QUANTITY):
            for a in range(SQUARE_SPAN):
                for b in range(SQUARE_SPAN):
                    target = ((v // own * SQUARE_SPAN + b) * own + v % own) * SQUARE_SPAN + a
                    table[target, (v * SQUARE_SPAN + a) * SQUARE_SPAN + b] = 1.0
        return table

    def pick_table(self):
        half_lat = WIN_LAT // 2
        run = self.cols * SQUARE_SPAN
        extra = half_lat * run - BLOCK
        picks = np.zeros((SQUARE_SPAN, BLOCK, 4 * BLOCK), np.float32)
        for ih in range(2):
            for q in range(half_lat * run):
                r, rest = divmod(q, run)
                column, b = divmod(rest, SQUARE_SPAN)
                source = (half_lat * ih + r) * self.cols + column
                if q < BLOCK:
                    picks[b, source, ih * BLOCK + q] = 1.0
                else:
                    for k in range(self.slots // 2):
                        picks[b, source, (2 + ih) * BLOCK + extra * k + q - BLOCK] = 1.0
        return picks


def fold_decoder(lq, wq, wkv_ref, wo, dm, perm, out_ref):
    width = wq.shape[1]
    heads = width // HD
    dquery = jnp.dot(lq, wq, preferred_element_type=F32) * HD ** (-0.5)
    d_hi = dquery.astype(BF16)
    d_lo = (dquery - d_hi.astype(F32)).astype(BF16)
    count = LEVEL_SLOTS * heads
    row = lax.broadcasted_iota(jnp.int32, (count, dquery.shape[0]), 0)
    slot = lax.broadcasted_iota(jnp.int32, (count, dquery.shape[0]), 1)
    spread = (row // heads == slot).astype(F32).astype(BF16)
    row = lax.broadcasted_iota(jnp.int32, (count, width), 0)
    mine = row % heads == lax.broadcasted_iota(jnp.int32, (count, width), 1) // HD
    q_hi = jnp.dot(spread, d_hi, preferred_element_type=F32)
    q_hi = jnp.where(mine, q_hi, 0.0).astype(BF16)
    q_lo = jnp.dot(spread, d_lo, preferred_element_type=F32)
    q_lo = jnp.where(mine, q_lo, 0.0).astype(BF16)
    wk = wkv_ref[0]
    g = lax.dot_general(q_hi, wk, NT, preferred_element_type=F32)
    g = g + lax.dot_general(q_lo, wk, NT, preferred_element_type=F32)
    g_hi = g.astype(BF16)
    out_ref[0, 0:count, :] = g_hi
    out_ref[0, count : 2 * count, :] = (g - g_hi.astype(F32)).astype(BF16)
    dm_hi = dm.astype(BF16)
    dm_lo = (dm - dm_hi.astype(F32)).astype(BF16)
    dm_hi = jnp.dot(perm, dm_hi, preferred_element_type=F32).astype(BF16)
    dm_lo = jnp.dot(perm, dm_lo, preferred_element_type=F32).astype(BF16)
    m_t = lax.dot_general(dm_hi, wo, NT, preferred_element_type=F32)
    m_t = m_t + lax.dot_general(dm_lo, wo, NT, preferred_element_type=F32)
    pixels = m_t.shape[0]
    stacked = jnp.concatenate([m_t] * heads, axis=0)
    row_head = lax.broadcasted_iota(jnp.int32, stacked.shape, 0) // pixels
    lane_head = lax.broadcasted_iota(jnp.int32, stacked.shape, 1) // HD
    stacked = jnp.where(row_head == lane_head, stacked, 0.0)
    s_hi = stacked.astype(BF16)
    s_lo = (stacked - s_hi.astype(F32)).astype(BF16)
    wv = wkv_ref[1]
    n_t = lax.dot_general(s_hi, wv, NT, preferred_element_type=F32)
    n_t = n_t + lax.dot_general(s_lo, wv, NT, preferred_element_type=F32)
    out_ref[0, 2 * count :, :] = n_t.astype(BF16)


def main_kernel(
    geo,
    tok_ref,
    mask_ref,
    wqkv_ref,
    wproj_ref,
    wup_ref,
    wdown_ref,
    lq_ref,
    wq_ref,
    wkv_ref,
    wo_ref,
    dm_ref,
    order_ref,
    position_ref,
    perm_ref,
    pick_ref,
    out_ref,
    raw,
    marks,
    qkv,
    proj,
    up,
    down,
    lq,
    wq,
    wkv,
    wo,
    dm,
    order,
    position,
    perm,
    pick,
    fold,
    first,
    own,
    halo,
    differs,
    hid,
    dw,
    du,
    ready,
    fold_base,
    x_one,
    base_pix,
    pix,
    pieces,
    checked,
    load_sem,
    weight_send,
    weight_recv,
    halo_send,
    halo_recv,
    piece_send,
    piece_recv,
):
    group, grid, var = (lax.axis_index(name) for name in ("group", "grid", "var"))
    bands, cores, windows, half = geo.bands, geo.cores, geo.windows, geo.half
    features, levels, width, heads = geo.features, geo.levels, geo.width, geo.heads
    sibling = (group, grid, lax.rem(var + 1, cores))

    def turn(step, column=grid):
        near = column * cores // bands == var
        rest = lax.rem(step + column + windows - 2, windows - 1)
        return jnp.where(near, jnp.where(step == 0, windows - 1, rest), step)

    east_grid = lax.rem(grid + 1, bands)
    west = (group, lax.rem(grid + bands - 1, bands), var)
    east = (group, east_grid, var)
    barrier = pltpu.get_barrier_semaphore()
    if geo.scatter:
        peers = bands * cores
        me = grid * cores + var

        @pl.loop(1, peers)
        def _(step):
            peer = lax.rem(me + step, peers)
            pl.semaphore_signal(
                barrier, inc=1, device_id=(group, peer // cores, lax.rem(peer, cores)), device_id_type=MESH
            )

        greeted = peers - 1
    else:
        for peer in (sibling, west, east):
            pl.semaphore_signal(barrier, inc=1, device_id=peer, device_id_type=MESH)
        greeted = 3

    loads = []

    def load(source, target):
        copy = pltpu.make_async_copy(source, target, load_sem.at[len(loads)])
        copy.start()
        loads.append(copy)
        return copy

    tiles = geo.rows // 8
    first_tile = var * (geo.row_count // 8)
    slabs = []
    for h in (1, 0):
        for s in range(geo.taken // 8):
            tile = lax.rem(first_tile + s, tiles)
            some = slice(h * geo.half_cols, (h + 1) * geo.half_cols)
            slabs.append(
                load(
                    tok_ref.at[some, :, pl.ds(pl.multiple_of(tile * 8, 8), 8), :],
                    raw.at[some, :, 8 * s : 8 * s + 8, :],
                )
            )
    fold_loads = [
        load(a, b)
        for a, b in ((lq_ref, lq), (wq_ref, wq), (wkv_ref, wkv), (wo_ref, wo), (dm_ref, dm), (perm_ref, perm))
    ]
    late_loads = [
        load(a, b)
        for a, b in (
            (mask_ref, marks.at[0]),
            (wqkv_ref, qkv.at[0]),
            (wproj_ref, proj.at[0]),
            (wup_ref, up.at[0]),
            (wdown_ref, down.at[0]),
            (position_ref, position),
            (order_ref, order),
            (pick_ref, pick),
        )
    ]

    depth = geo.half_cols * levels * geo.taken

    at = lax.broadcasted_iota(jnp.int32, (half, depth), 0)
    level = sum(jnp.where(at >= geo.half_patches * n, 1, 0) for n in range(1, levels))
    at = at - geo.half_patches * level
    row = sum(jnp.where(at >= geo.half_cols * n, 1, 0) for n in range(1, WIN_LAT + 1))
    wanted = ((at - geo.half_cols * row) * levels + level) * geo.taken + row + WIN_LAT // 2
    wanted = jnp.where(row < WIN_LAT, wanted, depth * 2)
    wanted = lax.broadcasted_iota(jnp.int32, (half, depth), 1) - wanted

    def collect(h, w, target):
        slab = raw[h * geo.half_cols : (h + 1) * geo.half_cols].reshape(depth, features)
        picked = (wanted == WIN_LAT * w).astype(F32).astype(BF16)
        target[w] = jnp.dot(picked, slab, preferred_element_type=F32).astype(BF16)

    for copy in slabs[: len(slabs) // 2]:
        copy.wait()
    collect(1, turn(0, east_grid), first)
    pl.semaphore_wait(barrier, greeted)

    def remote(source, target, send, recv, peer):
        copy = pltpu.make_async_remote_copy(
            src_ref=source, dst_ref=target, send_sem=send, recv_sem=recv, device_id=peer, device_id_type=MESH
        )
        copy.start()
        return copy

    copies = [remote(mask_ref, marks.at[1], weight_send.at[0], weight_recv.at[0], east)]
    halos = []

    def pass_on(step):
        w = turn(step, east_grid)
        halos.append(remote(first.at[w], halo.at[w], halo_send.at[w], halo_recv.at[w], east))

    pass_on(0)
    for n, (source, target) in enumerate(((wqkv_ref, qkv), (wproj_ref, proj), (wup_ref, up), (wdown_ref, down))):
        copies.append(remote(source, target.at[1], weight_send.at[n + 1], weight_recv.at[n + 1], sibling))

    for step in range(1, windows):
        collect(1, turn(step, east_grid), first)
    for copy in slabs[len(slabs) // 2 :]:
        copy.wait()
    for step in range(windows):
        collect(0, turn(step), own)
    for step in range(1, windows):
        pass_on(step)
    for copy in fold_loads:
        copy.wait()
    fold_decoder(lq[...], wq[...], wkv, wo[...], dm[...], perm[...], fold)

    tokens = geo.tokens
    q_pos = lax.broadcasted_iota(jnp.int32, (tokens, KEYS), 0)
    k_pos = lax.broadcasted_iota(jnp.int32, (tokens, KEYS), 1)
    diagonal = q_pos == k_pos

    def region_of(pos):
        pos = jnp.where(pos >= half, pos - half, pos)
        for level in range(levels - 1, 0, -1):
            start = geo.half_patches * level
            pos = jnp.where(pos >= start, pos - start, pos)
        return pos >= geo.half_patches // 2

    differs[...] = jnp.where(region_of(q_pos) != region_of(k_pos), -1e30, 0.0)
    lane_head = lax.broadcasted_iota(jnp.int32, (tokens, width), 1) // HD
    lane_head_keys = lax.broadcasted_iota(jnp.int32, (KEYS, width), 1) // HD

    for copy in late_loads:
        copy.wait()
    copies.append(remote(fold.at[0], fold.at[1], weight_send.at[5], weight_recv.at[5], sibling))

    count = heads * LEVEL_SLOTS
    pixels = geo.pixels
    row_size = pixels // cores // SQUARE_SPAN
    rows = geo.slots * row_size
    half_lat = WIN_LAT // 2
    extra = half_lat * geo.cols * SQUARE_SPAN - BLOCK
    pix[geo.isobars :] = jnp.zeros((geo.slots - geo.isobars, pixels, BLOCK), F32)
    units = up.shape[2]

    def piece_copy(w, ih, core, action):
        band = lax.rem(var * windows + w + ih, bands)
        here = jnp.logical_and(band == grid, core == var)
        source, target = pieces.at[w, ih, core], out_ref.at[grid, ih]

        @pl.when(here)
        def _():
            if action == "start":
                pltpu.make_async_copy(source, target, piece_recv.at[grid, ih]).start()

        @pl.when(jnp.logical_not(here))
        def _():
            if action == "start":
                pltpu.make_async_remote_copy(
                    src_ref=source,
                    dst_ref=target,
                    send_sem=piece_send.at[w, ih, core],
                    recv_sem=piece_recv.at[grid, ih],
                    device_id=(group, band, core),
                    device_id_type=MESH,
                ).start()
            else:
                pltpu.make_async_copy(source, source, piece_send.at[w, ih, core]).wait()

    def arrive(w):
        pltpu.make_async_copy(halo.at[w], halo.at[w], halo_recv.at[w]).wait()

    def send(w, some=range(cores)):
        for core in some:
            checked[...] = pieces[w, :, core].astype(F32).max(axis=0)
        if geo.scatter:
            for core in some:
                for ih in range(2):
                    piece_copy(w, ih, core, "start")

    def attend(w):
        x = jnp.concatenate([own[w], halo[w]], axis=0).astype(F32)
        n1 = layer_norm(x[half:]).astype(BF16)
        target = position[0:1, :] + (var * geo.row_count + WIN_LAT * w + half_lat)
        target = jnp.where(target >= geo.rows, target - geo.rows, target)
        there = lax.broadcasted_iota(jnp.int32, (geo.rows, KEYS), 0) == target
        there = there.astype(F32).astype(BF16)
        opened = jnp.zeros((1, KEYS), F32)
        column = lax.broadcasted_iota(jnp.int32, (geo.cols, KEYS), 0)
        for h in range(2):
            seen = (marks[h] > 0).astype(F32).astype(BF16)
            seen = jnp.dot(seen, there, preferred_element_type=F32)
            seen = jnp.where(column == position[1 + h : 2 + h, :], seen, 0.0)
            opened = opened + jnp.sum(seen, axis=0, keepdims=True)
        allowed = jnp.logical_or(jnp.broadcast_to(opened, diagonal.shape) > 0.5, diagonal)
        cut = jnp.logical_and(var == cores - 1, w == windows - 1)
        bias = jnp.where(allowed, 0.0, -1e30) + differs[...] * jnp.where(cut, 1.0, 0.0)
        yield
        scores, values = [], []
        for s in range(cores):
            q, k, v = (
                jnp.concatenate(
                    [ready[s, i, w], jnp.dot(n1, qkv[s, i], preferred_element_type=F32).astype(BF16)], axis=0
                )
                for i in range(3)
            )
            q = q * jnp.asarray(HD ** (-0.5), BF16)
            tail = jnp.zeros((KEYS - tokens, width), BF16)
            k = jnp.concatenate([k, tail], axis=0)
            values.append(jnp.concatenate([v, tail], axis=0))
            q_all = jnp.concatenate(
                [jnp.where(lane_head == h, q, jnp.zeros_like(q)) for h in range(heads)], axis=0
            )
            yield
            scores.append(lax.dot_general(q_all, k, NT, preferred_element_type=F32))
            yield
        attended = x
        for s in range(cores):
            weights = []
            for h in range(heads):
                one = scores[s][h * tokens : (h + 1) * tokens] + bias
                peak = jnp.max(one, axis=-1, keepdims=True)
                e = jnp.exp(one - peak)
                total = jnp.sum(e, axis=-1, keepdims=True)
                weights.append((e * (1.0 / total)).astype(BF16))
            weights = jnp.concatenate(weights, axis=1)
            v = values[s]
            v_all = jnp.concatenate(
                [jnp.where(lane_head_keys == h, v, jnp.zeros_like(v)) for h in range(heads)], axis=0
            )
            context = jnp.dot(weights, v_all, preferred_element_type=F32).astype(BF16)
            yield
            attended = attended + jnp.dot(context, proj[s], preferred_element_type=F32)
            if s == cores - 1:
                x_one[w] = attended
            yield

    def finish(w):
        n2 = layer_norm(x_one[w]).astype(BF16)
        yield
        for s in range(cores):
            for c in range(0, units, CHUNK):
                one = jnp.dot(n2, up[s, :, c : c + CHUNK], preferred_element_type=F32)
                one = 0.5 * one * (1.0 + lax.erf(one * 2.0 ** (-0.5)))
                hid[:, s * units + c : s * units + c + CHUNK] = one.astype(BF16)
                yield
        latent = x_one[w] + jnp.dot(
            hid[...], down[...].reshape(cores * units, features), preferred_element_type=F32
        )
        yield
        n3 = layer_norm(latent.astype(BF16).astype(F32)).astype(BF16)
        n3 = jnp.dot(order[...], n3, preferred_element_type=F32).astype(BF16)
        n3, others = n3[:BLOCK], n3[BLOCK:]
        yield
        base = lax.dot_general(fold_base[...], n3, NT, preferred_element_type=F32)
        base_pix[...] = base[:pixels] + base[pixels:]
        for s in range(cores):
            g = lax.dot_general(fold[s, 0 : 2 * count, :], others, NT, preferred_element_type=F32)
            g = g[:count] + g[count:]
            scores = [jnp.zeros((count, BLOCK), F32)]
            scores += [g[:, j * BLOCK : (j + 1) * BLOCK] for j in range(levels - 1)]
            peak = functools.reduce(jnp.maximum, scores)
            e = [jnp.exp(one - peak) for one in scores]
            inverse = 1.0 / sum(e)
            u = lax.dot_general(fold[s, 2 * count :, :], others, NT, preferred_element_type=F32)
            for j in range(levels - 1):
                dw[j, s * count : (s + 1) * count, :] = e[j + 1] * inverse
                du[j, s * heads * pixels : (s + 1) * heads * pixels, :] = u[:, j * BLOCK : (j + 1) * BLOCK]
        yield

    def paint(w):
        low = pixels // cores
        lane = lax.broadcasted_iota(jnp.int32, (2 * row_size, BLOCK), 1) - lane_base
        lane = jnp.where(lane < 0, lane + BLOCK, lane)
        for core in range(cores):
            top = core * low
            for part in range(top, top + low, 8):
                totals = [base_pix[part : part + 8, :]] * geo.isobars
                for s in range(cores):
                    for h in range(heads):
                        for j in range(levels - 1):
                            at = (s * heads + h) * pixels + part
                            value = du[j, at : at + 8, :]
                            for level in range(geo.isobars):
                                row = s * count + level * heads + h
                                totals[level] = totals[level] + dw[j, row : row + 1, :] * value
                for level in range(geo.isobars):
                    pix[level, part : part + 8, :] = totals[level]
            total = jnp.zeros((rows, 4 * BLOCK), F32)
            for b in range(SQUARE_SPAN):
                at = top + b * row_size
                part = pix[:, at : at + row_size, :].reshape(rows, BLOCK)
                total = total + jnp.dot(part.astype(BF16), pick[b], preferred_element_type=F32)
            for ih in range(2):
                left = jnp.zeros((2 * row_size, BLOCK), F32)
                for k in range(geo.slots // 2):
                    at = slice(2 * row_size * k, 2 * row_size * (k + 1))
                    inside = jnp.logical_and(lane >= extra * k, lane < extra * (k + 1))
                    left = jnp.where(inside, total[at, (2 + ih) * BLOCK : (3 + ih) * BLOCK], left)
                main = total[:, ih * BLOCK : (ih + 1) * BLOCK]
                pieces[w, ih, core] = jnp.concatenate([main, left], axis=0).astype(BF16)
            yield

    def run(order="", **steps):
        for name in order:
            next(steps[name])

    mask_copy, qkv_copy, proj_copy, up_copy, down_copy, fold_copy = copies
    for copy in (mask_copy, qkv_copy, proj_copy):
        copy.wait()
    lane_base = lax.rem(grid * geo.run + bands * geo.run - geo.run // 2, BLOCK) if geo.scatter else 0
    if geo.scatter:
        for b in range(SQUARE_SPAN):
            for part in range(4):
                lanes = slice(part * BLOCK, (part + 1) * BLOCK)
                pick[b, :, lanes] = pltpu.roll(pick[b, :, lanes].astype(F32), lane_base, 1).astype(BF16)
    n_own = layer_norm(own[...].reshape(windows * half, features).astype(F32)).astype(BF16)
    for s in range(cores):
        for i in range(3):
            one = jnp.dot(n_own, qkv[s, i], preferred_element_type=F32).astype(BF16)
            ready[s, i] = one.reshape(windows, half, width)
    arrive(turn(0))
    run("a" * ORDER.count("a"), a=attend(turn(0)))
    for copy in (up_copy, down_copy, fold_copy):
        copy.wait()
    whole = jnp.zeros((pixels, features), F32)
    for s in range(cores):
        for h in range(heads):
            top = 2 * count + h * pixels
            whole = whole + fold[s, top : top + pixels, :].astype(F32)
    whole_hi = whole.astype(BF16)
    fold_base[0:pixels, :] = whole_hi
    fold_base[pixels:, :] = (whole - whole_hi.astype(F32)).astype(BF16)

    last = windows - 1

    def complete(w):
        yield from finish(w)
        yield from paint(w)

    @pl.loop(0, last)
    def _(step):
        arrive(turn(step + 1))
        run(ORDER, a=attend(turn(step + 1)), b=complete(turn(step)))
        send(turn(step))

    finishing = complete(turn(last))
    run("b" * (ORDER.count("b") - cores), b=finishing)
    for core in range(cores):
        next(finishing)
        send(turn(last), (core,))

    for copy in halos:
        copy.wait_send()
    if geo.scatter:

        @pl.loop(0, bands)
        def _(s):
            for ih in range(2):
                target = out_ref.at[s, ih]
                pltpu.make_async_copy(target, target, piece_recv.at[s, ih]).wait()

        @pl.loop(0, windows)
        def _(w):
            for ih in range(2):
                for core in range(cores):
                    piece_copy(w, ih, core, "finish")

    else:
        copy = pltpu.make_async_copy(pieces, out_ref, load_sem.at[0])
        copy.start()
        copy.wait()


def forecast(geo, *args):
    tables = (
        jnp.asarray(geo.order_table(), BF16),
        jnp.asarray(geo.position_table(), jnp.int32),
        jnp.asarray(geo.pixel_table(), BF16),
        jnp.asarray(geo.pick_table(), BF16),
    )
    features, width, cores, windows = geo.features, geo.width, geo.cores, geo.windows
    units = args[4].shape[1]
    fold_rows = geo.heads * (2 * LEVEL_SLOTS + geo.pixels)
    vmem = pltpu.VMEM
    dma = pltpu.SemaphoreType.DMA
    if geo.scatter:
        out_shape = (geo.bands, 2, BLOCK, BLOCK)
    else:
        out_shape = (windows, 2, cores, BLOCK, BLOCK)
    return pl.pallas_call(
        functools.partial(main_kernel, geo),
        out_shape=jax.ShapeDtypeStruct(out_shape, BF16),
        in_specs=[pl.BlockSpec(memory_space=pltpu.HBM)] * (len(args) + len(tables)),
        out_specs=pl.BlockSpec(memory_space=vmem if geo.scatter else pltpu.HBM),
        scratch_shapes=[
            vmem((geo.cols, geo.levels, geo.taken, features), BF16),
            vmem((2, geo.cols, geo.rows), jnp.int32),
            vmem((cores, 3, features, width), BF16),
            vmem((cores, width, features), BF16),
            vmem((cores, features, units), BF16),
            vmem((cores, units, features), BF16),
            *[vmem(one.shape, one.dtype) for one in args[6:]],
            *[vmem(one.shape, one.dtype) for one in tables],
            vmem((cores, fold_rows, features), BF16),
            vmem((windows, geo.half, features), BF16),
            vmem((windows, geo.half, features), BF16),
            vmem((windows, geo.half, features), BF16),
            vmem((geo.tokens, KEYS), F32),
            vmem((geo.tokens, cores * units), BF16),
            vmem((geo.levels - 1, cores * geo.heads * LEVEL_SLOTS, BLOCK), F32),
            vmem((geo.levels - 1, cores * geo.heads * geo.pixels, BLOCK), F32),
            vmem((cores, 3, windows, geo.half, width), BF16),
            vmem((2 * geo.pixels, features), BF16),
            vmem((windows, geo.tokens, features), F32),
            vmem((geo.pixels, BLOCK), F32),
            vmem((geo.slots, geo.pixels, BLOCK), F32),
            vmem((windows, 2, cores, BLOCK, BLOCK), BF16),
            vmem((BLOCK, BLOCK), F32),
            dma((geo.taken // 4 + 15,)),
            dma((6,)),
            dma((6,)),
            dma((windows,)),
            dma((windows,)),
            dma((windows, 2, cores)),
            dma((geo.bands, 2)),
        ],
        compiler_params=pltpu.CompilerParams(
            collective_id=0, has_side_effects=True, vmem_limit_bytes=30 * 2**20
        ),
    )(*[pltpu.with_memory_space_constraint(one, pltpu.HBM) for one in (*args, *tables)])


def assemble_kernel(isobars, run, got_ref, out_ref, out, sems):
    bands = got_ref.shape[0]
    half_lat = WIN_LAT // 2
    groups = (isobars + 1) // 2
    tiles = out.shape[-1] // BLOCK
    extra = half_lat * run - BLOCK
    bases = lane_bases(bands, run)
    lane = lax.broadcasted_iota(jnp.int32, (1, BLOCK), 1)
    sublane = lax.broadcasted_iota(jnp.int32, (1, 8, BLOCK), 1)

    def around(start, length):
        start = start % BLOCK
        if start + length <= BLOCK:
            return jnp.logical_and(lane >= start, lane < start + length)
        return jnp.logical_or(lane >= start, lane < start + length - BLOCK)

    def put(merged, value, start, length):
        while length > 0:
            start = start % (tiles * BLOCK)
            tile, part = start // BLOCK, min(length, BLOCK - start % BLOCK)
            old = merged[tile]
            merged[tile] = value if old is None else jnp.where(around(start, part), value, old)
            start, length = start + part, length - part

    copies = []
    middle = (groups + 1) // 2
    for first, last in ((0, middle), (middle, groups)):
        low, high = 2 * first, min(2 * last, isobars)
        found = {}
        for ih in range(2):
            pieces = [got_ref[s, ih, 16 * first : 16 * last, :].astype(F32) for s in range(bands)]
            rests = [got_ref[s, ih, 16 * groups : 16 * groups + 16, :].astype(F32) for s in range(bands)]
            left = []
            for k in range(first, last):
                one = rests[0]
                for s in range(1, bands):
                    one = jnp.where(around(bases[s] + extra * k, extra), rests[s], one)
                left.append(pltpu.roll(one, (-extra * k) % BLOCK, 1) if k > 0 else one)
            left = jnp.concatenate(left, axis=0)
            for r in range(half_lat):
                merged = [None] * tiles
                for s in range(bands):
                    put(merged, pieces[s], bases[s] + run * r, min(run, BLOCK - run * r))
                if run * (r + 1) > BLOCK:
                    for s in range(bands):
                        put(merged, left, bases[s] + BLOCK, run * (r + 1) - BLOCK)
                if r > 0:
                    merged = [pltpu.roll(one, BLOCK - run * r, 1) for one in merged]
                    merged = [
                        jnp.where(lane < BLOCK - run * r, merged[t], merged[(t + 1) % tiles])
                        for t in range(tiles)
                    ]
                found[(1 - ih) * half_lat + r] = merged
        for top in range(0, 2 * half_lat, 2):
            for t in range(tiles):
                upper = found[top][t].reshape(-1, 8, BLOCK)
                lower = found[top + 1][t].reshape(-1, 8, BLOCK)
                some = (
                    jnp.where(sublane < 4, upper, pltpu.roll(lower, 4, 1)),
                    jnp.where(sublane < 4, pltpu.roll(upper, 4, 1), lower),
                )
                for v in range(2):
                    out[v, low:high, 4 * top : 4 * top + 8, t * BLOCK : (t + 1) * BLOCK] = some[v][: high - low]
        for v in range(2):
            copy = pltpu.make_async_copy(
                out.at[v, low:high], out_ref.at[v, low:high], sems.at[len(copies)]
            )
            copy.start()
            copies.append(copy)
    for copy in copies:
        copy.wait()


def assemble(got, geo):
    shape = (TARGET_QUANTITY // geo.cores, geo.isobars, WIN_LAT * SQUARE_SPAN, geo.bands * geo.run)
    return pl.pallas_call(
        functools.partial(assemble_kernel, geo.isobars, geo.run),
        out_shape=jax.ShapeDtypeStruct(shape, F32),
        out_specs=pl.BlockSpec(memory_space=pltpu.HBM),
        scratch_shapes=[pltpu.VMEM(shape, F32), pltpu.SemaphoreType.DMA((4,))],
        compiler_params=pltpu.CompilerParams(vmem_limit_bytes=40 * 2**20),
    )(got)


def exchange(pieces, geo):
    half_lat = WIN_LAT // 2
    run = geo.cols * SQUARE_SPAN
    quantities = TARGET_QUANTITY // geo.cores
    rows = geo.slots * quantities * SQUARE_SPAN
    extra = half_lat * run - BLOCK
    lead = pieces.shape[:3]
    main = pieces[:, :, :, :rows].reshape(*lead, geo.slots, quantities, SQUARE_SPAN, BLOCK)
    rest = pieces[:, :, :, rows:, : extra * (geo.slots // 2)]
    rest = rest.reshape(*lead, 2, quantities, SQUARE_SPAN, geo.slots // 2, extra)
    rest = jnp.moveaxis(rest, 6, 3).reshape(*lead, geo.slots, quantities, SQUARE_SPAN, extra)
    maps = jnp.concatenate([main, rest], axis=-1)[:, :, :, : geo.isobars]
    maps = maps.reshape(*lead, geo.isobars, quantities, SQUARE_SPAN, half_lat, run)
    maps = jnp.transpose(maps, (2, 4, 3, 0, 1, 6, 5, 7))
    maps = maps.reshape(TARGET_QUANTITY, geo.isobars, geo.row_count * SQUARE_SPAN, run)
    maps = lax.all_to_all(maps, "var", split_axis=0, concat_axis=2, tiled=True)
    maps = jnp.roll(maps, half_lat * SQUARE_SPAN, 2)
    maps = lax.all_to_all(maps, "grid", split_axis=2, concat_axis=3, tiled=True)
    return jnp.roll(maps, -(run // 2), 3).astype(F32)


def local(
    tokens,
    key_mask,
    w_qkv,
    w_proj,
    w_up,
    w_down,
    level_query,
    w_dec_q,
    w_dec_kv,
    w_dec_o,
    decode_matrix,
):
    geo = Geometry(
        tokens, w_proj, level_query, decode_matrix, lax.axis_size("var"), lax.axis_size("grid")
    )
    pieces = forecast(
        geo,
        jnp.transpose(tokens, (1, 2, 0, 3)),
        key_mask.T,
        w_qkv,
        w_proj,
        w_up,
        w_down,
        level_query,
        w_dec_q,
        w_dec_kv,
        w_dec_o,
        decode_matrix.T,
    )
    if geo.scatter:
        return assemble(pieces, geo)
    return exchange(pieces, geo)


def solution(mesh):
    placed = (
        P("group", "grid", None, None),
        P("group", "grid"),
        P(None, None, "var"),
        P("var", None),
        P(None, "var"),
        P("var", None),
        P(),
        P(None, "var"),
        P(None, None, "var"),
        P("var", None),
        P(),
    )
    return jax.shard_map(
        local,
        mesh=mesh,
        in_specs=placed,
        out_specs=P("var", "group", "grid", None),
        check_vma=False,
    )
```

```python
import functools

import jax
import jax.numpy as jnp
import numpy as np
from jax import lax
from jax.experimental import pallas as pl
from jax.experimental.pallas import tpu as pltpu
from jax.sharding import PartitionSpec as P

HD = 64
TARGET_QUANTITY = 4
SQUARE_SPAN = 4
WIN_LAT = 6
EPSILON = 1e-05
BLOCK = 128
KEYS = 256
CHUNK = 256
LEVEL_SLOTS = 16
ORDER = "aabaabbbbaabbbbabababbb"
MESH = pl.DeviceIdType.MESH
NT = (((1,), (1,)), ((), ()))
F32 = jnp.float32
BF16 = jnp.bfloat16


def layer_norm(values):
    center = values - jnp.mean(values, axis=-1, keepdims=True)
    spread = jnp.mean(center * center, axis=-1, keepdims=True)
    return center * lax.rsqrt(spread + EPSILON)


def lane_bases(bands, run):
    return [(s * run + bands * run - run // 2) % (bands * run) for s in range(bands)]


class Geometry:
    def __init__(self, tokens, w_proj, level_query, decode_matrix, cores, bands):
        self.rows, self.cols, self.levels, self.features = tokens.shape
        self.cores, self.bands = cores, bands
        self.half_cols = self.cols // 2
        self.row_count = self.rows // cores
        self.windows = self.row_count // WIN_LAT
        self.taken = 8 * (-(-(self.row_count + WIN_LAT // 2) // 8))
        self.half_patches = WIN_LAT * self.half_cols
        self.half = 16 * (-(-(self.levels * self.half_patches) // 16))
        self.tokens = 2 * self.half
        self.patches = 2 * self.half_patches
        self.width = w_proj.shape[0]
        self.heads = self.width // HD
        self.isobars = level_query.shape[0]
        self.slots = self.isobars + self.isobars % 2
        self.pixels = decode_matrix.shape[1]
        self.run = self.cols * SQUARE_SPAN
        self.extra = WIN_LAT // 2 * self.run - BLOCK
        self.bases = lane_bases(bands, self.run)
        covered = [(base + lane) % BLOCK for base in self.bases for lane in range(self.extra)]
        self.scatter = (
            bands * WIN_LAT == self.rows
            and (bands * self.run) % BLOCK == 0
            and self.extra * (self.slots // 2) <= BLOCK
            and sorted(covered) == list(range(BLOCK))
        )

    def place(self, half, level, r, c):
        return half * self.half + level * self.half_patches + r * self.half_cols + c

    def each(self):
        for half in range(2):
            for level in range(self.levels):
                for r in range(WIN_LAT):
                    for c in range(self.half_cols):
                        yield half, level, r, c

    def order_table(self):
        table = np.zeros((self.levels * BLOCK, self.tokens), np.float32)
        for half, level, r, c in self.each():
            patch = r * self.cols + (1 - half) * self.half_cols + c
            table[level * BLOCK + patch, self.place(half, level, r, c)] = 1.0
            if level > 0:
                table[level * BLOCK + patch, self.place(half, 0, r, c)] = -1.0
        return table

    def position_table(self):
        table = np.full((8, KEYS), -1, np.int32)
        table[0] = 0
        for half, level, r, c in self.each():
            at = self.place(half, level, r, c)
            table[0, at] = r
            table[1 + half, at] = c + half * self.half_cols
        return table

    def pixel_table(self):
        table = np.zeros((self.pixels, self.pixels), np.float32)
        own = TARGET_QUANTITY // self.cores
        for v in range(TARGET_QUANTITY):
            for a in range(SQUARE_SPAN):
                for b in range(SQUARE_SPAN):
                    target = ((v // own * SQUARE_SPAN + b) * own + v % own) * SQUARE_SPAN + a
                    table[target, (v * SQUARE_SPAN + a) * SQUARE_SPAN + b] = 1.0
        return table

    def pick_table(self):
        half_lat = WIN_LAT // 2
        run = self.cols * SQUARE_SPAN
        extra = half_lat * run - BLOCK
        picks = np.zeros((SQUARE_SPAN, BLOCK, 4 * BLOCK), np.float32)
        for ih in range(2):
            for q in range(half_lat * run):
                r, rest = divmod(q, run)
                column, b = divmod(rest, SQUARE_SPAN)
                source = (half_lat * ih + r) * self.cols + column
                if q < BLOCK:
                    picks[b, source, ih * BLOCK + q] = 1.0
                else:
                    for k in range(self.slots // 2):
                        picks[b, source, (2 + ih) * BLOCK + extra * k + q - BLOCK] = 1.0
        return picks


def fold_decoder(lq, wq, wkv_ref, wo, dm, perm, out_ref):
    width = wq.shape[1]
    heads = width // HD
    dquery = jnp.dot(lq, wq, preferred_element_type=F32) * HD ** (-0.5)
    d_hi = dquery.astype(BF16)
    d_lo = (dquery - d_hi.astype(F32)).astype(BF16)
    count = LEVEL_SLOTS * heads
    row = lax.broadcasted_iota(jnp.int32, (count, dquery.shape[0]), 0)
    slot = lax.broadcasted_iota(jnp.int32, (count, dquery.shape[0]), 1)
    spread = (row // heads == slot).astype(F32).astype(BF16)
    row = lax.broadcasted_iota(jnp.int32, (count, width), 0)
    mine = row % heads == lax.broadcasted_iota(jnp.int32, (count, width), 1) // HD
    q_hi = jnp.dot(spread, d_hi, preferred_element_type=F32)
    q_hi = jnp.where(mine, q_hi, 0.0).astype(BF16)
    q_lo = jnp.dot(spread, d_lo, preferred_element_type=F32)
    q_lo = jnp.where(mine, q_lo, 0.0).astype(BF16)
    wk = wkv_ref[0]
    g = lax.dot_general(q_hi, wk, NT, preferred_element_type=F32)
    g = g + lax.dot_general(q_lo, wk, NT, preferred_element_type=F32)
    g_hi = g.astype(BF16)
    out_ref[0, 0:count, :] = g_hi
    out_ref[0, count : 2 * count, :] = (g - g_hi.astype(F32)).astype(BF16)
    dm_hi = dm.astype(BF16)
    dm_lo = (dm - dm_hi.astype(F32)).astype(BF16)
    dm_hi = jnp.dot(perm, dm_hi, preferred_element_type=F32).astype(BF16)
    dm_lo = jnp.dot(perm, dm_lo, preferred_element_type=F32).astype(BF16)
    m_t = lax.dot_general(dm_hi, wo, NT, preferred_element_type=F32)
    m_t = m_t + lax.dot_general(dm_lo, wo, NT, preferred_element_type=F32)
    pixels = m_t.shape[0]
    stacked = jnp.concatenate([m_t] * heads, axis=0)
    row_head = lax.broadcasted_iota(jnp.int32, stacked.shape, 0) // pixels
    lane_head = lax.broadcasted_iota(jnp.int32, stacked.shape, 1) // HD
    stacked = jnp.where(row_head == lane_head, stacked, 0.0)
    s_hi = stacked.astype(BF16)
    s_lo = (stacked - s_hi.astype(F32)).astype(BF16)
    wv = wkv_ref[1]
    n_t = lax.dot_general(s_hi, wv, NT, preferred_element_type=F32)
    n_t = n_t + lax.dot_general(s_lo, wv, NT, preferred_element_type=F32)
    out_ref[0, 2 * count :, :] = n_t.astype(BF16)


def main_kernel(
    geo,
    tok_ref,
    mask_ref,
    wqkv_ref,
    wproj_ref,
    wup_ref,
    wdown_ref,
    lq_ref,
    wq_ref,
    wkv_ref,
    wo_ref,
    dm_ref,
    order_ref,
    position_ref,
    perm_ref,
    pick_ref,
    out_ref,
    raw,
    marks,
    qkv,
    proj,
    up,
    down,
    lq,
    wq,
    wkv,
    wo,
    dm,
    order,
    position,
    perm,
    pick,
    fold,
    first,
    own,
    halo,
    differs,
    hid,
    dw,
    du,
    ready,
    fold_base,
    x_one,
    base_pix,
    pix,
    pieces,
    checked,
    load_sem,
    weight_send,
    weight_recv,
    halo_send,
    halo_recv,
    piece_send,
    piece_recv,
):
    group, grid, var = (lax.axis_index(name) for name in ("group", "grid", "var"))
    bands, cores, windows, half = geo.bands, geo.cores, geo.windows, geo.half
    features, levels, width, heads = geo.features, geo.levels, geo.width, geo.heads
    sibling = (group, grid, lax.rem(var + 1, cores))

    def turn(step, column=grid):
        near = column * cores // bands == var
        rest = lax.rem(step + column + windows - 2, windows - 1)
        return jnp.where(near, jnp.where(step == 0, windows - 1, rest), step)

    east_grid = lax.rem(grid + 1, bands)
    west = (group, lax.rem(grid + bands - 1, bands), var)
    east = (group, east_grid, var)
    barrier = pltpu.get_barrier_semaphore()
    if geo.scatter:
        peers = bands * cores
        me = grid * cores + var

        @pl.loop(1, peers)
        def _(step):
            peer = lax.rem(me + step, peers)
            pl.semaphore_signal(
                barrier, inc=1, device_id=(group, peer // cores, lax.rem(peer, cores)), device_id_type=MESH
            )

        greeted = peers - 1
    else:
        for peer in (sibling, west, east):
            pl.semaphore_signal(barrier, inc=1, device_id=peer, device_id_type=MESH)
        greeted = 3

    loads = []

    def load(source, target):
        copy = pltpu.make_async_copy(source, target, load_sem.at[len(loads)])
        copy.start()
        loads.append(copy)
        return copy

    tiles = geo.rows // 8
    first_tile = var * (geo.row_count // 8)
    slabs = []
    for h in (1, 0):
        for s in range(geo.taken // 8):
            tile = lax.rem(first_tile + s, tiles)
            some = slice(h * geo.half_cols, (h + 1) * geo.half_cols)
            slabs.append(
                load(
                    tok_ref.at[some, :, pl.ds(pl.multiple_of(tile * 8, 8), 8), :],
                    raw.at[some, :, 8 * s : 8 * s + 8, :],
                )
            )
    fold_loads = [
        load(a, b)
        for a, b in ((lq_ref, lq), (wq_ref, wq), (wkv_ref, wkv), (wo_ref, wo), (dm_ref, dm), (perm_ref, perm))
    ]
    late_loads = [
        load(a, b)
        for a, b in (
            (mask_ref, marks.at[0]),
            (wqkv_ref, qkv.at[0]),
            (wproj_ref, proj.at[0]),
            (wup_ref, up.at[0]),
            (wdown_ref, down.at[0]),
            (position_ref, position),
            (order_ref, order),
            (pick_ref, pick),
        )
    ]

    depth = geo.half_cols * levels * geo.taken

    at = lax.broadcasted_iota(jnp.int32, (half, depth), 0)
    level = sum(jnp.where(at >= geo.half_patches * n, 1, 0) for n in range(1, levels))
    at = at - geo.half_patches * level
    row = sum(jnp.where(at >= geo.half_cols * n, 1, 0) for n in range(1, WIN_LAT + 1))
    wanted = ((at - geo.half_cols * row) * levels + level) * geo.taken + row + WIN_LAT // 2
    wanted = jnp.where(row < WIN_LAT, wanted, depth * 2)
    wanted = lax.broadcasted_iota(jnp.int32, (half, depth), 1) - wanted

    def collect(h, w, target):
        slab = raw[h * geo.half_cols : (h + 1) * geo.half_cols].reshape(depth, features)
        picked = (wanted == WIN_LAT * w).astype(F32).astype(BF16)
        target[w] = jnp.dot(picked, slab, preferred_element_type=F32).astype(BF16)

    for copy in slabs[: len(slabs) // 2]:
        copy.wait()
    collect(1, turn(0, east_grid), first)
    pl.semaphore_wait(barrier, greeted)

    def remote(source, target, send, recv, peer):
        copy = pltpu.make_async_remote_copy(
            src_ref=source, dst_ref=target, send_sem=send, recv_sem=recv, device_id=peer, device_id_type=MESH
        )
        copy.start()
        return copy

    copies = [remote(mask_ref, marks.at[1], weight_send.at[0], weight_recv.at[0], east)]
    halos = []

    def pass_on(step):
        w = turn(step, east_grid)
        halos.append(remote(first.at[w], halo.at[w], halo_send.at[w], halo_recv.at[w], east))

    pass_on(0)
    for n, (source, target) in enumerate(((wqkv_ref, qkv), (wproj_ref, proj), (wup_ref, up), (wdown_ref, down))):
        copies.append(remote(source, target.at[1], weight_send.at[n + 1], weight_recv.at[n + 1], sibling))

    for step in range(1, windows):
        collect(1, turn(step, east_grid), first)
    pass_on(1)
    for copy in slabs[len(slabs) // 2 :]:
        copy.wait()
    for step in range(windows):
        collect(0, turn(step), own)
    for step in range(2, windows):
        pass_on(step)
    for copy in fold_loads:
        copy.wait()
    fold_decoder(lq[...], wq[...], wkv, wo[...], dm[...], perm[...], fold)

    tokens = geo.tokens
    q_pos = lax.broadcasted_iota(jnp.int32, (tokens, KEYS), 0)
    k_pos = lax.broadcasted_iota(jnp.int32, (tokens, KEYS), 1)
    diagonal = q_pos == k_pos

    def region_of(pos):
        pos = jnp.where(pos >= half, pos - half, pos)
        for level in range(levels - 1, 0, -1):
            start = geo.half_patches * level
            pos = jnp.where(pos >= start, pos - start, pos)
        return pos >= geo.half_patches // 2

    differs[...] = jnp.where(region_of(q_pos) != region_of(k_pos), -1e30, 0.0)
    lane_head = lax.broadcasted_iota(jnp.int32, (tokens, width), 1) // HD
    lane_head_keys = lax.broadcasted_iota(jnp.int32, (KEYS, width), 1) // HD

    for copy in late_loads:
        copy.wait()
    copies.append(remote(fold.at[0], fold.at[1], weight_send.at[5], weight_recv.at[5], sibling))

    count = heads * LEVEL_SLOTS
    pixels = geo.pixels
    row_size = pixels // cores // SQUARE_SPAN
    rows = geo.slots * row_size
    half_lat = WIN_LAT // 2
    extra = half_lat * geo.cols * SQUARE_SPAN - BLOCK
    pix[geo.isobars :] = jnp.zeros((geo.slots - geo.isobars, pixels, BLOCK), F32)
    units = up.shape[2]

    def piece_copy(w, ih, core, action):
        band = lax.rem(var * windows + w + ih, bands)
        here = jnp.logical_and(band == grid, core == var)
        source, target = pieces.at[w, ih, core], out_ref.at[grid, ih]

        @pl.when(here)
        def _():
            if action == "start":
                pltpu.make_async_copy(source, target, piece_recv.at[grid, ih]).start()

        @pl.when(jnp.logical_not(here))
        def _():
            if action == "start":
                pltpu.make_async_remote_copy(
                    src_ref=source,
                    dst_ref=target,
                    send_sem=piece_send.at[w, ih, core],
                    recv_sem=piece_recv.at[grid, ih],
                    device_id=(group, band, core),
                    device_id_type=MESH,
                ).start()
            else:
                pltpu.make_async_copy(source, source, piece_send.at[w, ih, core]).wait()

    def arrive(w):
        pltpu.make_async_copy(halo.at[w], halo.at[w], halo_recv.at[w]).wait()

    def send(w, some=range(cores)):
        for core in some:
            checked[...] = pieces[w, :, core].astype(F32).max(axis=0)
        if geo.scatter:
            for core in some:
                for ih in range(2):
                    piece_copy(w, ih, core, "start")

    def attend(w):
        x = jnp.concatenate([own[w], halo[w]], axis=0).astype(F32)
        n1 = layer_norm(x[half:]).astype(BF16)
        target = position[0:1, :] + (var * geo.row_count + WIN_LAT * w + half_lat)
        target = jnp.where(target >= geo.rows, target - geo.rows, target)
        there = lax.broadcasted_iota(jnp.int32, (geo.rows, KEYS), 0) == target
        there = there.astype(F32).astype(BF16)
        opened = jnp.zeros((1, KEYS), F32)
        column = lax.broadcasted_iota(jnp.int32, (geo.cols, KEYS), 0)
        for h in range(2):
            seen = (marks[h] > 0).astype(F32).astype(BF16)
            seen = jnp.dot(seen, there, preferred_element_type=F32)
            seen = jnp.where(column == position[1 + h : 2 + h, :], seen, 0.0)
            opened = opened + jnp.sum(seen, axis=0, keepdims=True)
        allowed = jnp.logical_or(jnp.broadcast_to(opened, diagonal.shape) > 0.5, diagonal)
        cut = jnp.logical_and(var == cores - 1, w == windows - 1)
        bias = jnp.where(allowed, 0.0, -1e30) + differs[...] * jnp.where(cut, 1.0, 0.0)
        yield
        scores, values = [], []
        for s in range(cores):
            q, k, v = (
                jnp.concatenate(
                    [ready[s, i, w], jnp.dot(n1, qkv[s, i], preferred_element_type=F32).astype(BF16)], axis=0
                )
                for i in range(3)
            )
            q = q * jnp.asarray(HD ** (-0.5), BF16)
            tail = jnp.zeros((KEYS - tokens, width), BF16)
            k = jnp.concatenate([k, tail], axis=0)
            values.append(jnp.concatenate([v, tail], axis=0))
            q_all = jnp.concatenate(
                [jnp.where(lane_head == h, q, jnp.zeros_like(q)) for h in range(heads)], axis=0
            )
            yield
            scores.append(lax.dot_general(q_all, k, NT, preferred_element_type=F32))
            yield
        attended = x
        for s in range(cores):
            weights = []
            for h in range(heads):
                one = scores[s][h * tokens : (h + 1) * tokens] + bias
                peak = jnp.max(one, axis=-1, keepdims=True)
                e = jnp.exp(one - peak)
                total = jnp.sum(e, axis=-1, keepdims=True)
                weights.append((e * (1.0 / total)).astype(BF16))
            weights = jnp.concatenate(weights, axis=1)
            v = values[s]
            v_all = jnp.concatenate(
                [jnp.where(lane_head_keys == h, v, jnp.zeros_like(v)) for h in range(heads)], axis=0
            )
            context = jnp.dot(weights, v_all, preferred_element_type=F32).astype(BF16)
            yield
            attended = attended + jnp.dot(context, proj[s], preferred_element_type=F32)
            if s == cores - 1:
                x_one[w] = attended
            yield

    def finish(w):
        n2 = layer_norm(x_one[w]).astype(BF16)
        yield
        for s in range(cores):
            for c in range(0, units, CHUNK):
                one = jnp.dot(n2, up[s, :, c : c + CHUNK], preferred_element_type=F32)
                one = 0.5 * one * (1.0 + lax.erf(one * 2.0 ** (-0.5)))
                hid[:, s * units + c : s * units + c + CHUNK] = one.astype(BF16)
                yield
        latent = x_one[w] + jnp.dot(
            hid[...], down[...].reshape(cores * units, features), preferred_element_type=F32
        )
        yield
        n3 = layer_norm(latent.astype(BF16).astype(F32)).astype(BF16)
        n3 = jnp.dot(order[...], n3, preferred_element_type=F32).astype(BF16)
        n3, others = n3[:BLOCK], n3[BLOCK:]
        yield
        base = lax.dot_general(fold_base[...], n3, NT, preferred_element_type=F32)
        base_pix[...] = base[:pixels] + base[pixels:]
        for s in range(cores):
            g = lax.dot_general(fold[s, 0 : 2 * count, :], others, NT, preferred_element_type=F32)
            g = g[:count] + g[count:]
            scores = [jnp.zeros((count, BLOCK), F32)]
            scores += [g[:, j * BLOCK : (j + 1) * BLOCK] for j in range(levels - 1)]
            peak = functools.reduce(jnp.maximum, scores)
            e = [jnp.exp(one - peak) for one in scores]
            inverse = 1.0 / sum(e)
            u = lax.dot_general(fold[s, 2 * count :, :], others, NT, preferred_element_type=F32)
            for j in range(levels - 1):
                dw[j, s * count : (s + 1) * count, :] = e[j + 1] * inverse
                du[j, s * heads * pixels : (s + 1) * heads * pixels, :] = u[:, j * BLOCK : (j + 1) * BLOCK]
        yield

    def paint(w):
        low = pixels // cores
        lane = lax.broadcasted_iota(jnp.int32, (2 * row_size, BLOCK), 1) - lane_base
        lane = jnp.where(lane < 0, lane + BLOCK, lane)
        for core in range(cores):
            top = core * low
            for part in range(top, top + low, 8):
                totals = [base_pix[part : part + 8, :]] * geo.isobars
                for s in range(cores):
                    for h in range(heads):
                        for j in range(levels - 1):
                            at = (s * heads + h) * pixels + part
                            value = du[j, at : at + 8, :]
                            for level in range(geo.isobars):
                                row = s * count + level * heads + h
                                totals[level] = totals[level] + dw[j, row : row + 1, :] * value
                for level in range(geo.isobars):
                    pix[level, part : part + 8, :] = totals[level]
            total = jnp.zeros((rows, 4 * BLOCK), F32)
            for b in range(SQUARE_SPAN):
                at = top + b * row_size
                part = pix[:, at : at + row_size, :].reshape(rows, BLOCK)
                total = total + jnp.dot(part.astype(BF16), pick[b], preferred_element_type=F32)
            for ih in range(2):
                left = jnp.zeros((2 * row_size, BLOCK), F32)
                for k in range(geo.slots // 2):
                    at = slice(2 * row_size * k, 2 * row_size * (k + 1))
                    inside = jnp.logical_and(lane >= extra * k, lane < extra * (k + 1))
                    left = jnp.where(inside, total[at, (2 + ih) * BLOCK : (3 + ih) * BLOCK], left)
                main = total[:, ih * BLOCK : (ih + 1) * BLOCK]
                pieces[w, ih, core] = jnp.concatenate([main, left], axis=0).astype(BF16)
            yield

    def run(order="", **steps):
        for name in order:
            next(steps[name])

    mask_copy, qkv_copy, proj_copy, up_copy, down_copy, fold_copy = copies
    for copy in (mask_copy, qkv_copy, proj_copy):
        copy.wait()
    lane_base = lax.rem(grid * geo.run + bands * geo.run - geo.run // 2, BLOCK) if geo.scatter else 0
    if geo.scatter:
        for b in range(SQUARE_SPAN):
            for part in range(4):
                lanes = slice(part * BLOCK, (part + 1) * BLOCK)
                pick[b, :, lanes] = pltpu.roll(pick[b, :, lanes].astype(F32), lane_base, 1).astype(BF16)
    n_own = layer_norm(own[...].reshape(windows * half, features).astype(F32)).astype(BF16)
    for s in range(cores):
        for i in range(3):
            one = jnp.dot(n_own, qkv[s, i], preferred_element_type=F32).astype(BF16)
            ready[s, i] = one.reshape(windows, half, width)
    arrive(turn(0))
    run("a" * ORDER.count("a"), a=attend(turn(0)))
    for copy in (up_copy, down_copy, fold_copy):
        copy.wait()
    whole = jnp.zeros((pixels, features), F32)
    for s in range(cores):
        for h in range(heads):
            top = 2 * count + h * pixels
            whole = whole + fold[s, top : top + pixels, :].astype(F32)
    whole_hi = whole.astype(BF16)
    fold_base[0:pixels, :] = whole_hi
    fold_base[pixels:, :] = (whole - whole_hi.astype(F32)).astype(BF16)

    last = windows - 1

    def complete(w):
        yield from finish(w)
        yield from paint(w)

    @pl.loop(0, last)
    def _(step):
        arrive(turn(step + 1))
        run(ORDER, a=attend(turn(step + 1)), b=complete(turn(step)))
        send(turn(step))

    finishing = complete(turn(last))
    run("b" * (ORDER.count("b") - cores), b=finishing)
    for core in range(cores):
        next(finishing)
        send(turn(last), (core,))

    for copy in halos:
        copy.wait_send()
    if geo.scatter:

        @pl.loop(0, bands)
        def _(s):
            for ih in range(2):
                target = out_ref.at[s, ih]
                pltpu.make_async_copy(target, target, piece_recv.at[s, ih]).wait()

        @pl.loop(0, windows)
        def _(w):
            for ih in range(2):
                for core in range(cores):
                    piece_copy(w, ih, core, "finish")

    else:
        copy = pltpu.make_async_copy(pieces, out_ref, load_sem.at[0])
        copy.start()
        copy.wait()


def forecast(geo, *args):
    tables = (
        jnp.asarray(geo.order_table(), BF16),
        jnp.asarray(geo.position_table(), jnp.int32),
        jnp.asarray(geo.pixel_table(), BF16),
        jnp.asarray(geo.pick_table(), BF16),
    )
    features, width, cores, windows = geo.features, geo.width, geo.cores, geo.windows
    units = args[4].shape[1]
    fold_rows = geo.heads * (2 * LEVEL_SLOTS + geo.pixels)
    vmem = pltpu.VMEM
    dma = pltpu.SemaphoreType.DMA
    if geo.scatter:
        out_shape = (geo.bands, 2, BLOCK, BLOCK)
    else:
        out_shape = (windows, 2, cores, BLOCK, BLOCK)
    return pl.pallas_call(
        functools.partial(main_kernel, geo),
        out_shape=jax.ShapeDtypeStruct(out_shape, BF16),
        in_specs=[pl.BlockSpec(memory_space=pltpu.HBM)] * (len(args) + len(tables)),
        out_specs=pl.BlockSpec(memory_space=vmem if geo.scatter else pltpu.HBM),
        scratch_shapes=[
            vmem((geo.cols, geo.levels, geo.taken, features), BF16),
            vmem((2, geo.cols, geo.rows), jnp.int32),
            vmem((cores, 3, features, width), BF16),
            vmem((cores, width, features), BF16),
            vmem((cores, features, units), BF16),
            vmem((cores, units, features), BF16),
            *[vmem(one.shape, one.dtype) for one in args[6:]],
            *[vmem(one.shape, one.dtype) for one in tables],
            vmem((cores, fold_rows, features), BF16),
            vmem((windows, geo.half, features), BF16),
            vmem((windows, geo.half, features), BF16),
            vmem((windows, geo.half, features), BF16),
            vmem((geo.tokens, KEYS), F32),
            vmem((geo.tokens, cores * units), BF16),
            vmem((geo.levels - 1, cores * geo.heads * LEVEL_SLOTS, BLOCK), F32),
            vmem((geo.levels - 1, cores * geo.heads * geo.pixels, BLOCK), F32),
            vmem((cores, 3, windows, geo.half, width), BF16),
            vmem((2 * geo.pixels, features), BF16),
            vmem((windows, geo.tokens, features), F32),
            vmem((geo.pixels, BLOCK), F32),
            vmem((geo.slots, geo.pixels, BLOCK), F32),
            vmem((windows, 2, cores, BLOCK, BLOCK), BF16),
            vmem((BLOCK, BLOCK), F32),
            dma((geo.taken // 4 + 15,)),
            dma((6,)),
            dma((6,)),
            dma((windows,)),
            dma((windows,)),
            dma((windows, 2, cores)),
            dma((geo.bands, 2)),
        ],
        compiler_params=pltpu.CompilerParams(
            collective_id=0, has_side_effects=True, vmem_limit_bytes=30 * 2**20
        ),
    )(*[pltpu.with_memory_space_constraint(one, pltpu.HBM) for one in (*args, *tables)])


def assemble_kernel(isobars, run, got_ref, out_ref, out, sems):
    bands = got_ref.shape[0]
    half_lat = WIN_LAT // 2
    groups = (isobars + 1) // 2
    tiles = out.shape[-1] // BLOCK
    extra = half_lat * run - BLOCK
    bases = lane_bases(bands, run)
    lane = lax.broadcasted_iota(jnp.int32, (1, BLOCK), 1)
    sublane = lax.broadcasted_iota(jnp.int32, (1, 8, BLOCK), 1)

    def around(start, length):
        start = start % BLOCK
        if start + length <= BLOCK:
            return jnp.logical_and(lane >= start, lane < start + length)
        return jnp.logical_or(lane >= start, lane < start + length - BLOCK)

    def put(merged, value, start, length):
        while length > 0:
            start = start % (tiles * BLOCK)
            tile, part = start // BLOCK, min(length, BLOCK - start % BLOCK)
            old = merged[tile]
            merged[tile] = value if old is None else jnp.where(around(start, part), value, old)
            start, length = start + part, length - part

    copies = []
    middle = (groups + 1) // 2
    for first, last in ((0, middle), (middle, groups)):
        low, high = 2 * first, min(2 * last, isobars)
        found = {}
        for ih in range(2):
            pieces = [got_ref[s, ih, 16 * first : 16 * last, :].astype(F32) for s in range(bands)]
            rests = [got_ref[s, ih, 16 * groups : 16 * groups + 16, :].astype(F32) for s in range(bands)]
            left = []
            for k in range(first, last):
                one = rests[0]
                for s in range(1, bands):
                    one = jnp.where(around(bases[s] + extra * k, extra), rests[s], one)
                left.append(pltpu.roll(one, (-extra * k) % BLOCK, 1) if k > 0 else one)
            left = jnp.concatenate(left, axis=0)
            for r in range(half_lat):
                merged = [None] * tiles
                for s in range(bands):
                    put(merged, pieces[s], bases[s] + run * r, min(run, BLOCK - run * r))
                if run * (r + 1) > BLOCK:
                    for s in range(bands):
                        put(merged, left, bases[s] + BLOCK, run * (r + 1) - BLOCK)
                if r > 0:
                    merged = [pltpu.roll(one, BLOCK - run * r, 1) for one in merged]
                    merged = [
                        jnp.where(lane < BLOCK - run * r, merged[t], merged[(t + 1) % tiles])
                        for t in range(tiles)
                    ]
                found[(1 - ih) * half_lat + r] = merged
        for top in range(0, 2 * half_lat, 2):
            for t in range(tiles):
                upper = found[top][t].reshape(-1, 8, BLOCK)
                lower = found[top + 1][t].reshape(-1, 8, BLOCK)
                some = (
                    jnp.where(sublane < 4, upper, pltpu.roll(lower, 4, 1)),
                    jnp.where(sublane < 4, pltpu.roll(upper, 4, 1), lower),
                )
                for v in range(2):
                    out[v, low:high, 4 * top : 4 * top + 8, t * BLOCK : (t + 1) * BLOCK] = some[v][: high - low]
        for v in range(2):
            copy = pltpu.make_async_copy(
                out.at[v, low:high], out_ref.at[v, low:high], sems.at[len(copies)]
            )
            copy.start()
            copies.append(copy)
    for copy in copies:
        copy.wait()


def assemble(got, geo):
    shape = (TARGET_QUANTITY // geo.cores, geo.isobars, WIN_LAT * SQUARE_SPAN, geo.bands * geo.run)
    return pl.pallas_call(
        functools.partial(assemble_kernel, geo.isobars, geo.run),
        out_shape=jax.ShapeDtypeStruct(shape, F32),
        out_specs=pl.BlockSpec(memory_space=pltpu.HBM),
        scratch_shapes=[pltpu.VMEM(shape, F32), pltpu.SemaphoreType.DMA((4,))],
        compiler_params=pltpu.CompilerParams(vmem_limit_bytes=40 * 2**20),
    )(got)


def exchange(pieces, geo):
    half_lat = WIN_LAT // 2
    run = geo.cols * SQUARE_SPAN
    quantities = TARGET_QUANTITY // geo.cores
    rows = geo.slots * quantities * SQUARE_SPAN
    extra = half_lat * run - BLOCK
    lead = pieces.shape[:3]
    main = pieces[:, :, :, :rows].reshape(*lead, geo.slots, quantities, SQUARE_SPAN, BLOCK)
    rest = pieces[:, :, :, rows:, : extra * (geo.slots // 2)]
    rest = rest.reshape(*lead, 2, quantities, SQUARE_SPAN, geo.slots // 2, extra)
    rest = jnp.moveaxis(rest, 6, 3).reshape(*lead, geo.slots, quantities, SQUARE_SPAN, extra)
    maps = jnp.concatenate([main, rest], axis=-1)[:, :, :, : geo.isobars]
    maps = maps.reshape(*lead, geo.isobars, quantities, SQUARE_SPAN, half_lat, run)
    maps = jnp.transpose(maps, (2, 4, 3, 0, 1, 6, 5, 7))
    maps = maps.reshape(TARGET_QUANTITY, geo.isobars, geo.row_count * SQUARE_SPAN, run)
    maps = lax.all_to_all(maps, "var", split_axis=0, concat_axis=2, tiled=True)
    maps = jnp.roll(maps, half_lat * SQUARE_SPAN, 2)
    maps = lax.all_to_all(maps, "grid", split_axis=2, concat_axis=3, tiled=True)
    return jnp.roll(maps, -(run // 2), 3).astype(F32)


def local(
    tokens,
    key_mask,
    w_qkv,
    w_proj,
    w_up,
    w_down,
    level_query,
    w_dec_q,
    w_dec_kv,
    w_dec_o,
    decode_matrix,
):
    geo = Geometry(
        tokens, w_proj, level_query, decode_matrix, lax.axis_size("var"), lax.axis_size("grid")
    )
    pieces = forecast(
        geo,
        jnp.transpose(tokens, (1, 2, 0, 3)),
        key_mask.T,
        w_qkv,
        w_proj,
        w_up,
        w_down,
        level_query,
        w_dec_q,
        w_dec_kv,
        w_dec_o,
        decode_matrix.T,
    )
    if geo.scatter:
        return assemble(pieces, geo)
    return exchange(pieces, geo)


def solution(mesh):
    placed = (
        P("group", "grid", None, None),
        P("group", "grid"),
        P(None, None, "var"),
        P("var", None),
        P(None, "var"),
        P("var", None),
        P(),
        P(None, "var"),
        P(None, None, "var"),
        P("var", None),
        P(),
    )
    return jax.shard_map(
        local,
        mesh=mesh,
        in_specs=placed,
        out_specs=P("var", "group", "grid", None),
        check_vma=False,
    )
```
